32 devices in a mesh: groups: 2 (over x), strip: 16 (over z, y, core).
Axes of the slice: x: 2, y: 2, z: 4, core: 2. Of those that a mesh axis runs over, the one named last changes fastest.
Arguments:
- incoming_wave: float32 [8, 2, 256, 1024], P('groups', None, 'strip'), parts along dimension 0, may hold values from -64 to 64
- speed_class_map: int32 [4, 256, 1024], P('groups', 'strip'), parts along dimension 0, may hold values from 0 to 15
- spectral_entry_index: int32 [8, 4], P('groups'), parts along dimension 0, may hold values from 0 to 15
- filter_weights: float32 [16, 16, 2, 13], replicated, may hold values from -1.6 to 1.6
- scaled_pulsations: float32 [16], replicated, may hold values from 1 to 6
- inverse_speed_classes: float32 [16], replicated, may hold values from 0.3 to 1.5
Outputs:
- image: float32 [4, 256, 1024], P('groups', 'strip'), parts along dimension 0
- handed: float32 [8, 2, 256, 1024], P('groups', None, 'strip'), parts along dimension 0
The draws below stay inside these ranges and needn't reach their ends.
There are 2 independent parts, one for each index of `groups`. The reference program is written for one: setup_inputs(seed, part) draws one part's arguments, and reference() takes and returns one part's arrays. A program takes and returns all parts, laid end to end along the dimension named above; an argument that names none is the same for every part. Nothing has to cross between parts.
All inputs are finite; a program needn't handle non-finite values.
Results may differ from the reference program's by a relative error of at most 0.0003.
Values sent between devices are 32-bit elements; how exact they have to be, the bound alone decides.
A program may use at most 128 MiB of HBM per device.

```python
import math
import jax
import jax.numpy as jnp
from jax import lax

NY = 1024
SECTIONS = 4
LEVELS = 2
ORDER = 12
NFREQ = 4
NBIN = 16
NW = 16
SIDEWAYS_COUNT = 64


def draw_incoming_wave(key, part):
    noise_key = jax.random.fold_in(jax.random.fold_in(key, 11), 0)
    total_rows = SECTIONS * SIDEWAYS_COUNT
    shifted_rows = (jnp.arange(total_rows, dtype=jnp.int32) - SIDEWAYS_COUNT // 2) % total_rows
    position = (shifted_rows % SIDEWAYS_COUNT).astype(jnp.float32) / max(SIDEWAYS_COUNT - 1, 1)
    profile = jnp.exp(jnp.log(3.0) * position)[None, None, :, None]
    base = jnp.clip(jax.random.normal(noise_key, (NFREQ, 2, total_rows, NY), jnp.float32), -6.0, 6.0)
    return base * profile


def touch_ends(values, rng, smallest, top_value):
    longest = values.shape.index(max(values.shape))
    spots = []
    for shift in (0, 1):
        where = [jax.random.randint(jax.random.fold_in(rng, axis), (), 0, length) for axis, length in enumerate(values.shape)]
        where[longest] = (where[longest] + shift) % values.shape[longest]
        spots.append(tuple(where))
    return values.at[spots[0]].set(smallest).at[spots[1]].set(top_value)


def scatter_about(own_key, dims, spread, bound, kind=jnp.bfloat16):
    drawn = spread * jax.random.normal(own_key, dims, jnp.float32)
    return jnp.clip(drawn, min=-bound, max=bound).astype(kind)


def setup_inputs(seed: int = 0, part: int = 0) -> dict:
    streams_of = jax.random.split(jax.random.key(seed), 7)
    part_splits = jax.random.split(jax.random.fold_in(streams_of[6], part), 7)
    return {
        "incoming_wave": draw_incoming_wave(jax.random.fold_in(jax.random.fold_in(streams_of[6], part), 71), part),
        "speed_class_map": touch_ends(jax.random.randint(part_splits[1], (LEVELS, SECTIONS * SIDEWAYS_COUNT, NY), 0, NBIN), jax.random.fold_in(part_splits[1], 1), 0, NBIN - 1).astype(jnp.int32),
        "spectral_entry_index": touch_ends(jax.random.randint(part_splits[2], (SECTIONS, NFREQ), 0, NW), jax.random.fold_in(part_splits[2], 1), 0, NW - 1).astype(jnp.int32),
        "filter_weights": scatter_about(streams_of[3], (NW, NBIN, 2, ORDER + 1), 0.28, 1.6, jnp.float32),
        "scaled_pulsations": jnp.clip(jnp.exp(jax.random.uniform(streams_of[4], (NW,), jnp.float32, math.log(1.0), math.log(6.0))), 1.0, 6.0),
        "inverse_speed_classes": jnp.clip(jnp.exp(jax.random.uniform(streams_of[5], (NBIN,), jnp.float32, math.log(0.3), math.log(1.5))), 0.3, 1.5),
    }


def stencil_padded(padded):
    vertical = padded[:, :, :-2, :] + padded[:, :, 2:, :]
    middle = padded[:, :, 1:-1, :]
    return -0.5 * middle[..., 1:-1] + 0.25 * (vertical[..., 1:-1] + middle[..., :-2] + middle[..., 2:]) + 0.125 * (vertical[..., :-2] + vertical[..., 2:])

def mcclellan_step(field):
    return stencil_padded(jnp.pad(field, ((0, 0), (0, 0), (1, 1), (1, 1))))

def complex_times(coeff, field):
    real_part = coeff[:, 0] * field[:, 0] - coeff[:, 1] * field[:, 1]
    imag_part = coeff[:, 0] * field[:, 1] + coeff[:, 1] * field[:, 0]
    return jnp.stack([real_part, imag_part], axis=1)

def image_downward(field, speed_strata, freq_row, filter_weights, scaled_pulsations, inverse_speed_classes):
    highest = lax.Precision.HIGHEST
    freq_select = (freq_row[:, None] == jnp.arange(NW, dtype=jnp.int32)[None, :]).astype(jnp.float32)
    freq_coeffs = jnp.einsum('fw,wbck->fbck', freq_select, filter_weights, precision=highest)
    freq_omega = jnp.dot(freq_select, scaled_pulsations, precision=highest)
    wavefield = field
    raws = []
    for level in range(LEVELS):
        cells = speed_strata[level].reshape(-1)
        bin_onehot = (cells[None, :] == jnp.arange(NBIN, dtype=jnp.int32)[:, None]).astype(jnp.float32)
        cell_slowness = jnp.dot(inverse_speed_classes, bin_onehot, precision=highest).reshape(SIDEWAYS_COUNT, NY)
        table = jnp.einsum('fbck,bn->kfcn', freq_coeffs, bin_onehot, precision=highest).reshape(ORDER + 1, NFREQ, 2, SIDEWAYS_COUNT, NY)
        previous = wavefield
        current = mcclellan_step(wavefield)
        accumulated = complex_times(table[0], previous) + complex_times(table[1], current)
        for order_index in range(2, ORDER + 1):
            following = 2.0 * mcclellan_step(current) - previous
            accumulated = accumulated + complex_times(table[order_index], following)
            previous, current = (current, following)
        phase_angle = freq_omega[:, None, None] * cell_slowness[None]
        cosine = jnp.cos(phase_angle)
        sine_part = jnp.sin(phase_angle)
        real_part = accumulated[:, 0] * cosine - accumulated[:, 1] * sine_part
        imag_part = accumulated[:, 0] * sine_part + accumulated[:, 1] * cosine
        wavefield = jnp.stack([real_part, imag_part], axis=1)
        raws.append(lax.optimization_barrier(jnp.sum(real_part, axis=0)))
    return (wavefield, raws)

def reference(incoming_wave, speed_class_map, spectral_entry_index, filter_weights, scaled_pulsations, inverse_speed_classes):
    half_shift = SIDEWAYS_COUNT // 2
    incoming_wave = jnp.roll(incoming_wave, -half_shift, axis=2)
    speed_class_map = jnp.roll(speed_class_map, -half_shift, axis=1)
    bottoms = []
    images = []
    handed_parts = []
    for vertical_slab in range(SECTIONS):
        speed_strata = speed_class_map[:, vertical_slab * SIDEWAYS_COUNT:(vertical_slab + 1) * SIDEWAYS_COUNT, :]
        above_floor_lines, above_unscaled_waves = image_downward(incoming_wave[:, :, vertical_slab * SIDEWAYS_COUNT:(vertical_slab + 1) * SIDEWAYS_COUNT, :], speed_strata, spectral_entry_index[vertical_slab], filter_weights, scaled_pulsations, inverse_speed_classes)
        bottoms.append(above_floor_lines)
        if vertical_slab == 0:
            totals = above_unscaled_waves
            handed_parts.append(above_floor_lines)
        else:
            second_bottom, second_raws = image_downward(bottoms[vertical_slab - 1], speed_strata, spectral_entry_index[vertical_slab - 1], filter_weights, scaled_pulsations, inverse_speed_classes)
            totals = [above_unscaled_waves[level] + second_raws[level] for level in range(LEVELS)]
            handed_parts.append(second_bottom)
        section_images = []
        for level in range(LEVELS):
            raw_image = totals[level]
            mean_square = jnp.sum(raw_image * raw_image) / (SIDEWAYS_COUNT * NY)
            section_images.append(raw_image / jnp.sqrt(mean_square + 1e-06))
        images.append(jnp.stack(section_images, axis=0))
    image = jnp.roll(jnp.concatenate(images, axis=1), half_shift, axis=1)
    handed = jnp.roll(jnp.concatenate(handed_parts, axis=2), half_shift, axis=2)
    return (image, handed)
```

```python
import functools
import jax
import jax.numpy as jnp
from jax import lax
from jax.experimental import pallas as pl
from jax.experimental.pallas import tpu as pltpu
from jax.sharding import PartitionSpec as P

SECTIONS = 4
LEVELS = 2
ORDER = 12
NFREQ = 4
NBIN = 16
NW = 16


def extended_2(shard, sides, width):
    for axis, dim in sides:
        devices, length = (lax.axis_size(axis), shard.shape[dim])
        up = [(i, (i + 1) % devices) for i in range(devices)]
        down = [(j, i) for i, j in up]
        last = lax.slice_in_dim(shard, length - width, length, axis=dim)
        initial = lax.slice_in_dim(shard, 0, width, axis=dim)
        before = lax.ppermute(last, axis, up)
        after = lax.ppermute(initial, axis, down)
        shard = jnp.concatenate([before, shard, after], axis=dim)
    return shard


def from_behind(shard, axis, by):
    devices = lax.axis_size(axis)
    return lax.ppermute(shard, axis, [(i, (i + by) % devices) for i in range(devices)])


def stencil_padded(padded):
    vertical = padded[:, :, :-2, :] + padded[:, :, 2:, :]
    middle = padded[:, :, 1:-1, :]
    return (
        -0.5 * middle[..., 1:-1]
        + 0.25 * (vertical[..., 1:-1] + middle[..., :-2] + middle[..., 2:])
        + 0.125 * (vertical[..., :-2] + vertical[..., 2:])
    )


def complex_times(coeff, field):
    real_part = coeff[:, 0] * field[:, 0] - coeff[:, 1] * field[:, 1]
    imag_part = coeff[:, 0] * field[:, 1] + coeff[:, 1] * field[:, 0]
    return jnp.stack([real_part, imag_part], axis=1)


def shards(
    incoming_wave,
    speed_class_map,
    spectral_entry_index,
    filter_weights,
    scaled_pulsations,
    inverse_speed_classes,
):
    highest = lax.Precision.HIGHEST
    summed_along = incoming_wave.shape[2]
    summed_across = incoming_wave.shape[3]
    strip_count = lax.axis_size("strip")
    lateral_count = strip_count // SECTIONS
    position = (lax.axis_index("strip") - lateral_count // 2) % strip_count
    vertical_slab = position // lateral_count
    lateral_place = position % lateral_count
    section_rows = summed_along * lateral_count
    section_cells = section_rows * summed_across
    margin = ORDER
    extended_rows = summed_along + 2 * margin
    lateral_rows = (
        lateral_place * summed_along - margin + jnp.arange(extended_rows, dtype=jnp.int32)
    )
    inside = ((lateral_rows >= 0) & (lateral_rows < section_rows)).astype(jnp.float32)[
        None, None, :, None
    ]

    def mcclellan_step(field):
        padded = jnp.pad(field, ((0, 0), (0, 0), (1, 1), (0, 0)))
        padded = jnp.pad(padded, ((0, 0), (0, 0), (0, 0), (1, 1)))
        result = stencil_padded(padded)
        result = result * inside
        return result

    def interior(field):
        return field[:, :, margin : margin + summed_along, :]

    def image_downward(field, batch_index):
        freq_row = lax.dynamic_index_in_dim(spectral_entry_index, batch_index, 0, keepdims=False)
        freq_select = (freq_row[:, None] == jnp.arange(NW, dtype=jnp.int32)[None, :]).astype(
            jnp.float32
        )
        freq_coeffs = jnp.einsum("fw,wbck->fbck", freq_select, filter_weights, precision=highest)
        freq_omega = jnp.dot(freq_select, scaled_pulsations, precision=highest)
        wavefield = field
        raws = []
        for level in range(LEVELS):
            cells = speed_class_map[level].reshape(-1)
            bin_onehot = (cells[None, :] == jnp.arange(NBIN, dtype=jnp.int32)[:, None]).astype(
                jnp.float32
            )
            cell_slowness = jnp.dot(inverse_speed_classes, bin_onehot, precision=highest).reshape(
                summed_along, summed_across
            )
            table = jnp.einsum("fbck,bn->kfcn", freq_coeffs, bin_onehot, precision=highest).reshape(
                ORDER + 1, NFREQ, 2, summed_along, summed_across
            )
            extended = extended_2(wavefield, (("strip", 2),), ORDER) * inside
            previous = extended
            current = mcclellan_step(extended)
            accumulated = complex_times(table[0], interior(previous)) + complex_times(
                table[1], interior(current)
            )

            def recursion_step(order_index, state_tuple):
                before, present, running = state_tuple
                following = 2.0 * mcclellan_step(present) - before
                coeff = lax.dynamic_index_in_dim(table, order_index, 0, keepdims=False)
                running = running + complex_times(coeff, interior(following))
                return (present, following, running)

            previous, current, accumulated = lax.fori_loop(
                2, ORDER + 1, recursion_step, (previous, current, accumulated)
            )
            phase_angle = freq_omega[:, None, None] * cell_slowness[None]
            cosine = jnp.cos(phase_angle)
            sine_part = jnp.sin(phase_angle)
            real_part = accumulated[:, 0] * cosine - accumulated[:, 1] * sine_part
            imag_part = accumulated[:, 0] * sine_part + accumulated[:, 1] * cosine
            wavefield = jnp.stack([real_part, imag_part], axis=1)
            raws.append(jnp.sum(real_part, axis=0))
        return (wavefield, raws)

    above_floor_lines, above_unscaled_waves = image_downward(incoming_wave, vertical_slab)
    arriving = from_behind(above_floor_lines, "strip", lateral_count)
    second_bottom, second_raws = image_downward(arriving, jnp.maximum(vertical_slab - 1, 0))
    handed = jnp.where(vertical_slab == 0, above_floor_lines, second_bottom)
    first_section = (vertical_slab > 0).astype(jnp.float32)
    totals = [
        above_unscaled_waves[level] + first_section * second_raws[level] for level in range(LEVELS)
    ]
    selector = (jnp.arange(SECTIONS, dtype=jnp.int32) == vertical_slab).astype(jnp.float32)
    images = []
    for level in range(LEVELS):
        raw_image = totals[level]
        spread = lax.psum(selector * jnp.sum(raw_image * raw_image), "strip")
        mean_square = jnp.sum(spread * selector) / section_cells
        images.append(raw_image / jnp.sqrt(mean_square + 1e-06))
    return (jnp.stack(images, axis=0), handed)


SUB = 8
LANES = 128
PAD = 5
UNROLL = 8
TOGETHER = 4
MESH = pl.DeviceIdType.MESH


def at_row(row):
    return pl.ds(pl.multiple_of(row * SUB, SUB), SUB)


def kernel(
    strip_count,
    entry_ref,
    wave_ref,
    map_ref,
    table_ref,
    image_ref,
    handed_ref,
    starts,
    work,
    bottom,
    last,
    last_in,
    wave_out,
    map_out,
    map_all,
    raw,
    raw_in,
    sum_own,
    sum_in,
    swap_sems,
    halo_sems,
    hand_sems,
    fin_sems,
    raw_sems,
    sum_sems,
):
    nfh = wave_ref.shape[0] // 2
    length = wave_ref.shape[2]
    rows = 2 * length
    blocks = wave_ref.shape[3] // LANES
    lateral = strip_count // SECTIONS
    shift = lateral // 2
    pairs = lateral // 2
    margin = ORDER
    first = PAD + margin
    me = lax.axis_index("strip")
    position = lax.rem(me + strip_count - shift, strip_count)
    section = position // lateral
    place = lax.rem(position, lateral)
    pair = place // 2
    half = lax.rem(place, 2)
    up = jnp.where(pair > 0, 1, 0)
    down = jnp.where(pair < pairs - 1, 1, 0)
    has_up = pair > 0
    has_down = pair < pairs - 1
    has_before = section > 0
    has_after = section < SECTIONS - 1
    other = 1 - half

    def device(pos):
        return {"strip": lax.rem(pos + shift + strip_count, strip_count)}

    partner = device(position + 1 - 2 * half)
    upper = device(position - 2)
    lower = device(position + 2)
    deeper = device(position + lateral)
    shallower = device(position + strip_count - lateral)

    def remote(src, dst, sems, index, target):
        return pltpu.make_async_remote_copy(
            src_ref=src,
            dst_ref=dst,
            send_sem=sems.at[(0,) + index],
            recv_sem=sems.at[(1,) + index],
            device_id=target,
            device_id_type=MESH,
        )

    def span(row, count):
        return pl.ds(pl.multiple_of(row * SUB, SUB), count * SUB)

    zero = jnp.zeros((SUB, LANES), jnp.float32)
    for edge in (first - 1, first + rows):
        for f in range(nfh):
            for c in range(2):
                for s in range(2 * LEVELS):
                    starts[s, f, c, at_row(edge), :] = zero
        for c in range(2):
            for k in range(ORDER):
                work[k, c, at_row(edge), :] = zero

    barrier = pltpu.get_barrier_semaphore()
    for d in range(1, lateral):
        mate = device(section * lateral + lax.rem(place + d, lateral))
        pl.semaphore_signal(barrier, inc=1, device_id=mate, device_id_type=MESH)
    for target in (deeper, shallower):
        pl.semaphore_signal(barrier, inc=1, device_id=target, device_id_type=MESH)

    def rearrange(load, store):
        for g in range(length // SUB):
            for j in range(blocks):
                store(g, j, load(g, j))

    def strided(row, g, j):
        return pl.ds((row + g * SUB) * SUB + j, SUB, stride=SUB)

    own_row = half * length
    swaps = []
    for f in range(nfh):
        for c in range(2):
            rearrange(
                lambda g, j: wave_ref[other * nfh + f, c, pl.ds(g * SUB, SUB), pl.ds(j * LANES, LANES)],
                lambda g, j, x: pltpu_store(wave_out.at[f, c], strided(0, g, j), x),
            )
        if f == 0:
            pl.semaphore_wait(barrier, lateral + 1)
        copy = remote(
            wave_out.at[f],
            starts.at[0, f, :, span(first + own_row, length), :],
            swap_sems,
            (f,),
            partner,
        )
        copy.start()
        swaps.append(copy)
    for l in range(LEVELS):
        rearrange(
            lambda g, j: map_ref[l, pl.ds(g * SUB, SUB), pl.ds(j * LANES, LANES)],
            lambda g, j, x: pltpu_store(map_out.at[l], strided(0, g, j), x),
        )
    copy = remote(
        map_out, map_all.at[:, span(own_row, length), :], swap_sems, (nfh,), partner
    )
    copy.start()
    swaps.append(copy)
    for f in range(nfh):
        for c in range(2):
            rearrange(
                lambda g, j: wave_ref[half * nfh + f, c, pl.ds(g * SUB, SUB), pl.ds(j * LANES, LANES)],
                lambda g, j, x: pltpu_store(
                    starts.at[0, f, c], strided(first + own_row, g, j), x
                ),
            )
    for l in range(LEVELS):
        rearrange(
            lambda g, j: map_ref[l, pl.ds(g * SUB, SUB), pl.ds(j * LANES, LANES)],
            lambda g, j, x: pltpu_store(map_all.at[l], strided(own_row, g, j), x),
        )

    def halo_up(stage, f):
        ref = starts.at[stage, f]
        return remote(
            ref.at[:, span(first, margin), :],
            ref.at[:, span(first + rows, margin), :],
            halo_sems,
            (stage, f, 0),
            upper,
        )

    def halo_down(stage, f):
        ref = starts.at[stage, f]
        return remote(
            ref.at[:, span(first + rows - margin, margin), :],
            ref.at[:, span(first - margin, margin), :],
            halo_sems,
            (stage, f, 1),
            lower,
        )

    def send_halo(stage, f):
        pl.when(has_up)(lambda: halo_up(stage, f).start())
        pl.when(has_down)(lambda: halo_down(stage, f).start())

    def wait_halo(stage, f):
        pl.when(has_down)(lambda: halo_up(stage, f).wait_recv())
        pl.when(has_up)(lambda: halo_down(stage, f).wait_recv())

    def hand_parts(f):
        parts = ((0, margin), (rows - margin, margin), (margin, rows - 2 * margin))
        return [
            remote(
                bottom.at[f, :, span(row, count), :],
                starts.at[LEVELS, f, :, span(first + row, count), :],
                hand_sems,
                (f, n),
                deeper,
            )
            for n, (row, count) in enumerate(parts)
        ]

    lane = lax.broadcasted_iota(jnp.int32, (SUB, LANES), 1)
    sub = lax.broadcasted_iota(jnp.int32, (SUB, LANES), 0)
    at_first = lane == 0
    at_last = lane == LANES - 1
    keep_first = sub > 0
    keep_last = sub < SUB - 1

    def across(u):
        right = pltpu.roll(u, 1, 1)
        right_fix = jnp.where(keep_first, pltpu.roll(right, 1, 0), 0.0)
        left = pltpu.roll(u, LANES - 1, 1)
        left_fix = jnp.where(keep_last, pltpu.roll(left, SUB - 1, 0), 0.0)
        return jnp.where(at_first, right_fix, right) + jnp.where(at_last, left_fix, left)

    def reach(k):
        return ((margin - k + UNROLL - 1) // UNROLL) * UNROLL

    def apply(k, present, before, target):
        extra = reach(k)
        low = first - up * extra
        count = (rows + (up + down) * extra) // UNROLL

        def block(i, carry):
            base = low + i * UNROLL
            v = [
                [present[c, at_row(base - 1 + n), :] for n in range(UNROLL + 2)]
                for c in range(2)
            ]
            old = None
            if before is not None:
                old = [
                    [before[c, at_row(base + n), :] for n in range(UNROLL)] for c in range(2)
                ]
            values = []
            for c in range(2):
                q = [v[c][n] + v[c][n + 1] for n in range(UNROLL + 1)]
                for n in range(UNROLL):
                    u = q[n] + q[n + 1]
                    w = across(u) + (u + u)
                    centre = v[c][n + 1]
                    if old is None:
                        value = 0.125 * w - centre
                    else:
                        value = 0.25 * w - (centre + centre + old[c][n])
                    values.append(value)
            for c in range(2):
                for n in range(UNROLL):
                    target[c, at_row(base + n), :] = values[c * UNROLL + n]
            return carry

        lax.fori_loop(0, count, block, 0)

    def unit(tick, level, f, meanwhile=None):
        stage = tick * LEVELS + level
        start = starts.at[stage, f]
        apply(1, start, None, work.at[0])
        apply(2, work.at[0], start, work.at[1])

        def step(k, carry):
            apply(k, work.at[k - 2], work.at[k - 3], work.at[k - 1])
            return carry

        lax.fori_loop(3, ORDER + 1, step, 0)
        if meanwhile is not None:
            meanwhile()
        batch = section if tick == 0 else jnp.maximum(section - 1, 0)
        entry = entry_ref[batch, half * nfh + f]

        def combine(i, carry):
            spots = [TOGETHER * i + n for n in range(TOGETHER)]
            bins = [map_all[level, at_row(r), :] for r in spots]
            real = [None] * TOGETHER
            imag = [None] * TOGETHER
            for n, r in enumerate(spots):
                for k in range(ORDER + 1):
                    cr, ci = (
                        jnp.take_along_axis(
                            jnp.broadcast_to(
                                table_ref[entry, pl.ds(2 * k + c, 1), :], (SUB, LANES)
                            ),
                            bins[n],
                            axis=1,
                            mode="promise_in_bounds",
                        )
                        for c in range(2)
                    )
                    source = start if k == 0 else work.at[k - 1]
                    tr = source[0, at_row(first + r), :]
                    ti = source[1, at_row(first + r), :]
                    re = cr * tr - ci * ti
                    im = cr * ti + ci * tr
                    real[n] = re if k == 0 else real[n] + re
                    imag[n] = im if k == 0 else imag[n] + im
            for n, r in enumerate(spots):
                re, im = real[n], imag[n]
                if tick == 0 and f == 0:
                    raw[level, at_row(r), :] = re
                else:
                    part = re if tick == 0 else jnp.where(has_before, re, 0.0)
                    raw[level, at_row(r), :] = raw[level, at_row(r), :] + part
                for c, value in enumerate((re, im)):
                    if level < LEVELS - 1:
                        starts[stage + 1, f, c, at_row(first + r), :] = value
                    elif tick == 0:
                        bottom[f, c, at_row(r), :] = value
                    else:
                        last[f, c, at_row(r), :] = jnp.where(
                            has_before, value, bottom[f, c, at_row(r), :]
                        )
            return carry

        lax.fori_loop(0, rows // TOGETHER, combine, 0)

    def finish_wave(f):
        return remote(
            last.at[f, :, span(other * length, length), :],
            last_in.at[f],
            fin_sems,
            (f,),
            partner,
        )

    def finish_raw(l):
        return remote(
            raw.at[l, span(other * length, length), :], raw_in.at[l], raw_sems, (l,), partner
        )

    for f in range(nfh):
        swaps[f].wait_recv()
        send_halo(0, f)
    swaps[nfh].wait_recv()
    for level in range(LEVELS):
        for f in range(nfh):
            wait_halo(level, f)
            unit(0, level, f)
            if level < LEVELS - 1:
                send_halo(level + 1, f)
            else:

                @pl.when(has_after)
                def _():
                    for copy in hand_parts(f):
                        copy.start()

    def forward(f):
        @pl.when(has_before)
        def _():
            high, low, mid = hand_parts(f)
            high.wait_recv()
            pl.when(has_up)(lambda: halo_up(LEVELS, f).start())
            low.wait_recv()
            pl.when(has_down)(lambda: halo_down(LEVELS, f).start())
            mid.wait_recv()

    def skip_or(fn):
        pl.when(has_before)(fn)

    forward(0)
    for level in range(LEVELS):
        for f in range(nfh):

            @pl.when(has_before)
            def _():
                wait_halo(LEVELS + level, f)

            later = f + 1 if level == 0 and f + 1 < nfh else None
            unit(1, level, f, None if later is None else lambda: forward(later))
            if level < LEVELS - 1:

                @pl.when(has_before)
                def _():
                    send_halo(LEVELS + level + 1, f)

            else:
                finish_wave(f).start()
        finish_raw(level).start()

    for l in range(LEVELS):
        finish_raw(l).wait_recv()

        def merge(i, carry):
            value = raw[l, at_row(own_row + i), :] + raw_in[l, at_row(i), :]
            raw_in[l, at_row(i), :] = value
            return carry + value * value

        sum_own[pl.ds(l * SUB, SUB), :] = lax.fori_loop(0, length, merge, zero)
    for d in range(1, lateral):
        mate = device(section * lateral + lax.rem(place + d, lateral))
        remote(sum_own, sum_in.at[d], sum_sems, (d,), mate).start()

    for f in range(nfh):
        for c in range(2):
            rearrange(
                lambda g, j: last[f, c, strided(own_row, g, j), :],
                lambda g, j, x: out_store(handed_ref, half * nfh + f, c, g, j, x),
            )
    for f in range(nfh):
        finish_wave(f).wait_recv()
        for c in range(2):
            rearrange(
                lambda g, j: last_in[f, c, strided(0, g, j), :],
                lambda g, j, x: out_store(handed_ref, other * nfh + f, c, g, j, x),
            )

    total = sum_own[...]
    for d in range(1, lateral):
        mate = device(section * lateral + lax.rem(place + d, lateral))
        remote(sum_own, sum_in.at[d], sum_sems, (d,), mate).wait_recv()
        total = total + sum_in[d]
    cells = length * lateral * blocks * LANES
    for l in range(LEVELS):
        mean = jnp.sum(total[l * SUB : (l + 1) * SUB], axis=(0, 1), keepdims=True) / cells
        scale = jnp.broadcast_to(1.0 / jnp.sqrt(mean + 1e-06), (SUB, LANES))

        def put(g, j, x):
            image_ref[l, pl.ds(g * SUB, SUB), pl.ds(j * LANES, LANES)] = x * scale

        rearrange(lambda g, j: raw_in[l, strided(0, g, j), :], put)

    for copy in swaps:
        copy.wait_send()
    for f in range(nfh):
        send_done = lambda make, stage: make(stage, f).wait_send()
        for stage in range(2 * LEVELS):
            live_up = has_up if stage < LEVELS else has_up & has_before
            live_down = has_down if stage < LEVELS else has_down & has_before
            pl.when(live_up)(lambda: send_done(halo_up, stage))
            pl.when(live_down)(lambda: send_done(halo_down, stage))

        @pl.when(has_after)
        def _():
            for copy in hand_parts(f):
                copy.wait_send()

        finish_wave(f).wait_send()
    for l in range(LEVELS):
        finish_raw(l).wait_send()
    for d in range(1, lateral):
        mate = device(section * lateral + lax.rem(place + d, lateral))
        remote(sum_own, sum_in.at[d], sum_sems, (d,), mate).wait_send()


def pltpu_store(ref, where, x):
    ref[where, :] = x


def out_store(ref, f, c, g, j, x):
    ref[f, c, pl.ds(g * SUB, SUB), pl.ds(j * LANES, LANES)] = x


def paired(
    incoming_wave,
    speed_class_map,
    spectral_entry_index,
    filter_weights,
    scaled_pulsations,
    inverse_speed_classes,
):
    strip_count = lax.axis_size("strip")
    lateral = strip_count // SECTIONS
    length = incoming_wave.shape[2]
    nfh = NFREQ // 2
    rows = 2 * length
    tall = (rows + 2 * ORDER + 2 * PAD) * SUB
    table = phase_table(filter_weights, scaled_pulsations, inverse_speed_classes)
    f32 = jnp.float32
    vmem = pl.BlockSpec(memory_space=pltpu.VMEM)

    def dma(*shape):
        return pltpu.SemaphoreType.DMA((2,) + shape)

    return pl.pallas_call(
        functools.partial(kernel, strip_count),
        out_shape=(
            jax.ShapeDtypeStruct(speed_class_map.shape, f32),
            jax.ShapeDtypeStruct(incoming_wave.shape, f32),
        ),
        in_specs=[pl.BlockSpec(memory_space=pltpu.SMEM), vmem, vmem, vmem],
        out_specs=(vmem, vmem),
        scratch_shapes=[
            pltpu.VMEM((2 * LEVELS, nfh, 2, tall, LANES), f32),
            pltpu.VMEM((ORDER, 2, tall, LANES), f32),
            pltpu.VMEM((nfh, 2, rows * SUB, LANES), f32),
            pltpu.VMEM((nfh, 2, rows * SUB, LANES), f32),
            pltpu.VMEM((nfh, 2, length * SUB, LANES), f32),
            pltpu.VMEM((nfh, 2, length * SUB, LANES), f32),
            pltpu.VMEM((LEVELS, length * SUB, LANES), jnp.int32),
            pltpu.VMEM((LEVELS, rows * SUB, LANES), jnp.int32),
            pltpu.VMEM((LEVELS, rows * SUB, LANES), f32),
            pltpu.VMEM((LEVELS, length * SUB, LANES), f32),
            pltpu.VMEM((LEVELS * SUB, LANES), f32),
            pltpu.VMEM((lateral, LEVELS * SUB, LANES), f32),
            dma(nfh + 1),
            dma(2 * LEVELS, nfh, 2),
            dma(nfh, 3),
            dma(nfh),
            dma(LEVELS),
            dma(lateral),
        ],
        compiler_params=pltpu.CompilerParams(
            collective_id=0, has_side_effects=True, vmem_limit_bytes=48 * 1024 * 1024
        ),
    )(spectral_entry_index, incoming_wave, speed_class_map, table)


def transposed(x):
    lane = lax.broadcasted_iota(jnp.int32, (SUB, LANES), 1)
    x = list(x)
    for step in (1, 2, 4):
        odd = (lane // step) % 2 == 1
        for a in range(8):
            if (a // step) % 2 == 0:
                low, high = x[a], x[a + step]
                x[a] = jnp.where(odd, pltpu.roll(high, step, 1), low)
                x[a + step] = jnp.where(odd, high, pltpu.roll(low, LANES - step, 1))
    return x


def quad_kernel(
    strip_count,
    entry_ref,
    wave_ref,
    map_ref,
    table_ref,
    image_ref,
    handed_ref,
    starts,
    terms,
    paired_sum,
    running,
    bottom,
    wave_in,
    map_in,
    bins,
    raw,
    wave_out,
    raw_out,
    raw_in,
    sum_own,
    sum_in,
    wave_sems,
    map_sems,
    relay_sems,
    hand_sems,
    fin_sems,
    raw_sems,
    sum_sems,
    own_sems,
):
    length = wave_ref.shape[2]
    groups = length // SUB
    lateral = strip_count // SECTIONS
    shift = lateral // 2
    me = lax.axis_index("strip")
    position = lax.rem(me + strip_count - shift, strip_count)
    section = position // lateral
    place = lax.rem(position, lateral)
    chip = place // 2
    core = lax.rem(place, 2)
    has_before = section > 0
    has_after = section < SECTIONS - 1
    mates = {1: 2 * chip + 1 - core, 2: 2 * (1 - chip) + core, 3: 2 * (1 - chip) + 1 - core}

    def device(pos):
        return {"strip": lax.rem(pos + shift + strip_count, strip_count)}

    def mate_device(mate):
        return device(section * lateral + mate)

    deeper = device(position + lateral)
    shallower = device(position + strip_count - lateral)

    def remote(src, dst, sems, index, target, arrival=None):
        return pltpu.make_async_remote_copy(
            src_ref=src,
            dst_ref=dst,
            send_sem=sems.at[(0,) + index],
            recv_sem=sems.at[(1,) + (index if arrival is None else arrival)],
            device_id=target,
            device_id_type=MESH,
        )

    barrier = pltpu.get_barrier_semaphore()
    for x in (1, 2, 3):
        pl.semaphore_signal(
            barrier, inc=1, device_id=mate_device(mates[x]), device_id_type=MESH
        )
    for target in (deeper, shallower):
        pl.semaphore_signal(barrier, inc=1, device_id=target, device_id_type=MESH)
    own_wave = pltpu.make_async_copy(wave_ref.at[place], wave_in.at[place], own_sems.at[0])
    own_map = pltpu.make_async_copy(map_ref, map_in.at[place], own_sems.at[1])
    own_wave.start()
    own_map.start()
    pl.semaphore_wait(barrier, lateral + 1)

    def wave_copy(x):
        return remote(
            wave_ref.at[mates[x]], wave_in.at[place], wave_sems, (x,), mate_device(mates[x])
        )

    def map_copy(level, x):
        return remote(
            map_ref.at[level],
            map_in.at[place, level],
            map_sems,
            (level, x),
            mate_device(mates[x]),
        )

    def map_relay(level):
        part = map_in.at[mates[2], level]
        return remote(part, part, relay_sems, (level,), mate_device(mates[1]))

    map_copy(0, 2).start()
    wave_copy(2).start()
    wave_copy(3).start()
    map_copy(1, 2).start()
    map_copy(0, 1).start()
    wave_copy(1).start()
    map_copy(1, 1).start()

    lane = lax.broadcasted_iota(jnp.int32, (SUB, LANES), 1)
    sub = lax.broadcasted_iota(jnp.int32, (SUB, LANES), 0)
    low_lane, high_lane = lane // 8, lane % 8
    to_left = jnp.where(low_lane > 0, lane - 8, jnp.where(high_lane > 0, 119 + high_lane, 0))
    to_right = jnp.where(low_lane < 15, lane + 8, jnp.where(high_lane < 7, high_lane + 1, 127))
    not_first_lane = lane > 0
    not_last_lane = lane < LANES - 1
    not_first_sub = sub > 0
    not_last_sub = sub < SUB - 1

    def cell(m, r):
        return pl.ds((m * SUB + r) * SUB, SUB)

    def lane_pick(x, index):
        return jnp.take_along_axis(x, index, axis=1, mode="promise_in_bounds")

    def spread(load, store):
        out = transposed([load(j) for j in range(8)])
        for m in range(8):
            store(m, out[m])

    def column(m, slot):
        return pl.ds(m * SUB * SUB + slot, SUB, stride=SUB)

    def spread_map(level):
        for d in range(lateral):
            for g in range(groups):
                spread(
                    lambda j: map_in[d, level, pl.ds(g * SUB, SUB), pl.ds(j * LANES, LANES)],
                    lambda m, x: ref_store(bins.at[level], column(m, groups * d + g), x),
                )

    def spread_wave():
        for d in range(lateral):
            for c in range(2):
                for g in range(groups):
                    spread(
                        lambda j: wave_in[d, c, pl.ds(g * SUB, SUB), pl.ds(j * LANES, LANES)],
                        lambda m, x: ref_store(
                            starts.at[0, c], column(m, groups * d + g), x
                        ),
                    )

    def gather_back(source, d, g):
        return transposed([source[column(m, groups * d + g), :] for m in range(8)])

    def coefficient(entry, k, c):
        return jnp.broadcast_to(table_ref[entry, pl.ds(2 * k + c, 1), :], (SUB, LANES))

    def stencil_step(level, entry, k, present, target, first):
        cr, ci = (coefficient(entry, k, c) for c in range(2))
        below = [[None] * 8, [None] * 8]
        for c in range(2):
            for m in range(8):
                edge = pltpu.roll(present[c, cell(m, 7), :], 1, 0)
                edge = jnp.where(not_first_sub, edge, 0.0)
                below[c][m] = edge + present[c, cell(m, 0), :]
        for r in range(8):
            for c in range(2):
                u = []
                for m in range(8):
                    here = present[c, cell(m, r), :]
                    if r < 7:
                        above = present[c, cell(m, r + 1), :]
                    else:
                        above = pltpu.roll(present[c, cell(m, 0), :], SUB - 1, 0)
                        above = jnp.where(not_last_sub, above, 0.0)
                    q = here + above
                    u.append(below[c][m] + q)
                    below[c][m] = q
                left = jnp.where(not_first_lane, lane_pick(u[7], to_left), 0.0)
                right = jnp.where(not_last_lane, lane_pick(u[0], to_right), 0.0)
                u = [left] + u + [right]
                h = [u[m] + u[m + 1] for m in range(9)]
                for m in range(8):
                    w = h[m] + h[m + 1]
                    here = present[c, cell(m, r), :]
                    if first:
                        both = 0.125 * w
                    else:
                        both = 0.25 * w - paired_sum[c, cell(m, r), :]
                    paired_sum[c, cell(m, r), :] = both
                    target[c, cell(m, r), :] = both - here
            for m in range(8):
                index = bins[level, cell(m, r), :]
                br, bi = lane_pick(cr, index), lane_pick(ci, index)
                tr, ti = (present[c, cell(m, r), :] for c in range(2))
                re = br * tr - bi * ti
                im = br * ti + bi * tr
                if not first:
                    re = running[0, cell(m, r), :] + re
                    im = running[1, cell(m, r), :] + im
                running[0, cell(m, r), :] = re
                running[1, cell(m, r), :] = im

    def unit(tick, level, output):
        stage = tick * LEVELS + level
        batch = section if tick == 0 else jnp.maximum(section - 1, 0)
        entry = entry_ref[batch, place]
        stencil_step(level, entry, 0, starts.at[stage], terms.at[1], True)

        def step(k, carry):
            stencil_step(
                level, entry, k, terms.at[lax.rem(k, 2)], terms.at[lax.rem(k + 1, 2)], False
            )
            return carry

        lax.fori_loop(1, ORDER, step, 0)
        final = terms.at[ORDER % 2]
        cr, ci = (coefficient(entry, ORDER, c) for c in range(2))
        for r in range(8):
            for m in range(8):
                index = bins[level, cell(m, r), :]
                br, bi = lane_pick(cr, index), lane_pick(ci, index)
                tr, ti = (final[c, cell(m, r), :] for c in range(2))
                re = running[0, cell(m, r), :] + (br * tr - bi * ti)
                im = running[1, cell(m, r), :] + (br * ti + bi * tr)
                output[0, cell(m, r), :] = re
                output[1, cell(m, r), :] = im
                if tick == 0:
                    raw[level, cell(m, r), :] = re
                else:
                    raw[level, cell(m, r), :] = raw[level, cell(m, r), :] + re

    def hand():
        return remote(bottom, starts.at[LEVELS], hand_sems, (), deeper)

    def finish_raw(level, d):
        return remote(
            raw_out.at[level, d],
            raw_in.at[level, place],
            raw_sems,
            (level, d),
            mate_device(d),
            (level, place),
        )

    def raw_arrival(level, f):
        return remote(
            raw_out.at[level, f], raw_in.at[level, f], raw_sems, (level, f), mate_device(f)
        )

    def finish_wave(d):
        return remote(
            wave_out.at[d], handed_ref.at[place], fin_sems, (d,), mate_device(d), (place,)
        )

    def wave_arrival(f):
        return remote(wave_out.at[f], handed_ref.at[f], fin_sems, (f,), mate_device(f))

    def send_raw(level):
        for d in range(lateral):
            for g in range(groups):
                for j, x in enumerate(gather_back(raw.at[level], d, g)):
                    raw_out[level, d, pl.ds(g * SUB, SUB), pl.ds(j * LANES, LANES)] = x
            pl.when(place != d)(lambda: finish_raw(level, d).start())

    own_map.wait()
    map_copy(0, 2).wait_recv()
    map_relay(0).start()
    map_copy(0, 1).wait_recv()
    map_relay(0).wait_recv()
    spread_map(0)
    own_wave.wait()
    for x in (1, 2, 3):
        wave_copy(x).wait_recv()
    spread_wave()
    unit(0, 0, starts.at[1])
    map_copy(1, 2).wait_recv()
    map_relay(1).start()
    map_copy(1, 1).wait_recv()
    map_relay(1).wait_recv()
    spread_map(1)
    unit(0, 1, bottom)
    pl.when(has_after)(lambda: hand().start())

    @pl.when(has_before)
    def _():
        hand().wait_recv()
        unit(1, 0, starts.at[LEVELS + 1])

    send_raw(0)
    pl.when(has_after)(lambda: hand().wait_send())

    @pl.when(has_before)
    def _():
        unit(1, 1, bottom)

    send_raw(1)
    for d in range(lateral):
        for c in range(2):
            for g in range(groups):
                for j, x in enumerate(gather_back(bottom.at[c], d, g)):
                    wave_out[d, c, pl.ds(g * SUB, SUB), pl.ds(j * LANES, LANES)] = x
        pl.when(place != d)(lambda: finish_wave(d).start())
    own_out = pltpu.make_async_copy(wave_out.at[place], handed_ref.at[place], own_sems.at[0])
    own_out.start()
    for level in range(LEVELS):
        own_raw = pltpu.make_async_copy(
            raw_out.at[level, place], raw_in.at[level, place], own_sems.at[1]
        )
        own_raw.start()
        own_raw.wait()
        for f in range(lateral):
            pl.when(place != f)(lambda: raw_arrival(level, f).wait_recv())

        def merge(g, total):
            row = pl.ds(pl.multiple_of(g * SUB, SUB), SUB)
            for j in range(8):
                col = pl.ds(j * LANES, LANES)
                value = raw_in[level, 0, row, col]
                for f in range(1, lateral):
                    value = value + raw_in[level, f, row, col]
                raw_in[level, 0, row, col] = value
                total = total + value * value
            return total

        sum_own[pl.ds(level * SUB, SUB), :] = lax.fori_loop(
            0, groups, merge, jnp.zeros((SUB, LANES), jnp.float32)
        )
    for x in (1, 2, 3):
        remote(sum_own, sum_in.at[x], sum_sems, (x,), mate_device(mates[x])).start()
    total = sum_own[...]
    for x in (1, 2, 3):
        remote(sum_own, sum_in.at[x], sum_sems, (x,), mate_device(mates[x])).wait_recv()
        total = total + sum_in[x]
    cells = length * lateral * SUB * LANES
    for level in range(LEVELS):
        mean = (
            jnp.sum(total[level * SUB : (level + 1) * SUB], axis=(0, 1), keepdims=True) / cells
        )
        scale = jnp.broadcast_to(1.0 / jnp.sqrt(mean + 1e-06), (SUB, LANES))
        for g in range(groups):
            for j in range(8):
                row, col = pl.ds(g * SUB, SUB), pl.ds(j * LANES, LANES)
                image_ref[level, row, col] = raw_in[level, 0, row, col] * scale
    own_out.wait()
    for f in range(lateral):
        pl.when(place != f)(lambda: wave_arrival(f).wait_recv())
    for x in (1, 2, 3):
        wave_copy(x).wait_send()
        remote(sum_own, sum_in.at[x], sum_sems, (x,), mate_device(mates[x])).wait_send()
    for level in range(LEVELS):
        for x in (1, 2):
            map_copy(level, x).wait_send()
        map_relay(level).wait_send()
    for d in range(lateral):

        @pl.when(place != d)
        def _():
            finish_wave(d).wait_send()
            for level in range(LEVELS):
                finish_raw(level, d).wait_send()


def ref_store(ref, where, x):
    ref[where, :] = x


def phase_table(filter_weights, scaled_pulsations, inverse_speed_classes):
    angle = scaled_pulsations[:, None] * inverse_speed_classes[None, :]
    cosine = jnp.cos(angle)[:, None, :]
    sine = jnp.sin(angle)[:, None, :]
    by_order = jnp.transpose(filter_weights, (2, 0, 3, 1))
    real = by_order[0] * cosine - by_order[1] * sine
    imag = by_order[0] * sine + by_order[1] * cosine
    table = jnp.stack([real, imag], axis=2).reshape(NW, 2 * (ORDER + 1), NBIN)
    return jnp.pad(table, ((0, 0), (0, 0), (0, LANES - NBIN)))


def quads(
    incoming_wave,
    speed_class_map,
    spectral_entry_index,
    filter_weights,
    scaled_pulsations,
    inverse_speed_classes,
):
    strip_count = lax.axis_size("strip")
    lateral = strip_count // SECTIONS
    length, across = incoming_wave.shape[2:]
    tall = length * lateral * SUB
    f32 = jnp.float32
    vmem = pl.BlockSpec(memory_space=pltpu.VMEM)

    def dma(*shape):
        return pltpu.SemaphoreType.DMA((2,) + shape)

    return pl.pallas_call(
        functools.partial(quad_kernel, strip_count),
        out_shape=(
            jax.ShapeDtypeStruct(speed_class_map.shape, f32),
            jax.ShapeDtypeStruct(incoming_wave.shape, f32),
        ),
        in_specs=[pl.BlockSpec(memory_space=pltpu.SMEM), vmem, vmem, vmem],
        out_specs=(vmem, vmem),
        scratch_shapes=[
            pltpu.VMEM((2 * LEVELS, 2, tall, LANES), f32),
            pltpu.VMEM((2, 2, tall, LANES), f32),
            pltpu.VMEM((2, tall, LANES), f32),
            pltpu.VMEM((2, tall, LANES), f32),
            pltpu.VMEM((2, tall, LANES), f32),
            pltpu.VMEM((lateral, 2, length, across), f32),
            pltpu.VMEM((lateral, LEVELS, length, across), jnp.int32),
            pltpu.VMEM((LEVELS, tall, LANES), jnp.int32),
            pltpu.VMEM((LEVELS, tall, LANES), f32),
            pltpu.VMEM((lateral, 2, length, across), f32),
            pltpu.VMEM((LEVELS, lateral, length, across), f32),
            pltpu.VMEM((LEVELS, lateral, length, across), f32),
            pltpu.VMEM((LEVELS * SUB, LANES), f32),
            pltpu.VMEM((lateral, LEVELS * SUB, LANES), f32),
            dma(lateral),
            dma(LEVELS, lateral),
            dma(LEVELS),
            dma(),
            dma(lateral),
            dma(LEVELS, lateral),
            dma(lateral),
            pltpu.SemaphoreType.DMA((2,)),
        ],
        compiler_params=pltpu.CompilerParams(
            collective_id=0, has_side_effects=True, vmem_limit_bytes=48 * 1024 * 1024
        ),
    )(
        spectral_entry_index,
        incoming_wave,
        speed_class_map,
        phase_table(filter_weights, scaled_pulsations, inverse_speed_classes),
    )


def fits(mesh):
    lateral = mesh.shape["strip"] // SECTIONS
    return NFREQ % 2 == 0 and lateral % 4 == 0


def whole_section(mesh, wave):
    lateral = mesh.shape["strip"] // SECTIONS
    full = lateral * wave.shape[2] == SUB * SUB and wave.shape[3] == SUB * LANES
    return lateral == NFREQ == 4 and wave.shape[2] % SUB == 0 and full


def body_for(mesh):
    def body(wave, *rest):
        whole = wave.shape[3] == SUB * LANES and wave.shape[2] % SUB == 0
        if whole_section(mesh, wave):
            return quads(wave, *rest)
        if fits(mesh) and whole and wave.shape[2] >= ORDER:
            return paired(wave, *rest)
        return shards(wave, *rest)

    return body


def solution(mesh):
    return jax.shard_map(
        body_for(mesh),
        mesh=mesh,
        in_specs=(
            P("groups", None, "strip", None),
            P("groups", "strip", None),
            P("groups", None),
            P(),
            P(),
            P(),
        ),
        out_specs=(P("groups", "strip", None), P("groups", None, "strip", None)),
        check_vma=False,
    )
```

```python
import functools
import jax
import jax.numpy as jnp
from jax import lax
from jax.experimental import pallas as pl
from jax.experimental.pallas import tpu as pltpu
from jax.sharding import PartitionSpec as P

SECTIONS = 4
LEVELS = 2
ORDER = 12
NFREQ = 4
NBIN = 16
NW = 16


def extended_2(shard, sides, width):
    for axis, dim in sides:
        devices, length = (lax.axis_size(axis), shard.shape[dim])
        up = [(i, (i + 1) % devices) for i in range(devices)]
        down = [(j, i) for i, j in up]
        last = lax.slice_in_dim(shard, length - width, length, axis=dim)
        initial = lax.slice_in_dim(shard, 0, width, axis=dim)
        before = lax.ppermute(last, axis, up)
        after = lax.ppermute(initial, axis, down)
        shard = jnp.concatenate([before, shard, after], axis=dim)
    return shard


def from_behind(shard, axis, by):
    devices = lax.axis_size(axis)
    return lax.ppermute(shard, axis, [(i, (i + by) % devices) for i in range(devices)])


def stencil_padded(padded):
    vertical = padded[:, :, :-2, :] + padded[:, :, 2:, :]
    middle = padded[:, :, 1:-1, :]
    return (
        -0.5 * middle[..., 1:-1]
        + 0.25 * (vertical[..., 1:-1] + middle[..., :-2] + middle[..., 2:])
        + 0.125 * (vertical[..., :-2] + vertical[..., 2:])
    )


def complex_times(coeff, field):
    real_part = coeff[:, 0] * field[:, 0] - coeff[:, 1] * field[:, 1]
    imag_part = coeff[:, 0] * field[:, 1] + coeff[:, 1] * field[:, 0]
    return jnp.stack([real_part, imag_part], axis=1)


def shards(
    incoming_wave,
    speed_class_map,
    spectral_entry_index,
    filter_weights,
    scaled_pulsations,
    inverse_speed_classes,
):
    highest = lax.Precision.HIGHEST
    summed_along = incoming_wave.shape[2]
    summed_across = incoming_wave.shape[3]
    strip_count = lax.axis_size("strip")
    lateral_count = strip_count // SECTIONS
    position = (lax.axis_index("strip") - lateral_count // 2) % strip_count
    vertical_slab = position // lateral_count
    lateral_place = position % lateral_count
    section_rows = summed_along * lateral_count
    section_cells = section_rows * summed_across
    margin = ORDER
    extended_rows = summed_along + 2 * margin
    lateral_rows = (
        lateral_place * summed_along - margin + jnp.arange(extended_rows, dtype=jnp.int32)
    )
    inside = ((lateral_rows >= 0) & (lateral_rows < section_rows)).astype(jnp.float32)[
        None, None, :, None
    ]

    def mcclellan_step(field):
        padded = jnp.pad(field, ((0, 0), (0, 0), (1, 1), (0, 0)))
        padded = jnp.pad(padded, ((0, 0), (0, 0), (0, 0), (1, 1)))
        result = stencil_padded(padded)
        result = result * inside
        return result

    def interior(field):
        return field[:, :, margin : margin + summed_along, :]

    def image_downward(field, batch_index):
        freq_row = lax.dynamic_index_in_dim(spectral_entry_index, batch_index, 0, keepdims=False)
        freq_select = (freq_row[:, None] == jnp.arange(NW, dtype=jnp.int32)[None, :]).astype(
            jnp.float32
        )
        freq_coeffs = jnp.einsum("fw,wbck->fbck", freq_select, filter_weights, precision=highest)
        freq_omega = jnp.dot(freq_select, scaled_pulsations, precision=highest)
        wavefield = field
        raws = []
        for level in range(LEVELS):
            cells = speed_class_map[level].reshape(-1)
            bin_onehot = (cells[None, :] == jnp.arange(NBIN, dtype=jnp.int32)[:, None]).astype(
                jnp.float32
            )
            cell_slowness = jnp.dot(inverse_speed_classes, bin_onehot, precision=highest).reshape(
                summed_along, summed_across
            )
            table = jnp.einsum("fbck,bn->kfcn", freq_coeffs, bin_onehot, precision=highest).reshape(
                ORDER + 1, NFREQ, 2, summed_along, summed_across
            )
            extended = extended_2(wavefield, (("strip", 2),), ORDER) * inside
            previous = extended
            current = mcclellan_step(extended)
            accumulated = complex_times(table[0], interior(previous)) + complex_times(
                table[1], interior(current)
            )

            def recursion_step(order_index, state_tuple):
                before, present, running = state_tuple
                following = 2.0 * mcclellan_step(present) - before
                coeff = lax.dynamic_index_in_dim(table, order_index, 0, keepdims=False)
                running = running + complex_times(coeff, interior(following))
                return (present, following, running)

            previous, current, accumulated = lax.fori_loop(
                2, ORDER + 1, recursion_step, (previous, current, accumulated)
            )
            phase_angle = freq_omega[:, None, None] * cell_slowness[None]
            cosine = jnp.cos(phase_angle)
            sine_part = jnp.sin(phase_angle)
            real_part = accumulated[:, 0] * cosine - accumulated[:, 1] * sine_part
            imag_part = accumulated[:, 0] * sine_part + accumulated[:, 1] * cosine
            wavefield = jnp.stack([real_part, imag_part], axis=1)
            raws.append(jnp.sum(real_part, axis=0))
        return (wavefield, raws)

    above_floor_lines, above_unscaled_waves = image_downward(incoming_wave, vertical_slab)
    arriving = from_behind(above_floor_lines, "strip", lateral_count)
    second_bottom, second_raws = image_downward(arriving, jnp.maximum(vertical_slab - 1, 0))
    handed = jnp.where(vertical_slab == 0, above_floor_lines, second_bottom)
    first_section = (vertical_slab > 0).astype(jnp.float32)
    totals = [
        above_unscaled_waves[level] + first_section * second_raws[level] for level in range(LEVELS)
    ]
    selector = (jnp.arange(SECTIONS, dtype=jnp.int32) == vertical_slab).astype(jnp.float32)
    images = []
    for level in range(LEVELS):
        raw_image = totals[level]
        spread = lax.psum(selector * jnp.sum(raw_image * raw_image), "strip")
        mean_square = jnp.sum(spread * selector) / section_cells
        images.append(raw_image / jnp.sqrt(mean_square + 1e-06))
    return (jnp.stack(images, axis=0), handed)


SUB = 8
LANES = 128
PAD = 5
UNROLL = 8
TOGETHER = 4
MESH = pl.DeviceIdType.MESH


def at_row(row):
    return pl.ds(pl.multiple_of(row * SUB, SUB), SUB)


def kernel(
    strip_count,
    entry_ref,
    wave_ref,
    map_ref,
    table_ref,
    image_ref,
    handed_ref,
    starts,
    work,
    bottom,
    last,
    last_in,
    wave_out,
    map_out,
    map_all,
    raw,
    raw_in,
    sum_own,
    sum_in,
    swap_sems,
    halo_sems,
    hand_sems,
    fin_sems,
    raw_sems,
    sum_sems,
):
    nfh = wave_ref.shape[0] // 2
    length = wave_ref.shape[2]
    rows = 2 * length
    blocks = wave_ref.shape[3] // LANES
    lateral = strip_count // SECTIONS
    shift = lateral // 2
    pairs = lateral // 2
    margin = ORDER
    first = PAD + margin
    me = lax.axis_index("strip")
    position = lax.rem(me + strip_count - shift, strip_count)
    section = position // lateral
    place = lax.rem(position, lateral)
    pair = place // 2
    half = lax.rem(place, 2)
    up = jnp.where(pair > 0, 1, 0)
    down = jnp.where(pair < pairs - 1, 1, 0)
    has_up = pair > 0
    has_down = pair < pairs - 1
    has_before = section > 0
    has_after = section < SECTIONS - 1
    other = 1 - half

    def device(pos):
        return {"strip": lax.rem(pos + shift + strip_count, strip_count)}

    partner = device(position + 1 - 2 * half)
    upper = device(position - 2)
    lower = device(position + 2)
    deeper = device(position + lateral)
    shallower = device(position + strip_count - lateral)

    def remote(src, dst, sems, index, target):
        return pltpu.make_async_remote_copy(
            src_ref=src,
            dst_ref=dst,
            send_sem=sems.at[(0,) + index],
            recv_sem=sems.at[(1,) + index],
            device_id=target,
            device_id_type=MESH,
        )

    def span(row, count):
        return pl.ds(pl.multiple_of(row * SUB, SUB), count * SUB)

    zero = jnp.zeros((SUB, LANES), jnp.float32)
    for edge in (first - 1, first + rows):
        for f in range(nfh):
            for c in range(2):
                for s in range(2 * LEVELS):
                    starts[s, f, c, at_row(edge), :] = zero
        for c in range(2):
            for k in range(ORDER):
                work[k, c, at_row(edge), :] = zero

    barrier = pltpu.get_barrier_semaphore()
    for d in range(1, lateral):
        mate = device(section * lateral + lax.rem(place + d, lateral))
        pl.semaphore_signal(barrier, inc=1, device_id=mate, device_id_type=MESH)
    for target in (deeper, shallower):
        pl.semaphore_signal(barrier, inc=1, device_id=target, device_id_type=MESH)

    def rearrange(load, store):
        for g in range(length // SUB):
            for j in range(blocks):
                store(g, j, load(g, j))

    def strided(row, g, j):
        return pl.ds((row + g * SUB) * SUB + j, SUB, stride=SUB)

    own_row = half * length
    swaps = []
    for f in range(nfh):
        for c in range(2):
            rearrange(
                lambda g, j: wave_ref[other * nfh + f, c, pl.ds(g * SUB, SUB), pl.ds(j * LANES, LANES)],
                lambda g, j, x: pltpu_store(wave_out.at[f, c], strided(0, g, j), x),
            )
        if f == 0:
            pl.semaphore_wait(barrier, lateral + 1)
        copy = remote(
            wave_out.at[f],
            starts.at[0, f, :, span(first + own_row, length), :],
            swap_sems,
            (f,),
            partner,
        )
        copy.start()
        swaps.append(copy)
    for l in range(LEVELS):
        rearrange(
            lambda g, j: map_ref[l, pl.ds(g * SUB, SUB), pl.ds(j * LANES, LANES)],
            lambda g, j, x: pltpu_store(map_out.at[l], strided(0, g, j), x),
        )
    copy = remote(
        map_out, map_all.at[:, span(own_row, length), :], swap_sems, (nfh,), partner
    )
    copy.start()
    swaps.append(copy)
    for f in range(nfh):
        for c in range(2):
            rearrange(
                lambda g, j: wave_ref[half * nfh + f, c, pl.ds(g * SUB, SUB), pl.ds(j * LANES, LANES)],
                lambda g, j, x: pltpu_store(
                    starts.at[0, f, c], strided(first + own_row, g, j), x
                ),
            )
    for l in range(LEVELS):
        rearrange(
            lambda g, j: map_ref[l, pl.ds(g * SUB, SUB), pl.ds(j * LANES, LANES)],
            lambda g, j, x: pltpu_store(map_all.at[l], strided(own_row, g, j), x),
        )

    def halo_up(stage, f):
        ref = starts.at[stage, f]
        return remote(
            ref.at[:, span(first, margin), :],
            ref.at[:, span(first + rows, margin), :],
            halo_sems,
            (stage, f, 0),
            upper,
        )

    def halo_down(stage, f):
        ref = starts.at[stage, f]
        return remote(
            ref.at[:, span(first + rows - margin, margin), :],
            ref.at[:, span(first - margin, margin), :],
            halo_sems,
            (stage, f, 1),
            lower,
        )

    def send_halo(stage, f):
        pl.when(has_up)(lambda: halo_up(stage, f).start())
        pl.when(has_down)(lambda: halo_down(stage, f).start())

    def wait_halo(stage, f):
        pl.when(has_down)(lambda: halo_up(stage, f).wait_recv())
        pl.when(has_up)(lambda: halo_down(stage, f).wait_recv())

    def hand_parts(f):
        parts = ((0, margin), (rows - margin, margin), (margin, rows - 2 * margin))
        return [
            remote(
                bottom.at[f, :, span(row, count), :],
                starts.at[LEVELS, f, :, span(first + row, count), :],
                hand_sems,
                (f, n),
                deeper,
            )
            for n, (row, count) in enumerate(parts)
        ]

    lane = lax.broadcasted_iota(jnp.int32, (SUB, LANES), 1)
    sub = lax.broadcasted_iota(jnp.int32, (SUB, LANES), 0)
    at_first = lane == 0
    at_last = lane == LANES - 1
    keep_first = sub > 0
    keep_last = sub < SUB - 1

    def across(u):
        right = pltpu.roll(u, 1, 1)
        right_fix = jnp.where(keep_first, pltpu.roll(right, 1, 0), 0.0)
        left = pltpu.roll(u, LANES - 1, 1)
        left_fix = jnp.where(keep_last, pltpu.roll(left, SUB - 1, 0), 0.0)
        return jnp.where(at_first, right_fix, right) + jnp.where(at_last, left_fix, left)

    def reach(k):
        return ((margin - k + UNROLL - 1) // UNROLL) * UNROLL

    def apply(k, present, before, target):
        extra = reach(k)
        low = first - up * extra
        count = (rows + (up + down) * extra) // UNROLL

        def block(i, carry):
            base = low + i * UNROLL
            v = [
                [present[c, at_row(base - 1 + n), :] for n in range(UNROLL + 2)]
                for c in range(2)
            ]
            old = None
            if before is not None:
                old = [
                    [before[c, at_row(base + n), :] for n in range(UNROLL)] for c in range(2)
                ]
            values = []
            for c in range(2):
                q = [v[c][n] + v[c][n + 1] for n in range(UNROLL + 1)]
                for n in range(UNROLL):
                    u = q[n] + q[n + 1]
                    w = across(u) + (u + u)
                    centre = v[c][n + 1]
                    if old is None:
                        value = 0.125 * w - centre
                    else:
                        value = 0.25 * w - (centre + centre + old[c][n])
                    values.append(value)
            for c in range(2):
                for n in range(UNROLL):
                    target[c, at_row(base + n), :] = values[c * UNROLL + n]
            return carry

        lax.fori_loop(0, count, block, 0)

    def unit(tick, level, f, meanwhile=None):
        stage = tick * LEVELS + level
        start = starts.at[stage, f]
        apply(1, start, None, work.at[0])
        apply(2, work.at[0], start, work.at[1])

        def step(k, carry):
            apply(k, work.at[k - 2], work.at[k - 3], work.at[k - 1])
            return carry

        lax.fori_loop(3, ORDER + 1, step, 0)
        if meanwhile is not None:
            meanwhile()
        batch = section if tick == 0 else jnp.maximum(section - 1, 0)
        entry = entry_ref[batch, half * nfh + f]

        def combine(i, carry):
            spots = [TOGETHER * i + n for n in range(TOGETHER)]
            bins = [map_all[level, at_row(r), :] for r in spots]
            real = [None] * TOGETHER
            imag = [None] * TOGETHER
            for n, r in enumerate(spots):
                for k in range(ORDER + 1):
                    cr, ci = (
                        jnp.take_along_axis(
                            jnp.broadcast_to(
                                table_ref[entry, pl.ds(2 * k + c, 1), :], (SUB, LANES)
                            ),
                            bins[n],
                            axis=1,
                            mode="promise_in_bounds",
                        )
                        for c in range(2)
                    )
                    source = start if k == 0 else work.at[k - 1]
                    tr = source[0, at_row(first + r), :]
                    ti = source[1, at_row(first + r), :]
                    re = cr * tr - ci * ti
                    im = cr * ti + ci * tr
                    real[n] = re if k == 0 else real[n] + re
                    imag[n] = im if k == 0 else imag[n] + im
            for n, r in enumerate(spots):
                re, im = real[n], imag[n]
                if tick == 0 and f == 0:
                    raw[level, at_row(r), :] = re
                else:
                    part = re if tick == 0 else jnp.where(has_before, re, 0.0)
                    raw[level, at_row(r), :] = raw[level, at_row(r), :] + part
                for c, value in enumerate((re, im)):
                    if level < LEVELS - 1:
                        starts[stage + 1, f, c, at_row(first + r), :] = value
                    elif tick == 0:
                        bottom[f, c, at_row(r), :] = value
                    else:
                        last[f, c, at_row(r), :] = jnp.where(
                            has_before, value, bottom[f, c, at_row(r), :]
                        )
            return carry

        lax.fori_loop(0, rows // TOGETHER, combine, 0)

    def finish_wave(f):
        return remote(
            last.at[f, :, span(other * length, length), :],
            last_in.at[f],
            fin_sems,
            (f,),
            partner,
        )

    def finish_raw(l):
        return remote(
            raw.at[l, span(other * length, length), :], raw_in.at[l], raw_sems, (l,), partner
        )

    for f in range(nfh):
        swaps[f].wait_recv()
        send_halo(0, f)
    swaps[nfh].wait_recv()
    for level in range(LEVELS):
        for f in range(nfh):
            wait_halo(level, f)
            unit(0, level, f)
            if level < LEVELS - 1:
                send_halo(level + 1, f)
            else:

                @pl.when(has_after)
                def _():
                    for copy in hand_parts(f):
                        copy.start()

    def forward(f):
        @pl.when(has_before)
        def _():
            high, low, mid = hand_parts(f)
            high.wait_recv()
            pl.when(has_up)(lambda: halo_up(LEVELS, f).start())
            low.wait_recv()
            pl.when(has_down)(lambda: halo_down(LEVELS, f).start())
            mid.wait_recv()

    def skip_or(fn):
        pl.when(has_before)(fn)

    forward(0)
    for level in range(LEVELS):
        for f in range(nfh):

            @pl.when(has_before)
            def _():
                wait_halo(LEVELS + level, f)

            later = f + 1 if level == 0 and f + 1 < nfh else None
            unit(1, level, f, None if later is None else lambda: forward(later))
            if level < LEVELS - 1:

                @pl.when(has_before)
                def _():
                    send_halo(LEVELS + level + 1, f)

            else:
                finish_wave(f).start()
        finish_raw(level).start()

    for l in range(LEVELS):
        finish_raw(l).wait_recv()

        def merge(i, carry):
            value = raw[l, at_row(own_row + i), :] + raw_in[l, at_row(i), :]
            raw_in[l, at_row(i), :] = value
            return carry + value * value

        sum_own[pl.ds(l * SUB, SUB), :] = lax.fori_loop(0, length, merge, zero)
    for d in range(1, lateral):
        mate = device(section * lateral + lax.rem(place + d, lateral))
        remote(sum_own, sum_in.at[d], sum_sems, (d,), mate).start()

    for f in range(nfh):
        for c in range(2):
            rearrange(
                lambda g, j: last[f, c, strided(own_row, g, j), :],
                lambda g, j, x: out_store(handed_ref, half * nfh + f, c, g, j, x),
            )
    for f in range(nfh):
        finish_wave(f).wait_recv()
        for c in range(2):
            rearrange(
                lambda g, j: last_in[f, c, strided(0, g, j), :],
                lambda g, j, x: out_store(handed_ref, other * nfh + f, c, g, j, x),
            )

    total = sum_own[...]
    for d in range(1, lateral):
        mate = device(section * lateral + lax.rem(place + d, lateral))
        remote(sum_own, sum_in.at[d], sum_sems, (d,), mate).wait_recv()
        total = total + sum_in[d]
    cells = length * lateral * blocks * LANES
    for l in range(LEVELS):
        mean = jnp.sum(total[l * SUB : (l + 1) * SUB], axis=(0, 1), keepdims=True) / cells
        scale = jnp.broadcast_to(1.0 / jnp.sqrt(mean + 1e-06), (SUB, LANES))

        def put(g, j, x):
            image_ref[l, pl.ds(g * SUB, SUB), pl.ds(j * LANES, LANES)] = x * scale

        rearrange(lambda g, j: raw_in[l, strided(0, g, j), :], put)

    for copy in swaps:
        copy.wait_send()
    for f in range(nfh):
        send_done = lambda make, stage: make(stage, f).wait_send()
        for stage in range(2 * LEVELS):
            live_up = has_up if stage < LEVELS else has_up & has_before
            live_down = has_down if stage < LEVELS else has_down & has_before
            pl.when(live_up)(lambda: send_done(halo_up, stage))
            pl.when(live_down)(lambda: send_done(halo_down, stage))

        @pl.when(has_after)
        def _():
            for copy in hand_parts(f):
                copy.wait_send()

        finish_wave(f).wait_send()
    for l in range(LEVELS):
        finish_raw(l).wait_send()
    for d in range(1, lateral):
        mate = device(section * lateral + lax.rem(place + d, lateral))
        remote(sum_own, sum_in.at[d], sum_sems, (d,), mate).wait_send()


def pltpu_store(ref, where, x):
    ref[where, :] = x


def out_store(ref, f, c, g, j, x):
    ref[f, c, pl.ds(g * SUB, SUB), pl.ds(j * LANES, LANES)] = x


def paired(
    incoming_wave,
    speed_class_map,
    spectral_entry_index,
    filter_weights,
    scaled_pulsations,
    inverse_speed_classes,
):
    strip_count = lax.axis_size("strip")
    lateral = strip_count // SECTIONS
    length = incoming_wave.shape[2]
    nfh = NFREQ // 2
    rows = 2 * length
    tall = (rows + 2 * ORDER + 2 * PAD) * SUB
    table = phase_table(filter_weights, scaled_pulsations, inverse_speed_classes)
    f32 = jnp.float32
    vmem = pl.BlockSpec(memory_space=pltpu.VMEM)

    def dma(*shape):
        return pltpu.SemaphoreType.DMA((2,) + shape)

    return pl.pallas_call(
        functools.partial(kernel, strip_count),
        out_shape=(
            jax.ShapeDtypeStruct(speed_class_map.shape, f32),
            jax.ShapeDtypeStruct(incoming_wave.shape, f32),
        ),
        in_specs=[pl.BlockSpec(memory_space=pltpu.SMEM), vmem, vmem, vmem],
        out_specs=(vmem, vmem),
        scratch_shapes=[
            pltpu.VMEM((2 * LEVELS, nfh, 2, tall, LANES), f32),
            pltpu.VMEM((ORDER, 2, tall, LANES), f32),
            pltpu.VMEM((nfh, 2, rows * SUB, LANES), f32),
            pltpu.VMEM((nfh, 2, rows * SUB, LANES), f32),
            pltpu.VMEM((nfh, 2, length * SUB, LANES), f32),
            pltpu.VMEM((nfh, 2, length * SUB, LANES), f32),
            pltpu.VMEM((LEVELS, length * SUB, LANES), jnp.int32),
            pltpu.VMEM((LEVELS, rows * SUB, LANES), jnp.int32),
            pltpu.VMEM((LEVELS, rows * SUB, LANES), f32),
            pltpu.VMEM((LEVELS, length * SUB, LANES), f32),
            pltpu.VMEM((LEVELS * SUB, LANES), f32),
            pltpu.VMEM((lateral, LEVELS * SUB, LANES), f32),
            dma(nfh + 1),
            dma(2 * LEVELS, nfh, 2),
            dma(nfh, 3),
            dma(nfh),
            dma(LEVELS),
            dma(lateral),
        ],
        compiler_params=pltpu.CompilerParams(
            collective_id=0, has_side_effects=True, vmem_limit_bytes=48 * 1024 * 1024
        ),
    )(spectral_entry_index, incoming_wave, speed_class_map, table)


ROWS = 2 * (ORDER + 1)


def transposed(x):
    lane = lax.broadcasted_iota(jnp.int32, (SUB, LANES), 1)
    x = list(x)
    for step in (1, 2, 4):
        odd = (lane // step) % 2 == 1
        for a in range(8):
            if (a // step) % 2 == 0:
                low, high = x[a], x[a + step]
                x[a] = jnp.where(odd, pltpu.roll(high, step, 1), low)
                x[a + step] = jnp.where(odd, high, pltpu.roll(low, LANES - step, 1))
    return x


def quad_kernel(
    strip_count,
    entry_ref,
    wave_ref,
    map_ref,
    table_ref,
    image_ref,
    handed_ref,
    starts,
    even,
    odd,
    paired_sum,
    running,
    coeffs,
    spread_table,
    bottom,
    wave_in,
    map_in,
    bins,
    raw,
    wave_out,
    raw_out,
    raw_in,
    sum_own,
    sum_in,
    wave_sems,
    map_sems,
    relay_sems,
    hand_sems,
    fin_sems,
    raw_sems,
    sum_sems,
    own_sems,
):
    length = wave_ref.shape[2]
    groups = length // SUB
    lateral = strip_count // SECTIONS
    shift = lateral // 2
    me = lax.axis_index("strip")
    position = lax.rem(me + strip_count - shift, strip_count)
    section = position // lateral
    place = lax.rem(position, lateral)
    chip = place // 2
    core = lax.rem(place, 2)
    has_before = section > 0
    has_after = section < SECTIONS - 1
    mates = {1: 2 * chip + 1 - core, 2: 2 * (1 - chip) + core, 3: 2 * (1 - chip) + 1 - core}

    def device(pos):
        return {"strip": lax.rem(pos + shift + strip_count, strip_count)}

    def mate_device(mate):
        return device(section * lateral + mate)

    deeper = device(position + lateral)
    shallower = device(position + strip_count - lateral)

    def remote(src, dst, sems, index, target, arrival=None):
        return pltpu.make_async_remote_copy(
            src_ref=src,
            dst_ref=dst,
            send_sem=sems.at[(0,) + index],
            recv_sem=sems.at[(1,) + (index if arrival is None else arrival)],
            device_id=target,
            device_id_type=MESH,
        )

    barrier = pltpu.get_barrier_semaphore()
    for x in (1, 2, 3):
        pl.semaphore_signal(
            barrier, inc=1, device_id=mate_device(mates[x]), device_id_type=MESH
        )
    for target in (deeper, shallower):
        pl.semaphore_signal(barrier, inc=1, device_id=target, device_id_type=MESH)
    own_wave = pltpu.make_async_copy(wave_ref.at[place], wave_in.at[place], own_sems.at[0])
    own_map = pltpu.make_async_copy(map_ref, map_in.at[place], own_sems.at[1])
    own_wave.start()
    own_map.start()
    pl.semaphore_wait(barrier, lateral + 1)

    def wave_copy(x):
        return remote(
            wave_ref.at[mates[x]], wave_in.at[place], wave_sems, (x,), mate_device(mates[x])
        )

    def map_copy(level, x):
        return remote(
            map_ref.at[level],
            map_in.at[place, level],
            map_sems,
            (level, x),
            mate_device(mates[x]),
        )

    def map_relay(level):
        part = map_in.at[mates[2], level]
        return remote(part, part, relay_sems, (level,), mate_device(mates[1]))

    map_copy(0, 2).start()
    wave_copy(2).start()
    wave_copy(3).start()
    map_copy(1, 2).start()
    map_copy(0, 1).start()
    wave_copy(1).start()
    map_copy(1, 1).start()

    lane = lax.broadcasted_iota(jnp.int32, (SUB, LANES), 1)
    sub = lax.broadcasted_iota(jnp.int32, (SUB, LANES), 0)
    low_lane, high_lane = lane // 8, lane % 8
    to_left = jnp.where(low_lane > 0, lane - 8, jnp.where(high_lane > 0, 119 + high_lane, 0))
    to_right = jnp.where(low_lane < 15, lane + 8, jnp.where(high_lane < 7, high_lane + 1, 127))
    not_first_lane = lane > 0
    not_last_lane = lane < LANES - 1
    not_first_sub = sub > 0
    not_last_sub = sub < SUB - 1

    def cell(m, r):
        return pl.ds((m * SUB + r) * SUB, SUB)

    def lane_pick(x, index):
        return jnp.take_along_axis(
            x, index, axis=1, mode="promise_in_bounds", wrap_negative_indices=False
        )

    def spread(load, store):
        out = transposed([load(j) for j in range(8)])
        for m in range(8):
            store(m, out[m])

    def column(m, slot):
        return pl.ds(m * SUB * SUB + slot, SUB, stride=SUB)

    def spread_map(level):
        for d in range(lateral):
            for g in range(groups):
                spread(
                    lambda j: map_in[d, level, pl.ds(g * SUB, SUB), pl.ds(j * LANES, LANES)],
                    lambda m, x: ref_store(bins.at[level], column(m, groups * d + g), x),
                )

    def spread_wave():
        for d in range(lateral):
            for c in range(2):
                for g in range(groups):
                    spread(
                        lambda j: wave_in[d, c, pl.ds(g * SUB, SUB), pl.ds(j * LANES, LANES)],
                        lambda m, x: ref_store(
                            starts.at[0, c], column(m, groups * d + g), x
                        ),
                    )

    def gather_back(source, d, g):
        return transposed([source[column(m, groups * d + g), :] for m in range(8)])

    def fill(level, tick):
        batch = section if tick == 0 else jnp.maximum(section - 1, 0)
        entry = entry_ref[batch, place]
        for half in range(2):
            block = table_ref[entry, pl.ds(half * SUB, SUB), :]
            for n in range(ROWS):
                spread_table[half, n] = jnp.broadcast_to(block[:, n : n + 1], (SUB, LANES))

        def one(i, carry):
            where = pl.ds(pl.multiple_of(i * SUB, SUB), SUB)
            bin_ = bins[level, where, :]
            high = bin_ >= SUB
            low_bits = bin_ % SUB
            for n in range(ROWS):
                a, b = (
                    jnp.take_along_axis(
                        spread_table[half, n],
                        low_bits,
                        axis=0,
                        mode="promise_in_bounds",
                        wrap_negative_indices=False,
                    )
                    for half in range(2)
                )
                coeffs[level, n, where, :] = jnp.where(high, b, a)
            return carry

        lax.fori_loop(0, SUB * SUB, one, 0)

    def stencil(present, target, first=False, last=False):
        def channel(c, carry):
            below = []
            for m in range(8):
                edge = pltpu.roll(present[c, cell(m, 7), :], 1, 0)
                edge = jnp.where(not_first_sub, edge, 0.0)
                below.append(edge + present[c, cell(m, 0), :])
            for r in range(8):
                u = []
                for m in range(8):
                    here = present[c, cell(m, r), :]
                    if r < 7:
                        above = present[c, cell(m, r + 1), :]
                    else:
                        above = pltpu.roll(present[c, cell(m, 0), :], SUB - 1, 0)
                        above = jnp.where(not_last_sub, above, 0.0)
                    q = here + above
                    u.append(below[m] + q)
                    below[m] = q
                left = jnp.where(not_first_lane, lane_pick(u[7], to_left), 0.0)
                right = jnp.where(not_last_lane, lane_pick(u[0], to_right), 0.0)
                u = [left] + u + [right]
                h = [u[m] + u[m + 1] for m in range(9)]
                for m in range(8):
                    w = h[m] + h[m + 1]
                    here = present[c, cell(m, r), :]
                    if first:
                        both = 0.125 * w
                    else:
                        both = 0.25 * w - paired_sum[c, cell(m, r), :]
                    if not last:
                        paired_sum[c, cell(m, r), :] = both
                    target[c, cell(m, r), :] = both - here
            return carry

        lax.fori_loop(0, 2, channel, 0)

    def add_orders(level, terms, where, total):
        re, im = (None, None) if total is None else total
        for order, ref in terms:
            tr, ti = (ref[c, where, :] for c in range(2))
            br = coeffs[level, order, where, :]
            bi = coeffs[level, ORDER + 1 + order, where, :]
            dr = br * tr - bi * ti
            di = br * ti + bi * tr
            re, im = (dr, di) if re is None else (re + dr, im + di)
        return re, im

    def sum_so_far(where):
        return [running[c, where, :] for c in range(2)]

    def unit(tick, level, output):
        start = starts.at[tick * LEVELS + level]
        stencil(start, odd, first=True)
        for i in range(SUB * SUB):
            where = pl.ds(i * SUB, SUB)
            total = add_orders(level, [(0, start), (1, odd)], where, None)
            for c in range(2):
                running[c, where, :] = total[c]

        def steps(i, carry):
            stencil(odd, even)
            stencil(even, odd)
            for n in range(SUB * SUB):
                where = pl.ds(n * SUB, SUB)
                terms = [(2 * i + 2, even), (2 * i + 3, odd)]
                total = add_orders(level, terms, where, sum_so_far(where))
                for c in range(2):
                    running[c, where, :] = total[c]
            return carry

        lax.fori_loop(0, ORDER // 2 - 1, steps, 0)
        stencil(odd, even, last=True)
        for r in range(SUB):
            for m in range(SUB):
                where = cell(m, r)
                total = add_orders(level, [(ORDER, even)], where, sum_so_far(where))
                for c in range(2):
                    output[c, where, :] = total[c]
                if tick == 0:
                    raw[level, where, :] = total[0]
                else:
                    raw[level, where, :] = raw[level, where, :] + total[0]

    def hand():
        return remote(bottom, starts.at[LEVELS], hand_sems, (), deeper)

    def finish_raw(level, d):
        return remote(
            raw_out.at[level, d],
            raw_in.at[level, place],
            raw_sems,
            (level, d),
            mate_device(d),
            (level, place),
        )

    def raw_arrival(level, f):
        return remote(
            raw_out.at[level, f], raw_in.at[level, f], raw_sems, (level, f), mate_device(f)
        )

    def finish_wave(d):
        return remote(
            wave_out.at[d], handed_ref.at[place], fin_sems, (d,), mate_device(d), (place,)
        )

    def wave_arrival(f):
        return remote(wave_out.at[f], handed_ref.at[f], fin_sems, (f,), mate_device(f))

    def send_raw(level):
        for d in range(lateral):
            for g in range(groups):
                for j, x in enumerate(gather_back(raw.at[level], d, g)):
                    raw_out[level, d, pl.ds(g * SUB, SUB), pl.ds(j * LANES, LANES)] = x
            pl.when(place != d)(lambda: finish_raw(level, d).start())

    own_map.wait()
    map_copy(0, 2).wait_recv()
    map_relay(0).start()
    map_copy(0, 1).wait_recv()
    map_relay(0).wait_recv()
    spread_map(0)
    fill(0, 0)
    own_wave.wait()
    for x in (1, 2, 3):
        wave_copy(x).wait_recv()
    spread_wave()
    unit(0, 0, starts.at[1])
    map_copy(1, 2).wait_recv()
    map_relay(1).start()
    map_copy(1, 1).wait_recv()
    map_relay(1).wait_recv()
    spread_map(1)
    fill(1, 0)
    unit(0, 1, bottom)
    pl.when(has_after)(lambda: hand().start())

    @pl.when(has_before)
    def _():
        fill(0, 1)
        fill(1, 1)
        hand().wait_recv()
        unit(1, 0, starts.at[LEVELS + 1])

    send_raw(0)
    pl.when(has_after)(lambda: hand().wait_send())

    @pl.when(has_before)
    def _():
        unit(1, 1, bottom)

    send_raw(1)
    for d in range(lateral):
        for c in range(2):
            for g in range(groups):
                for j, x in enumerate(gather_back(bottom.at[c], d, g)):
                    wave_out[d, c, pl.ds(g * SUB, SUB), pl.ds(j * LANES, LANES)] = x
        pl.when(place != d)(lambda: finish_wave(d).start())
    own_out = pltpu.make_async_copy(wave_out.at[place], handed_ref.at[place], own_sems.at[0])
    own_out.start()
    for level in range(LEVELS):
        own_raw = pltpu.make_async_copy(
            raw_out.at[level, place], raw_in.at[level, place], own_sems.at[1]
        )
        own_raw.start()
        own_raw.wait()
        for f in range(lateral):
            pl.when(place != f)(lambda: raw_arrival(level, f).wait_recv())

        def merge(g, total):
            row = pl.ds(pl.multiple_of(g * SUB, SUB), SUB)
            for j in range(8):
                col = pl.ds(j * LANES, LANES)
                value = raw_in[level, 0, row, col]
                for f in range(1, lateral):
                    value = value + raw_in[level, f, row, col]
                raw_in[level, 0, row, col] = value
                total = total + value * value
            return total

        sum_own[pl.ds(level * SUB, SUB), :] = lax.fori_loop(
            0, groups, merge, jnp.zeros((SUB, LANES), jnp.float32)
        )
    for x in (1, 2, 3):
        remote(sum_own, sum_in.at[x], sum_sems, (x,), mate_device(mates[x])).start()
    total = sum_own[...]
    for x in (1, 2, 3):
        remote(sum_own, sum_in.at[x], sum_sems, (x,), mate_device(mates[x])).wait_recv()
        total = total + sum_in[x]
    cells = length * lateral * SUB * LANES
    for level in range(LEVELS):
        mean = (
            jnp.sum(total[level * SUB : (level + 1) * SUB], axis=(0, 1), keepdims=True) / cells
        )
        scale = jnp.broadcast_to(1.0 / jnp.sqrt(mean + 1e-06), (SUB, LANES))
        for g in range(groups):
            for j in range(8):
                row, col = pl.ds(g * SUB, SUB), pl.ds(j * LANES, LANES)
                image_ref[level, row, col] = raw_in[level, 0, row, col] * scale
    own_out.wait()
    for f in range(lateral):
        pl.when(place != f)(lambda: wave_arrival(f).wait_recv())
    for x in (1, 2, 3):
        wave_copy(x).wait_send()
        remote(sum_own, sum_in.at[x], sum_sems, (x,), mate_device(mates[x])).wait_send()
    for level in range(LEVELS):
        for x in (1, 2):
            map_copy(level, x).wait_send()
        map_relay(level).wait_send()
    for d in range(lateral):

        @pl.when(place != d)
        def _():
            finish_wave(d).wait_send()
            for level in range(LEVELS):
                finish_raw(level, d).wait_send()


def ref_store(ref, where, x):
    ref[where, :] = x


def turned(filter_weights, scaled_pulsations, inverse_speed_classes):
    angle = scaled_pulsations[:, None, None] * inverse_speed_classes[None, :, None]
    cosine, sine = jnp.cos(angle), jnp.sin(angle)
    real, imag = filter_weights[:, :, 0], filter_weights[:, :, 1]
    return real * cosine - imag * sine, real * sine + imag * cosine


def phase_table(*tables):
    table = jnp.transpose(jnp.stack(turned(*tables), axis=3), (0, 2, 3, 1))
    table = table.reshape(NW, 2 * (ORDER + 1), NBIN)
    return jnp.pad(table, ((0, 0), (0, 0), (0, LANES - NBIN)))


def quads(
    incoming_wave,
    speed_class_map,
    spectral_entry_index,
    filter_weights,
    scaled_pulsations,
    inverse_speed_classes,
):
    strip_count = lax.axis_size("strip")
    lateral = strip_count // SECTIONS
    length, across = incoming_wave.shape[2:]
    tall = length * lateral * SUB
    f32 = jnp.float32
    vmem = pl.BlockSpec(memory_space=pltpu.VMEM)

    def dma(*shape):
        return pltpu.SemaphoreType.DMA((2,) + shape)

    return pl.pallas_call(
        functools.partial(quad_kernel, strip_count),
        out_shape=(
            jax.ShapeDtypeStruct(speed_class_map.shape, f32),
            jax.ShapeDtypeStruct(incoming_wave.shape, f32),
        ),
        in_specs=[pl.BlockSpec(memory_space=pltpu.SMEM), vmem, vmem, vmem],
        out_specs=(vmem, vmem),
        scratch_shapes=[
            pltpu.VMEM((2 * LEVELS, 2, tall, LANES), f32),
            pltpu.VMEM((2, tall, LANES), f32),
            pltpu.VMEM((2, tall, LANES), f32),
            pltpu.VMEM((2, tall, LANES), f32),
            pltpu.VMEM((2, tall, LANES), f32),
            pltpu.VMEM((LEVELS, ROWS, tall, LANES), f32),
            pltpu.VMEM((2, ROWS, SUB, LANES), f32),
            pltpu.VMEM((2, tall, LANES), f32),
            pltpu.VMEM((lateral, 2, length, across), f32),
            pltpu.VMEM((lateral, LEVELS, length, across), jnp.int32),
            pltpu.VMEM((LEVELS, tall, LANES), jnp.int32),
            pltpu.VMEM((LEVELS, tall, LANES), f32),
            pltpu.VMEM((lateral, 2, length, across), f32),
            pltpu.VMEM((LEVELS, lateral, length, across), f32),
            pltpu.VMEM((LEVELS, lateral, length, across), f32),
            pltpu.VMEM((LEVELS * SUB, LANES), f32),
            pltpu.VMEM((lateral, LEVELS * SUB, LANES), f32),
            dma(lateral),
            dma(LEVELS, lateral),
            dma(LEVELS),
            dma(),
            dma(lateral),
            dma(LEVELS, lateral),
            dma(lateral),
            pltpu.SemaphoreType.DMA((2,)),
        ],
        compiler_params=pltpu.CompilerParams(
            collective_id=0, has_side_effects=True, vmem_limit_bytes=48 * 1024 * 1024
        ),
    )(
        spectral_entry_index,
        incoming_wave,
        speed_class_map,
        jnp.concatenate(
            turned(filter_weights, scaled_pulsations, inverse_speed_classes), axis=2
        ),
    )


def fits(mesh):
    lateral = mesh.shape["strip"] // SECTIONS
    return NFREQ % 2 == 0 and lateral % 4 == 0


def whole_section(mesh, wave):
    lateral = mesh.shape["strip"] // SECTIONS
    full = lateral * wave.shape[2] == SUB * SUB and wave.shape[3] == SUB * LANES
    return lateral == NFREQ == 4 and wave.shape[2] % SUB == 0 and full


def body_for(mesh):
    def body(wave, *rest):
        whole = wave.shape[3] == SUB * LANES and wave.shape[2] % SUB == 0
        if whole_section(mesh, wave):
            return quads(wave, *rest)
        if fits(mesh) and whole and wave.shape[2] >= ORDER:
            return paired(wave, *rest)
        return shards(wave, *rest)

    return body


def solution(mesh):
    return jax.shard_map(
        body_for(mesh),
        mesh=mesh,
        in_specs=(
            P("groups", None, "strip", None),
            P("groups", "strip", None),
            P("groups", None),
            P(),
            P(),
            P(),
        ),
        out_specs=(P("groups", "strip", None), P("groups", None, "strip", None)),
        check_vma=False,
    )
```

```python
import functools
import jax
import jax.numpy as jnp
from jax import lax
from jax.experimental import pallas as pl
from jax.experimental.pallas import tpu as pltpu
from jax.sharding import PartitionSpec as P

SECTIONS = 4
LEVELS = 2
ORDER = 12
NFREQ = 4
NBIN = 16
NW = 16


def extended_2(shard, sides, width):
    for axis, dim in sides:
        devices, length = (lax.axis_size(axis), shard.shape[dim])
        up = [(i, (i + 1) % devices) for i in range(devices)]
        down = [(j, i) for i, j in up]
        last = lax.slice_in_dim(shard, length - width, length, axis=dim)
        initial = lax.slice_in_dim(shard, 0, width, axis=dim)
        before = lax.ppermute(last, axis, up)
        after = lax.ppermute(initial, axis, down)
        shard = jnp.concatenate([before, shard, after], axis=dim)
    return shard


def from_behind(shard, axis, by):
    devices = lax.axis_size(axis)
    return lax.ppermute(shard, axis, [(i, (i + by) % devices) for i in range(devices)])


def stencil_padded(padded):
    vertical = padded[:, :, :-2, :] + padded[:, :, 2:, :]
    middle = padded[:, :, 1:-1, :]
    return (
        -0.5 * middle[..., 1:-1]
        + 0.25 * (vertical[..., 1:-1] + middle[..., :-2] + middle[..., 2:])
        + 0.125 * (vertical[..., :-2] + vertical[..., 2:])
    )


def complex_times(coeff, field):
    real_part = coeff[:, 0] * field[:, 0] - coeff[:, 1] * field[:, 1]
    imag_part = coeff[:, 0] * field[:, 1] + coeff[:, 1] * field[:, 0]
    return jnp.stack([real_part, imag_part], axis=1)


def shards(
    incoming_wave,
    speed_class_map,
    spectral_entry_index,
    filter_weights,
    scaled_pulsations,
    inverse_speed_classes,
):
    highest = lax.Precision.HIGHEST
    summed_along = incoming_wave.shape[2]
    summed_across = incoming_wave.shape[3]
    strip_count = lax.axis_size("strip")
    lateral_count = strip_count // SECTIONS
    position = (lax.axis_index("strip") - lateral_count // 2) % strip_count
    vertical_slab = position // lateral_count
    lateral_place = position % lateral_count
    section_rows = summed_along * lateral_count
    section_cells = section_rows * summed_across
    margin = ORDER
    extended_rows = summed_along + 2 * margin
    lateral_rows = (
        lateral_place * summed_along - margin + jnp.arange(extended_rows, dtype=jnp.int32)
    )
    inside = ((lateral_rows >= 0) & (lateral_rows < section_rows)).astype(jnp.float32)[
        None, None, :, None
    ]

    def mcclellan_step(field):
        padded = jnp.pad(field, ((0, 0), (0, 0), (1, 1), (0, 0)))
        padded = jnp.pad(padded, ((0, 0), (0, 0), (0, 0), (1, 1)))
        result = stencil_padded(padded)
        result = result * inside
        return result

    def interior(field):
        return field[:, :, margin : margin + summed_along, :]

    def image_downward(field, batch_index):
        freq_row = lax.dynamic_index_in_dim(spectral_entry_index, batch_index, 0, keepdims=False)
        freq_select = (freq_row[:, None] == jnp.arange(NW, dtype=jnp.int32)[None, :]).astype(
            jnp.float32
        )
        freq_coeffs = jnp.einsum("fw,wbck->fbck", freq_select, filter_weights, precision=highest)
        freq_omega = jnp.dot(freq_select, scaled_pulsations, precision=highest)
        wavefield = field
        raws = []
        for level in range(LEVELS):
            cells = speed_class_map[level].reshape(-1)
            bin_onehot = (cells[None, :] == jnp.arange(NBIN, dtype=jnp.int32)[:, None]).astype(
                jnp.float32
            )
            cell_slowness = jnp.dot(inverse_speed_classes, bin_onehot, precision=highest).reshape(
                summed_along, summed_across
            )
            table = jnp.einsum("fbck,bn->kfcn", freq_coeffs, bin_onehot, precision=highest).reshape(
                ORDER + 1, NFREQ, 2, summed_along, summed_across
            )
            extended = extended_2(wavefield, (("strip", 2),), ORDER) * inside
            previous = extended
            current = mcclellan_step(extended)
            accumulated = complex_times(table[0], interior(previous)) + complex_times(
                table[1], interior(current)
            )

            def recursion_step(order_index, state_tuple):
                before, present, running = state_tuple
                following = 2.0 * mcclellan_step(present) - before
                coeff = lax.dynamic_index_in_dim(table, order_index, 0, keepdims=False)
                running = running + complex_times(coeff, interior(following))
                return (present, following, running)

            previous, current, accumulated = lax.fori_loop(
                2, ORDER + 1, recursion_step, (previous, current, accumulated)
            )
            phase_angle = freq_omega[:, None, None] * cell_slowness[None]
            cosine = jnp.cos(phase_angle)
            sine_part = jnp.sin(phase_angle)
            real_part = accumulated[:, 0] * cosine - accumulated[:, 1] * sine_part
            imag_part = accumulated[:, 0] * sine_part + accumulated[:, 1] * cosine
            wavefield = jnp.stack([real_part, imag_part], axis=1)
            raws.append(jnp.sum(real_part, axis=0))
        return (wavefield, raws)

    above_floor_lines, above_unscaled_waves = image_downward(incoming_wave, vertical_slab)
    arriving = from_behind(above_floor_lines, "strip", lateral_count)
    second_bottom, second_raws = image_downward(arriving, jnp.maximum(vertical_slab - 1, 0))
    handed = jnp.where(vertical_slab == 0, above_floor_lines, second_bottom)
    first_section = (vertical_slab > 0).astype(jnp.float32)
    totals = [
        above_unscaled_waves[level] + first_section * second_raws[level] for level in range(LEVELS)
    ]
    selector = (jnp.arange(SECTIONS, dtype=jnp.int32) == vertical_slab).astype(jnp.float32)
    images = []
    for level in range(LEVELS):
        raw_image = totals[level]
        spread = lax.psum(selector * jnp.sum(raw_image * raw_image), "strip")
        mean_square = jnp.sum(spread * selector) / section_cells
        images.append(raw_image / jnp.sqrt(mean_square + 1e-06))
    return (jnp.stack(images, axis=0), handed)


SUB = 8
LANES = 128
PAD = 5
UNROLL = 8
TOGETHER = 4
MESH = pl.DeviceIdType.MESH


def at_row(row):
    return pl.ds(pl.multiple_of(row * SUB, SUB), SUB)


def kernel(
    strip_count,
    entry_ref,
    wave_ref,
    map_ref,
    table_ref,
    image_ref,
    handed_ref,
    starts,
    work,
    bottom,
    last,
    last_in,
    wave_out,
    map_out,
    map_all,
    raw,
    raw_in,
    sum_own,
    sum_in,
    swap_sems,
    halo_sems,
    hand_sems,
    fin_sems,
    raw_sems,
    sum_sems,
):
    nfh = wave_ref.shape[0] // 2
    length = wave_ref.shape[2]
    rows = 2 * length
    blocks = wave_ref.shape[3] // LANES
    lateral = strip_count // SECTIONS
    shift = lateral // 2
    pairs = lateral // 2
    margin = ORDER
    first = PAD + margin
    me = lax.axis_index("strip")
    position = lax.rem(me + strip_count - shift, strip_count)
    section = position // lateral
    place = lax.rem(position, lateral)
    pair = place // 2
    half = lax.rem(place, 2)
    up = jnp.where(pair > 0, 1, 0)
    down = jnp.where(pair < pairs - 1, 1, 0)
    has_up = pair > 0
    has_down = pair < pairs - 1
    has_before = section > 0
    has_after = section < SECTIONS - 1
    other = 1 - half

    def device(pos):
        return {"strip": lax.rem(pos + shift + strip_count, strip_count)}

    partner = device(position + 1 - 2 * half)
    upper = device(position - 2)
    lower = device(position + 2)
    deeper = device(position + lateral)
    shallower = device(position + strip_count - lateral)

    def remote(src, dst, sems, index, target):
        return pltpu.make_async_remote_copy(
            src_ref=src,
            dst_ref=dst,
            send_sem=sems.at[(0,) + index],
            recv_sem=sems.at[(1,) + index],
            device_id=target,
            device_id_type=MESH,
        )

    def span(row, count):
        return pl.ds(pl.multiple_of(row * SUB, SUB), count * SUB)

    zero = jnp.zeros((SUB, LANES), jnp.float32)
    for edge in (first - 1, first + rows):
        for f in range(nfh):
            for c in range(2):
                for s in range(2 * LEVELS):
                    starts[s, f, c, at_row(edge), :] = zero
        for c in range(2):
            for k in range(ORDER):
                work[k, c, at_row(edge), :] = zero

    barrier = pltpu.get_barrier_semaphore()
    for d in range(1, lateral):
        mate = device(section * lateral + lax.rem(place + d, lateral))
        pl.semaphore_signal(barrier, inc=1, device_id=mate, device_id_type=MESH)
    for target in (deeper, shallower):
        pl.semaphore_signal(barrier, inc=1, device_id=target, device_id_type=MESH)

    def rearrange(load, store):
        for g in range(length // SUB):
            for j in range(blocks):
                store(g, j, load(g, j))

    def strided(row, g, j):
        return pl.ds((row + g * SUB) * SUB + j, SUB, stride=SUB)

    own_row = half * length
    swaps = []
    for f in range(nfh):
        for c in range(2):
            rearrange(
                lambda g, j: wave_ref[other * nfh + f, c, pl.ds(g * SUB, SUB), pl.ds(j * LANES, LANES)],
                lambda g, j, x: pltpu_store(wave_out.at[f, c], strided(0, g, j), x),
            )
        if f == 0:
            pl.semaphore_wait(barrier, lateral + 1)
        copy = remote(
            wave_out.at[f],
            starts.at[0, f, :, span(first + own_row, length), :],
            swap_sems,
            (f,),
            partner,
        )
        copy.start()
        swaps.append(copy)
    for l in range(LEVELS):
        rearrange(
            lambda g, j: map_ref[l, pl.ds(g * SUB, SUB), pl.ds(j * LANES, LANES)],
            lambda g, j, x: pltpu_store(map_out.at[l], strided(0, g, j), x),
        )
    copy = remote(
        map_out, map_all.at[:, span(own_row, length), :], swap_sems, (nfh,), partner
    )
    copy.start()
    swaps.append(copy)
    for f in range(nfh):
        for c in range(2):
            rearrange(
                lambda g, j: wave_ref[half * nfh + f, c, pl.ds(g * SUB, SUB), pl.ds(j * LANES, LANES)],
                lambda g, j, x: pltpu_store(
                    starts.at[0, f, c], strided(first + own_row, g, j), x
                ),
            )
    for l in range(LEVELS):
        rearrange(
            lambda g, j: map_ref[l, pl.ds(g * SUB, SUB), pl.ds(j * LANES, LANES)],
            lambda g, j, x: pltpu_store(map_all.at[l], strided(own_row, g, j), x),
        )

    def halo_up(stage, f):
        ref = starts.at[stage, f]
        return remote(
            ref.at[:, span(first, margin), :],
            ref.at[:, span(first + rows, margin), :],
            halo_sems,
            (stage, f, 0),
            upper,
        )

    def halo_down(stage, f):
        ref = starts.at[stage, f]
        return remote(
            ref.at[:, span(first + rows - margin, margin), :],
            ref.at[:, span(first - margin, margin), :],
            halo_sems,
            (stage, f, 1),
            lower,
        )

    def send_halo(stage, f):
        pl.when(has_up)(lambda: halo_up(stage, f).start())
        pl.when(has_down)(lambda: halo_down(stage, f).start())

    def wait_halo(stage, f):
        pl.when(has_down)(lambda: halo_up(stage, f).wait_recv())
        pl.when(has_up)(lambda: halo_down(stage, f).wait_recv())

    def hand_parts(f):
        parts = ((0, margin), (rows - margin, margin), (margin, rows - 2 * margin))
        return [
            remote(
                bottom.at[f, :, span(row, count), :],
                starts.at[LEVELS, f, :, span(first + row, count), :],
                hand_sems,
                (f, n),
                deeper,
            )
            for n, (row, count) in enumerate(parts)
        ]

    lane = lax.broadcasted_iota(jnp.int32, (SUB, LANES), 1)
    sub = lax.broadcasted_iota(jnp.int32, (SUB, LANES), 0)
    at_first = lane == 0
    at_last = lane == LANES - 1
    keep_first = sub > 0
    keep_last = sub < SUB - 1

    def across(u):
        right = pltpu.roll(u, 1, 1)
        right_fix = jnp.where(keep_first, pltpu.roll(right, 1, 0), 0.0)
        left = pltpu.roll(u, LANES - 1, 1)
        left_fix = jnp.where(keep_last, pltpu.roll(left, SUB - 1, 0), 0.0)
        return jnp.where(at_first, right_fix, right) + jnp.where(at_last, left_fix, left)

    def reach(k):
        return ((margin - k + UNROLL - 1) // UNROLL) * UNROLL

    def apply(k, present, before, target):
        extra = reach(k)
        low = first - up * extra
        count = (rows + (up + down) * extra) // UNROLL

        def block(i, carry):
            base = low + i * UNROLL
            v = [
                [present[c, at_row(base - 1 + n), :] for n in range(UNROLL + 2)]
                for c in range(2)
            ]
            old = None
            if before is not None:
                old = [
                    [before[c, at_row(base + n), :] for n in range(UNROLL)] for c in range(2)
                ]
            values = []
            for c in range(2):
                q = [v[c][n] + v[c][n + 1] for n in range(UNROLL + 1)]
                for n in range(UNROLL):
                    u = q[n] + q[n + 1]
                    w = across(u) + (u + u)
                    centre = v[c][n + 1]
                    if old is None:
                        value = 0.125 * w - centre
                    else:
                        value = 0.25 * w - (centre + centre + old[c][n])
                    values.append(value)
            for c in range(2):
                for n in range(UNROLL):
                    target[c, at_row(base + n), :] = values[c * UNROLL + n]
            return carry

        lax.fori_loop(0, count, block, 0)

    def unit(tick, level, f, meanwhile=None):
        stage = tick * LEVELS + level
        start = starts.at[stage, f]
        apply(1, start, None, work.at[0])
        apply(2, work.at[0], start, work.at[1])

        def step(k, carry):
            apply(k, work.at[k - 2], work.at[k - 3], work.at[k - 1])
            return carry

        lax.fori_loop(3, ORDER + 1, step, 0)
        if meanwhile is not None:
            meanwhile()
        batch = section if tick == 0 else jnp.maximum(section - 1, 0)
        entry = entry_ref[batch, half * nfh + f]

        def combine(i, carry):
            spots = [TOGETHER * i + n for n in range(TOGETHER)]
            bins = [map_all[level, at_row(r), :] for r in spots]
            real = [None] * TOGETHER
            imag = [None] * TOGETHER
            for n, r in enumerate(spots):
                for k in range(ORDER + 1):
                    cr, ci = (
                        jnp.take_along_axis(
                            jnp.broadcast_to(
                                table_ref[entry, pl.ds(2 * k + c, 1), :], (SUB, LANES)
                            ),
                            bins[n],
                            axis=1,
                            mode="promise_in_bounds",
                        )
                        for c in range(2)
                    )
                    source = start if k == 0 else work.at[k - 1]
                    tr = source[0, at_row(first + r), :]
                    ti = source[1, at_row(first + r), :]
                    re = cr * tr - ci * ti
                    im = cr * ti + ci * tr
                    real[n] = re if k == 0 else real[n] + re
                    imag[n] = im if k == 0 else imag[n] + im
            for n, r in enumerate(spots):
                re, im = real[n], imag[n]
                if tick == 0 and f == 0:
                    raw[level, at_row(r), :] = re
                else:
                    part = re if tick == 0 else jnp.where(has_before, re, 0.0)
                    raw[level, at_row(r), :] = raw[level, at_row(r), :] + part
                for c, value in enumerate((re, im)):
                    if level < LEVELS - 1:
                        starts[stage + 1, f, c, at_row(first + r), :] = value
                    elif tick == 0:
                        bottom[f, c, at_row(r), :] = value
                    else:
                        last[f, c, at_row(r), :] = jnp.where(
                            has_before, value, bottom[f, c, at_row(r), :]
                        )
            return carry

        lax.fori_loop(0, rows // TOGETHER, combine, 0)

    def finish_wave(f):
        return remote(
            last.at[f, :, span(other * length, length), :],
            last_in.at[f],
            fin_sems,
            (f,),
            partner,
        )

    def finish_raw(l):
        return remote(
            raw.at[l, span(other * length, length), :], raw_in.at[l], raw_sems, (l,), partner
        )

    for f in range(nfh):
        swaps[f].wait_recv()
        send_halo(0, f)
    swaps[nfh].wait_recv()
    for level in range(LEVELS):
        for f in range(nfh):
            wait_halo(level, f)
            unit(0, level, f)
            if level < LEVELS - 1:
                send_halo(level + 1, f)
            else:

                @pl.when(has_after)
                def _():
                    for copy in hand_parts(f):
                        copy.start()

    def forward(f):
        @pl.when(has_before)
        def _():
            high, low, mid = hand_parts(f)
            high.wait_recv()
            pl.when(has_up)(lambda: halo_up(LEVELS, f).start())
            low.wait_recv()
            pl.when(has_down)(lambda: halo_down(LEVELS, f).start())
            mid.wait_recv()

    def skip_or(fn):
        pl.when(has_before)(fn)

    forward(0)
    for level in range(LEVELS):
        for f in range(nfh):

            @pl.when(has_before)
            def _():
                wait_halo(LEVELS + level, f)

            later = f + 1 if level == 0 and f + 1 < nfh else None
            unit(1, level, f, None if later is None else lambda: forward(later))
            if level < LEVELS - 1:

                @pl.when(has_before)
                def _():
                    send_halo(LEVELS + level + 1, f)

            else:
                finish_wave(f).start()
        finish_raw(level).start()

    for l in range(LEVELS):
        finish_raw(l).wait_recv()

        def merge(i, carry):
            value = raw[l, at_row(own_row + i), :] + raw_in[l, at_row(i), :]
            raw_in[l, at_row(i), :] = value
            return carry + value * value

        sum_own[pl.ds(l * SUB, SUB), :] = lax.fori_loop(0, length, merge, zero)
    for d in range(1, lateral):
        mate = device(section * lateral + lax.rem(place + d, lateral))
        remote(sum_own, sum_in.at[d], sum_sems, (d,), mate).start()

    for f in range(nfh):
        for c in range(2):
            rearrange(
                lambda g, j: last[f, c, strided(own_row, g, j), :],
                lambda g, j, x: out_store(handed_ref, half * nfh + f, c, g, j, x),
            )
    for f in range(nfh):
        finish_wave(f).wait_recv()
        for c in range(2):
            rearrange(
                lambda g, j: last_in[f, c, strided(0, g, j), :],
                lambda g, j, x: out_store(handed_ref, other * nfh + f, c, g, j, x),
            )

    total = sum_own[...]
    for d in range(1, lateral):
        mate = device(section * lateral + lax.rem(place + d, lateral))
        remote(sum_own, sum_in.at[d], sum_sems, (d,), mate).wait_recv()
        total = total + sum_in[d]
    cells = length * lateral * blocks * LANES
    for l in range(LEVELS):
        mean = jnp.sum(total[l * SUB : (l + 1) * SUB], axis=(0, 1), keepdims=True) / cells
        scale = jnp.broadcast_to(1.0 / jnp.sqrt(mean + 1e-06), (SUB, LANES))

        def put(g, j, x):
            image_ref[l, pl.ds(g * SUB, SUB), pl.ds(j * LANES, LANES)] = x * scale

        rearrange(lambda g, j: raw_in[l, strided(0, g, j), :], put)

    for copy in swaps:
        copy.wait_send()
    for f in range(nfh):
        send_done = lambda make, stage: make(stage, f).wait_send()
        for stage in range(2 * LEVELS):
            live_up = has_up if stage < LEVELS else has_up & has_before
            live_down = has_down if stage < LEVELS else has_down & has_before
            pl.when(live_up)(lambda: send_done(halo_up, stage))
            pl.when(live_down)(lambda: send_done(halo_down, stage))

        @pl.when(has_after)
        def _():
            for copy in hand_parts(f):
                copy.wait_send()

        finish_wave(f).wait_send()
    for l in range(LEVELS):
        finish_raw(l).wait_send()
    for d in range(1, lateral):
        mate = device(section * lateral + lax.rem(place + d, lateral))
        remote(sum_own, sum_in.at[d], sum_sems, (d,), mate).wait_send()


def pltpu_store(ref, where, x):
    ref[where, :] = x


def out_store(ref, f, c, g, j, x):
    ref[f, c, pl.ds(g * SUB, SUB), pl.ds(j * LANES, LANES)] = x


def paired(
    incoming_wave,
    speed_class_map,
    spectral_entry_index,
    filter_weights,
    scaled_pulsations,
    inverse_speed_classes,
):
    strip_count = lax.axis_size("strip")
    lateral = strip_count // SECTIONS
    length = incoming_wave.shape[2]
    nfh = NFREQ // 2
    rows = 2 * length
    tall = (rows + 2 * ORDER + 2 * PAD) * SUB
    table = phase_table(filter_weights, scaled_pulsations, inverse_speed_classes)
    f32 = jnp.float32
    vmem = pl.BlockSpec(memory_space=pltpu.VMEM)

    def dma(*shape):
        return pltpu.SemaphoreType.DMA((2,) + shape)

    return pl.pallas_call(
        functools.partial(kernel, strip_count),
        out_shape=(
            jax.ShapeDtypeStruct(speed_class_map.shape, f32),
            jax.ShapeDtypeStruct(incoming_wave.shape, f32),
        ),
        in_specs=[pl.BlockSpec(memory_space=pltpu.SMEM), vmem, vmem, vmem],
        out_specs=(vmem, vmem),
        scratch_shapes=[
            pltpu.VMEM((2 * LEVELS, nfh, 2, tall, LANES), f32),
            pltpu.VMEM((ORDER, 2, tall, LANES), f32),
            pltpu.VMEM((nfh, 2, rows * SUB, LANES), f32),
            pltpu.VMEM((nfh, 2, rows * SUB, LANES), f32),
            pltpu.VMEM((nfh, 2, length * SUB, LANES), f32),
            pltpu.VMEM((nfh, 2, length * SUB, LANES), f32),
            pltpu.VMEM((LEVELS, length * SUB, LANES), jnp.int32),
            pltpu.VMEM((LEVELS, rows * SUB, LANES), jnp.int32),
            pltpu.VMEM((LEVELS, rows * SUB, LANES), f32),
            pltpu.VMEM((LEVELS, length * SUB, LANES), f32),
            pltpu.VMEM((LEVELS * SUB, LANES), f32),
            pltpu.VMEM((lateral, LEVELS * SUB, LANES), f32),
            dma(nfh + 1),
            dma(2 * LEVELS, nfh, 2),
            dma(nfh, 3),
            dma(nfh),
            dma(LEVELS),
            dma(lateral),
        ],
        compiler_params=pltpu.CompilerParams(
            collective_id=0, has_side_effects=True, vmem_limit_bytes=48 * 1024 * 1024
        ),
    )(spectral_entry_index, incoming_wave, speed_class_map, table)


ROWS = 2 * (ORDER + 1)
TICKS = 2


def lane_pick(x, index):
    return jnp.take_along_axis(
        x, index, axis=1, mode="promise_in_bounds", wrap_negative_indices=False
    )


def transposed(x):
    lane = lax.broadcasted_iota(jnp.int32, (SUB, LANES), 1)
    low = lane % SUB
    bits = [(step, (lane // step) % 2 == 1) for step in (1, 2, 4)]
    x = list(x)
    for step, bit in bits:
        x = [jnp.where(bit, x[(a + step) % SUB], x[a]) for a in range(SUB)]
    for a in range(1, SUB):
        x[a] = lane_pick(x[a], lane - low + (low + SUB - a) % SUB)
    x = [x[-n % SUB] for n in range(SUB)]
    for step, bit in bits:
        x = [jnp.where(bit, x[(m - step) % SUB], x[m]) for m in range(SUB)]
    return x


def chain_kernel(
    count,
    entry_ref,
    pulsation_ref,
    slowness_ref,
    weight_ref,
    wave_ref,
    map_ref,
    image_ref,
    handed_ref,
    starts,
    last,
    even,
    odd,
    paired_sum,
    running,
    coeffs,
    spread_table,
    wave_in,
    map_in,
    bins,
    raw,
    wave_out,
    raw_out,
    raw_in,
    sum_own,
    sum_in,
    wave_sems,
    map_sems,
    relay_sems,
    fin_sems,
    raw_sems,
    sum_sems,
    own_sems,
    own_raw_sems,
):
    length = wave_ref.shape[2]
    groups = length // SUB
    lateral = count // SECTIONS
    half = lateral // 2
    me = lax.axis_index("strip")
    plane = me // lateral
    place = lax.rem(me, lateral)
    side = place // 2
    core = lax.rem(place, 2)
    chain = lax.rem(plane + SECTIONS - 1, SECTIONS)
    section = lax.rem(chain + side, SECTIONS)
    slab = lax.rem(place + half, lateral)
    home = lax.rem(section + 1, SECTIONS)
    near = side == 0
    has_next = chain < SECTIONS - 1
    is_deep = section > 0

    def wrapped(index):
        return lax.rem(index + count, count)

    def device(index):
        return {"strip": wrapped(index)}

    def worker(plane_, f):
        return wrapped(plane_ * lateral + f)

    def owner(section_, d):
        return wrapped(section_ * lateral + half + d)

    partner = device(me + 1 - 2 * core)

    def remote(src, dst, sems, index, target, arrival=None):
        return pltpu.make_async_remote_copy(
            src_ref=src,
            dst_ref=dst,
            send_sem=sems.at[(0,) + index],
            recv_sem=sems.at[(1,) + (index if arrival is None else arrival)],
            device_id=target,
            device_id_type=MESH,
        )

    barrier = pltpu.get_barrier_semaphore()
    base = (plane - 1) * lateral
    for n in range(3 * lateral):
        mate = wrapped(base + n)

        @pl.when(mate != me)
        def _():
            pl.semaphore_signal(barrier, inc=1, device_id=device(mate), device_id_type=MESH)

    own_wave = pltpu.make_async_copy(wave_ref.at[place], wave_in.at[slab], own_sems.at[0])
    own_map = pltpu.make_async_copy(map_ref, map_in.at[side, slab], own_sems.at[1])
    pl.when(near)(own_wave.start)
    pl.when(near | has_next)(own_map.start)

    lane = lax.broadcasted_iota(jnp.int32, (SUB, LANES), 1)
    sub = lax.broadcasted_iota(jnp.int32, (SUB, LANES), 0)
    high_lane, low_lane = lane // SUB, lane % SUB
    to_left = jnp.where(high_lane > 0, lane - SUB, jnp.where(low_lane > 0, 119 + low_lane, 0))
    to_right = jnp.where(
        high_lane < 15, lane + SUB, jnp.where(low_lane < 7, low_lane + 1, LANES - 1)
    )
    not_first_lane = lane > 0
    not_last_lane = lane < LANES - 1
    not_first_sub = sub > 0
    not_last_sub = sub < SUB - 1

    entry = entry_ref[chain, place]
    angle = pulsation_ref[entry] * jnp.broadcast_to(slowness_ref[...], (SUB, LANES))
    cosine, sine = jnp.cos(angle), jnp.sin(angle)
    for k in range(ORDER + 1):
        fr, fi = (
            jnp.broadcast_to(weight_ref[entry, k, pl.ds(c, 1), :], (SUB, LANES))
            for c in range(2)
        )
        turned = (fr * cosine - fi * sine, fr * sine + fi * cosine)
        for c in range(2):
            for part in range(NBIN // SUB):
                spread_table[part, (ORDER + 1) * c + k] = lane_pick(
                    turned[c], sub + part * SUB
                )

    pl.semaphore_wait(barrier, 3 * lateral - 1)

    def wave_copy(f):
        return remote(
            wave_ref.at[f],
            wave_in.at[slab],
            wave_sems,
            (f,),
            device(worker(home, f)),
            (slab,),
        )

    def wave_arrival(d):
        return remote(
            wave_ref.at[0], wave_in.at[d], wave_sems, (d,), device(owner(chain, d))
        )

    def map_copy(tick, y):
        to = worker(home if tick == 0 else section, 2 * y + core)
        copy = remote(
            map_ref,
            map_in.at[tick, slab],
            map_sems,
            (tick, y),
            device(to),
            (tick, slab // 2),
        )
        live = to != me
        return copy, live if tick == 0 else live & is_deep

    def map_arrival(tick, h):
        d = core + 2 * h
        source = owner(chain + tick, d)
        copy = remote(map_ref, map_in.at[tick, d], map_sems, (tick, h), device(source))
        return copy, source != me

    def map_relay(tick, h):
        part = map_in.at[tick, core + 2 * h]
        return remote(part, part, relay_sems, (tick, h), partner)

    def pass_map_on(tick):
        for h in range(2):
            copy, foreign = map_arrival(tick, h)
            pl.when(foreign)(copy.wait_recv)
            pl.when(jnp.logical_not(foreign))(own_map.wait)
            map_relay(tick, h).start()

    def start_map(tick):
        for y in range(2):
            copy, live = map_copy(tick, y)
            pl.when(live)(copy.start)

    start_map(0)
    for i in range(lateral):
        f = lax.rem(i + half * (1 - side), lateral)
        pl.when(worker(home, f) != me)(wave_copy(f).start)
    start_map(1)

    def cell(m, r):
        return pl.ds((m * SUB + r) * SUB, SUB)

    def column(m, slot):
        return pl.ds(m * SUB * SUB + slot, SUB, stride=SUB)

    def gather_back(source, d, g):
        return transposed([source[column(m, groups * d + g), :] for m in range(SUB)])

    def tile(g, j):
        return pl.ds(g * SUB, SUB), pl.ds(j * LANES, LANES)

    def spread(load, ref, d):
        for g in range(groups):
            for m, x in enumerate(transposed([load(*tile(g, j)) for j in range(SUB)])):
                ref[column(m, groups * d + g), :] = x

    def fill(tick, level):
        for d in range(lateral):
            spread(lambda row, col: map_in[tick, d, level, row, col], bins, d)
        n_cells = 2

        def some(i, carry):
            for n in range(n_cells):
                where = pl.ds(pl.multiple_of((i * n_cells + n) * SUB, SUB), SUB)
                bin_ = bins[where, :]
                high = bin_ >= SUB
                low_bits = bin_ % SUB
                for row in range(ROWS):
                    a, b = (
                        jnp.take_along_axis(
                            spread_table[part, row],
                            low_bits,
                            axis=0,
                            mode="promise_in_bounds",
                            wrap_negative_indices=False,
                        )
                        for part in range(NBIN // SUB)
                    )
                    coeffs[tick, level, row, where, :] = jnp.where(high, b, a)
            return carry

        lax.fori_loop(0, SUB * SUB // n_cells, some, 0)

    def stencil(present, target, first=False, last=False):
        def channel(c, carry):
            below = []
            for m in range(8):
                edge = pltpu.roll(present[c, cell(m, 7), :], 1, 0)
                edge = jnp.where(not_first_sub, edge, 0.0)
                below.append(edge + present[c, cell(m, 0), :])
            for r in range(8):
                u = []
                for m in range(8):
                    here = present[c, cell(m, r), :]
                    if r < 7:
                        above = present[c, cell(m, r + 1), :]
                    else:
                        above = pltpu.roll(present[c, cell(m, 0), :], SUB - 1, 0)
                        above = jnp.where(not_last_sub, above, 0.0)
                    q = here + above
                    u.append(below[m] + q)
                    below[m] = q
                left = jnp.where(not_first_lane, lane_pick(u[7], to_left), 0.0)
                right = jnp.where(not_last_lane, lane_pick(u[0], to_right), 0.0)
                u = [left] + u + [right]
                h = [u[m] + u[m + 1] for m in range(9)]
                for m in range(8):
                    w = h[m] + h[m + 1]
                    here = present[c, cell(m, r), :]
                    if first:
                        both = 0.125 * w
                    else:
                        both = 0.25 * w - paired_sum[c, cell(m, r), :]
                    if not last:
                        paired_sum[c, cell(m, r), :] = both
                    target[c, cell(m, r), :] = both - here
            return carry

        lax.fori_loop(0, 2, channel, 0)

    def add_orders(tick, level, terms, where, total):
        re, im = (None, None) if total is None else total
        for order, ref in terms:
            tr, ti = (ref[c, where, :] for c in range(2))
            br = coeffs[tick, level, order, where, :]
            bi = coeffs[tick, level, ORDER + 1 + order, where, :]
            dr = br * tr - bi * ti
            di = br * ti + bi * tr
            re, im = (dr, di) if re is None else (re + dr, im + di)
        return re, im

    def sum_so_far(where):
        return [running[c, where, :] for c in range(2)]

    def unit(tick, level, output):
        start = starts.at[tick * LEVELS + level]
        stencil(start, odd, first=True)
        for i in range(SUB * SUB):
            where = pl.ds(i * SUB, SUB)
            total = add_orders(tick, level, [(0, start), (1, odd)], where, None)
            for c in range(2):
                running[c, where, :] = total[c]

        def steps(i, carry):
            stencil(odd, even)
            stencil(even, odd)
            for n in range(SUB * SUB):
                where = pl.ds(n * SUB, SUB)
                terms = [(2 * i + 2, even), (2 * i + 3, odd)]
                total = add_orders(tick, level, terms, where, sum_so_far(where))
                for c in range(2):
                    running[c, where, :] = total[c]
            return carry

        lax.fori_loop(0, ORDER // 2 - 1, steps, 0)
        stencil(odd, even, last=True)
        for i in range(SUB * SUB):
            where = pl.ds(i * SUB, SUB)
            total = add_orders(tick, level, [(ORDER, even)], where, sum_so_far(where))
            for c in range(2):
                output[c, where, :] = total[c]
            raw[tick, level, where, :] = total[0]

    def raw_copy(tick, level, d):
        to = owner(chain + tick, d)
        copy = remote(
            raw_out.at[tick, level, d],
            raw_in.at[tick, level, place],
            raw_sems,
            (tick, level, d),
            device(to),
            (tick, level, place),
        )
        return copy, to != me

    def own_raw(tick, level):
        return pltpu.make_async_copy(
            raw_out.at[tick, level, slab],
            raw_in.at[tick, level, place],
            own_raw_sems.at[tick, level],
        )

    def raw_arrival(tick, level, f):
        source = worker(home if tick == 0 else section, f)
        copy = remote(
            raw_out.at[tick, level, f],
            raw_in.at[tick, level, f],
            raw_sems,
            (tick, level, f),
            device(source),
        )
        return copy, source != me

    def send_raw(tick, level):
        for d in range(lateral):
            for g in range(groups):
                for j, x in enumerate(gather_back(raw.at[tick, level], d, g)):
                    raw_out[(tick, level, d) + tile(g, j)] = x
            copy, foreign = raw_copy(tick, level, d)
            pl.when(foreign)(copy.start)
            pl.when(jnp.logical_not(foreign))(own_raw(tick, level).start)

    def wave_back(which, d):
        to = owner(chain + which, d)
        copy = remote(
            wave_out.at[which, d],
            handed_ref.at[place],
            fin_sems,
            (which, d),
            device(to),
            (1, place),
        )
        return copy, to != me

    def own_back(which):
        return pltpu.make_async_copy(
            wave_out.at[which, slab], handed_ref.at[place], own_sems.at[0]
        )

    def handed_arrival(f):
        source = worker(jnp.maximum(section, 1), f)
        copy = remote(
            wave_out.at[1, f], handed_ref.at[f], fin_sems, (1, f), device(source)
        )
        return copy, source != me

    def send_wave(which, source):
        for d in range(lateral):
            for c in range(2):
                for g in range(groups):
                    for j, x in enumerate(gather_back(source.at[c], d, g)):
                        wave_out[(which, d, c) + tile(g, j)] = x
            copy, foreign = wave_back(which, d)
            pl.when(foreign)(copy.start)
            pl.when(jnp.logical_not(foreign))(own_back(which).start)

    pass_map_on(0)
    for h in range(2):
        map_relay(0, h).wait_recv()
    fill(0, 0)
    fill(0, 1)
    for d in range(lateral):
        foreign = owner(chain, d) != me
        pl.when(foreign)(wave_arrival(d).wait_recv)
        pl.when(jnp.logical_not(foreign))(own_wave.wait)
        for c in range(2):
            spread(lambda row, col: wave_in[d, c, row, col], starts.at[0, c], d)
    unit(0, 0, starts.at[1])
    pl.when(has_next)(lambda: pass_map_on(1))
    unit(0, 1, starts.at[2])

    @pl.when(chain == 0)
    def _():
        send_wave(0, starts.at[2])

    for level in range(LEVELS):
        send_raw(0, level)

    @pl.when(has_next)
    def _():
        for h in range(2):
            map_relay(1, h).wait_recv()
        fill(1, 0)
        fill(1, 1)
        unit(1, 0, starts.at[3])
        send_raw(1, 0)
        unit(1, 1, last)
        send_raw(1, 1)
        send_wave(1, last)

    for level in range(LEVELS):
        for tick in range(TICKS):
            for f in range(lateral):
                copy, foreign = raw_arrival(tick, level, f)
                own = jnp.logical_not(foreign)
                if tick == 1:
                    foreign, own = foreign & is_deep, own & is_deep
                pl.when(foreign)(copy.wait_recv)
                pl.when(own)(own_raw(tick, level).wait)
        total = jnp.zeros((SUB, LANES), jnp.float32)
        for g in range(groups):
            for j in range(SUB):
                value = second = None
                for f in range(lateral):
                    a, b = (raw_in[(t, level, f) + tile(g, j)] for t in range(TICKS))
                    value = a if value is None else value + a
                    second = b if second is None else second + b
                value = value + jnp.where(is_deep, second, 0.0)
                image_ref[(level,) + tile(g, j)] = value
                total = total + value * value
        sum_own[pl.ds(level * SUB, SUB), :] = total

    def sum_copy(x):
        mate = lax.rem(slab + x, lateral)
        return remote(sum_own, sum_in.at[x], sum_sems, (x,), device(owner(section, mate)))

    for x in range(1, lateral):
        sum_copy(x).start()
    total = sum_own[...]
    for x in range(1, lateral):
        sum_copy(x).wait_recv()
        total = total + sum_in[x]
    cells = length * lateral * SUB * LANES
    for level in range(LEVELS):
        mean = (
            jnp.sum(total[level * SUB : (level + 1) * SUB], axis=(0, 1), keepdims=True) / cells
        )
        scale = jnp.broadcast_to(1.0 / jnp.sqrt(mean + 1e-06), (SUB, LANES))
        for g in range(groups):
            for j in range(SUB):
                where = (level,) + tile(g, j)
                image_ref[where] = image_ref[where] * scale
    for f in range(lateral):
        copy, foreign = handed_arrival(f)
        pl.when(foreign)(copy.wait_recv)
        pl.when(jnp.logical_not(foreign))(own_back(0).wait)
    for x in range(1, lateral):
        sum_copy(x).wait_send()
    for tick in range(TICKS):
        for y in range(2):
            copy, live = map_copy(tick, y)
            pl.when(live)(copy.wait_send)
    for h in range(2):
        map_relay(0, h).wait_send()
        pl.when(has_next)(map_relay(1, h).wait_send)
    for n in range(lateral):
        pl.when(worker(home, n) != me)(wave_copy(n).wait_send)
        for which, live in ((0, chain == 0), (1, has_next)):
            copy, foreign = wave_back(which, n)
            pl.when(foreign & live)(copy.wait_send)
        for level in range(LEVELS):
            for tick in range(TICKS):
                copy, foreign = raw_copy(tick, level, n)
                pl.when(foreign if tick == 0 else foreign & has_next)(copy.wait_send)


def phase_table(filter_weights, scaled_pulsations, inverse_speed_classes):
    angle = scaled_pulsations[:, None] * inverse_speed_classes[None, :]
    cosine = jnp.cos(angle)[:, None, :]
    sine = jnp.sin(angle)[:, None, :]
    by_order = jnp.transpose(filter_weights, (2, 0, 3, 1))
    real = by_order[0] * cosine - by_order[1] * sine
    imag = by_order[0] * sine + by_order[1] * cosine
    table = jnp.stack([real, imag], axis=2).reshape(NW, 2 * (ORDER + 1), NBIN)
    return jnp.pad(table, ((0, 0), (0, 0), (0, LANES - NBIN)))


def chains(
    incoming_wave,
    speed_class_map,
    spectral_entry_index,
    filter_weights,
    scaled_pulsations,
    inverse_speed_classes,
):
    count = lax.axis_size("strip")
    lateral = count // SECTIONS
    length, across = incoming_wave.shape[2:]
    tall = length * lateral * SUB
    f32 = jnp.float32
    vmem = pl.BlockSpec(memory_space=pltpu.VMEM)
    smem = pl.BlockSpec(memory_space=pltpu.SMEM)
    anywhere = pl.BlockSpec(memory_space=pl.ANY)
    blank = LANES - NBIN
    weights = jnp.pad(
        jnp.transpose(filter_weights, (0, 3, 2, 1)), ((0, 0), (0, 0), (0, 0), (0, blank))
    )
    slowness = jnp.pad(inverse_speed_classes[None], ((0, 0), (0, blank)))

    def dma(*shape):
        return pltpu.SemaphoreType.DMA((2,) + shape)

    return pl.pallas_call(
        functools.partial(chain_kernel, count),
        out_shape=(
            jax.ShapeDtypeStruct(speed_class_map.shape, f32),
            jax.ShapeDtypeStruct(incoming_wave.shape, f32),
        ),
        in_specs=[smem, smem, vmem, vmem, anywhere, anywhere],
        out_specs=(vmem, vmem),
        scratch_shapes=[
            pltpu.VMEM((TICKS * LEVELS, 2, tall, LANES), f32),
            pltpu.VMEM((2, tall, LANES), f32),
            pltpu.VMEM((2, tall, LANES), f32),
            pltpu.VMEM((2, tall, LANES), f32),
            pltpu.VMEM((2, tall, LANES), f32),
            pltpu.VMEM((2, tall, LANES), f32),
            pltpu.VMEM((TICKS, LEVELS, ROWS, tall, LANES), f32),
            pltpu.VMEM((NBIN // SUB, ROWS, SUB, LANES), f32),
            pltpu.VMEM((lateral, 2, length, across), f32),
            pltpu.VMEM((TICKS, lateral, LEVELS, length, across), jnp.int32),
            pltpu.VMEM((tall, LANES), jnp.int32),
            pltpu.VMEM((TICKS, LEVELS, tall, LANES), f32),
            pltpu.VMEM((2, lateral, 2, length, across), f32),
            pltpu.VMEM((TICKS, LEVELS, lateral, length, across), f32),
            pltpu.VMEM((TICKS, LEVELS, lateral, length, across), f32),
            pltpu.VMEM((LEVELS * SUB, LANES), f32),
            pltpu.VMEM((lateral, LEVELS * SUB, LANES), f32),
            dma(lateral),
            dma(TICKS, 2),
            dma(TICKS, 2),
            dma(2, lateral),
            dma(TICKS, LEVELS, lateral),
            dma(lateral),
            pltpu.SemaphoreType.DMA((2,)),
            pltpu.SemaphoreType.DMA((TICKS, LEVELS)),
        ],
        compiler_params=pltpu.CompilerParams(
            collective_id=0, has_side_effects=True, vmem_limit_bytes=60 * 1024 * 1024
        ),
    )(
        spectral_entry_index,
        scaled_pulsations,
        slowness,
        weights,
        incoming_wave,
        speed_class_map,
    )


def fits(mesh):
    lateral = mesh.shape["strip"] // SECTIONS
    return NFREQ % 2 == 0 and lateral % 4 == 0


def whole_section(mesh, wave):
    lateral = mesh.shape["strip"] // SECTIONS
    full = lateral * wave.shape[2] == SUB * SUB and wave.shape[3] == SUB * LANES
    return lateral == NFREQ == 4 and wave.shape[2] % SUB == 0 and full


def body_for(mesh):
    def body(wave, *rest):
        whole = wave.shape[3] == SUB * LANES and wave.shape[2] % SUB == 0
        if whole_section(mesh, wave):
            return chains(wave, *rest)
        if fits(mesh) and whole and wave.shape[2] >= ORDER:
            return paired(wave, *rest)
        return shards(wave, *rest)

    return body


def solution(mesh):
    return jax.shard_map(
        body_for(mesh),
        mesh=mesh,
        in_specs=(
            P("groups", None, "strip", None),
            P("groups", "strip", None),
            P("groups", None),
            P(),
            P(),
            P(),
        ),
        out_specs=(P("groups", "strip", None), P("groups", None, "strip", None)),
        check_vma=False,
    )
```

```python
import functools
import jax
import jax.numpy as jnp
from jax import lax
from jax.experimental import pallas as pl
from jax.experimental.pallas import tpu as pltpu
from jax.sharding import PartitionSpec as P

SECTIONS = 4
LEVELS = 2
ORDER = 12
NFREQ = 4
NBIN = 16
NW = 16


def extended_2(shard, sides, width):
    for axis, dim in sides:
        devices, length = (lax.axis_size(axis), shard.shape[dim])
        up = [(i, (i + 1) % devices) for i in range(devices)]
        down = [(j, i) for i, j in up]
        last = lax.slice_in_dim(shard, length - width, length, axis=dim)
        initial = lax.slice_in_dim(shard, 0, width, axis=dim)
        before = lax.ppermute(last, axis, up)
        after = lax.ppermute(initial, axis, down)
        shard = jnp.concatenate([before, shard, after], axis=dim)
    return shard


def from_behind(shard, axis, by):
    devices = lax.axis_size(axis)
    return lax.ppermute(shard, axis, [(i, (i + by) % devices) for i in range(devices)])


def stencil_padded(padded):
    vertical = padded[:, :, :-2, :] + padded[:, :, 2:, :]
    middle = padded[:, :, 1:-1, :]
    return (
        -0.5 * middle[..., 1:-1]
        + 0.25 * (vertical[..., 1:-1] + middle[..., :-2] + middle[..., 2:])
        + 0.125 * (vertical[..., :-2] + vertical[..., 2:])
    )


def complex_times(coeff, field):
    real_part = coeff[:, 0] * field[:, 0] - coeff[:, 1] * field[:, 1]
    imag_part = coeff[:, 0] * field[:, 1] + coeff[:, 1] * field[:, 0]
    return jnp.stack([real_part, imag_part], axis=1)


def shards(
    incoming_wave,
    speed_class_map,
    spectral_entry_index,
    filter_weights,
    scaled_pulsations,
    inverse_speed_classes,
):
    highest = lax.Precision.HIGHEST
    summed_along = incoming_wave.shape[2]
    summed_across = incoming_wave.shape[3]
    strip_count = lax.axis_size("strip")
    lateral_count = strip_count // SECTIONS
    position = (lax.axis_index("strip") - lateral_count // 2) % strip_count
    vertical_slab = position // lateral_count
    lateral_place = position % lateral_count
    section_rows = summed_along * lateral_count
    section_cells = section_rows * summed_across
    margin = ORDER
    extended_rows = summed_along + 2 * margin
    lateral_rows = (
        lateral_place * summed_along - margin + jnp.arange(extended_rows, dtype=jnp.int32)
    )
    inside = ((lateral_rows >= 0) & (lateral_rows < section_rows)).astype(jnp.float32)[
        None, None, :, None
    ]

    def mcclellan_step(field):
        padded = jnp.pad(field, ((0, 0), (0, 0), (1, 1), (0, 0)))
        padded = jnp.pad(padded, ((0, 0), (0, 0), (0, 0), (1, 1)))
        result = stencil_padded(padded)
        result = result * inside
        return result

    def interior(field):
        return field[:, :, margin : margin + summed_along, :]

    def image_downward(field, batch_index):
        freq_row = lax.dynamic_index_in_dim(spectral_entry_index, batch_index, 0, keepdims=False)
        freq_select = (freq_row[:, None] == jnp.arange(NW, dtype=jnp.int32)[None, :]).astype(
            jnp.float32
        )
        freq_coeffs = jnp.einsum("fw,wbck->fbck", freq_select, filter_weights, precision=highest)
        freq_omega = jnp.dot(freq_select, scaled_pulsations, precision=highest)
        wavefield = field
        raws = []
        for level in range(LEVELS):
            cells = speed_class_map[level].reshape(-1)
            bin_onehot = (cells[None, :] == jnp.arange(NBIN, dtype=jnp.int32)[:, None]).astype(
                jnp.float32
            )
            cell_slowness = jnp.dot(inverse_speed_classes, bin_onehot, precision=highest).reshape(
                summed_along, summed_across
            )
            table = jnp.einsum("fbck,bn->kfcn", freq_coeffs, bin_onehot, precision=highest).reshape(
                ORDER + 1, NFREQ, 2, summed_along, summed_across
            )
            extended = extended_2(wavefield, (("strip", 2),), ORDER) * inside
            previous = extended
            current = mcclellan_step(extended)
            accumulated = complex_times(table[0], interior(previous)) + complex_times(
                table[1], interior(current)
            )

            def recursion_step(order_index, state_tuple):
                before, present, running = state_tuple
                following = 2.0 * mcclellan_step(present) - before
                coeff = lax.dynamic_index_in_dim(table, order_index, 0, keepdims=False)
                running = running + complex_times(coeff, interior(following))
                return (present, following, running)

            previous, current, accumulated = lax.fori_loop(
                2, ORDER + 1, recursion_step, (previous, current, accumulated)
            )
            phase_angle = freq_omega[:, None, None] * cell_slowness[None]
            cosine = jnp.cos(phase_angle)
            sine_part = jnp.sin(phase_angle)
            real_part = accumulated[:, 0] * cosine - accumulated[:, 1] * sine_part
            imag_part = accumulated[:, 0] * sine_part + accumulated[:, 1] * cosine
            wavefield = jnp.stack([real_part, imag_part], axis=1)
            raws.append(jnp.sum(real_part, axis=0))
        return (wavefield, raws)

    above_floor_lines, above_unscaled_waves = image_downward(incoming_wave, vertical_slab)
    arriving = from_behind(above_floor_lines, "strip", lateral_count)
    second_bottom, second_raws = image_downward(arriving, jnp.maximum(vertical_slab - 1, 0))
    handed = jnp.where(vertical_slab == 0, above_floor_lines, second_bottom)
    first_section = (vertical_slab > 0).astype(jnp.float32)
    totals = [
        above_unscaled_waves[level] + first_section * second_raws[level] for level in range(LEVELS)
    ]
    selector = (jnp.arange(SECTIONS, dtype=jnp.int32) == vertical_slab).astype(jnp.float32)
    images = []
    for level in range(LEVELS):
        raw_image = totals[level]
        spread = lax.psum(selector * jnp.sum(raw_image * raw_image), "strip")
        mean_square = jnp.sum(spread * selector) / section_cells
        images.append(raw_image / jnp.sqrt(mean_square + 1e-06))
    return (jnp.stack(images, axis=0), handed)


SUB = 8
LANES = 128
PAD = 5
UNROLL = 8
TOGETHER = 4
MESH = pl.DeviceIdType.MESH


def at_row(row):
    return pl.ds(pl.multiple_of(row * SUB, SUB), SUB)


def kernel(
    strip_count,
    entry_ref,
    wave_ref,
    map_ref,
    table_ref,
    image_ref,
    handed_ref,
    starts,
    work,
    bottom,
    last,
    last_in,
    wave_out,
    map_out,
    map_all,
    raw,
    raw_in,
    sum_own,
    sum_in,
    swap_sems,
    halo_sems,
    hand_sems,
    fin_sems,
    raw_sems,
    sum_sems,
):
    nfh = wave_ref.shape[0] // 2
    length = wave_ref.shape[2]
    rows = 2 * length
    blocks = wave_ref.shape[3] // LANES
    lateral = strip_count // SECTIONS
    shift = lateral // 2
    pairs = lateral // 2
    margin = ORDER
    first = PAD + margin
    me = lax.axis_index("strip")
    position = lax.rem(me + strip_count - shift, strip_count)
    section = position // lateral
    place = lax.rem(position, lateral)
    pair = place // 2
    half = lax.rem(place, 2)
    up = jnp.where(pair > 0, 1, 0)
    down = jnp.where(pair < pairs - 1, 1, 0)
    has_up = pair > 0
    has_down = pair < pairs - 1
    has_before = section > 0
    has_after = section < SECTIONS - 1
    other = 1 - half

    def device(pos):
        return {"strip": lax.rem(pos + shift + strip_count, strip_count)}

    partner = device(position + 1 - 2 * half)
    upper = device(position - 2)
    lower = device(position + 2)
    deeper = device(position + lateral)
    shallower = device(position + strip_count - lateral)

    def remote(src, dst, sems, index, target):
        return pltpu.make_async_remote_copy(
            src_ref=src,
            dst_ref=dst,
            send_sem=sems.at[(0,) + index],
            recv_sem=sems.at[(1,) + index],
            device_id=target,
            device_id_type=MESH,
        )

    def span(row, count):
        return pl.ds(pl.multiple_of(row * SUB, SUB), count * SUB)

    zero = jnp.zeros((SUB, LANES), jnp.float32)
    for edge in (first - 1, first + rows):
        for f in range(nfh):
            for c in range(2):
                for s in range(2 * LEVELS):
                    starts[s, f, c, at_row(edge), :] = zero
        for c in range(2):
            for k in range(ORDER):
                work[k, c, at_row(edge), :] = zero

    barrier = pltpu.get_barrier_semaphore()
    for d in range(1, lateral):
        mate = device(section * lateral + lax.rem(place + d, lateral))
        pl.semaphore_signal(barrier, inc=1, device_id=mate, device_id_type=MESH)
    for target in (deeper, shallower):
        pl.semaphore_signal(barrier, inc=1, device_id=target, device_id_type=MESH)

    def rearrange(load, store):
        for g in range(length // SUB):
            for j in range(blocks):
                store(g, j, load(g, j))

    def strided(row, g, j):
        return pl.ds((row + g * SUB) * SUB + j, SUB, stride=SUB)

    own_row = half * length
    swaps = []
    for f in range(nfh):
        for c in range(2):
            rearrange(
                lambda g, j: wave_ref[other * nfh + f, c, pl.ds(g * SUB, SUB), pl.ds(j * LANES, LANES)],
                lambda g, j, x: pltpu_store(wave_out.at[f, c], strided(0, g, j), x),
            )
        if f == 0:
            pl.semaphore_wait(barrier, lateral + 1)
        copy = remote(
            wave_out.at[f],
            starts.at[0, f, :, span(first + own_row, length), :],
            swap_sems,
            (f,),
            partner,
        )
        copy.start()
        swaps.append(copy)
    for l in range(LEVELS):
        rearrange(
            lambda g, j: map_ref[l, pl.ds(g * SUB, SUB), pl.ds(j * LANES, LANES)],
            lambda g, j, x: pltpu_store(map_out.at[l], strided(0, g, j), x),
        )
    copy = remote(
        map_out, map_all.at[:, span(own_row, length), :], swap_sems, (nfh,), partner
    )
    copy.start()
    swaps.append(copy)
    for f in range(nfh):
        for c in range(2):
            rearrange(
                lambda g, j: wave_ref[half * nfh + f, c, pl.ds(g * SUB, SUB), pl.ds(j * LANES, LANES)],
                lambda g, j, x: pltpu_store(
                    starts.at[0, f, c], strided(first + own_row, g, j), x
                ),
            )
    for l in range(LEVELS):
        rearrange(
            lambda g, j: map_ref[l, pl.ds(g * SUB, SUB), pl.ds(j * LANES, LANES)],
            lambda g, j, x: pltpu_store(map_all.at[l], strided(own_row, g, j), x),
        )

    def halo_up(stage, f):
        ref = starts.at[stage, f]
        return remote(
            ref.at[:, span(first, margin), :],
            ref.at[:, span(first + rows, margin), :],
            halo_sems,
            (stage, f, 0),
            upper,
        )

    def halo_down(stage, f):
        ref = starts.at[stage, f]
        return remote(
            ref.at[:, span(first + rows - margin, margin), :],
            ref.at[:, span(first - margin, margin), :],
            halo_sems,
            (stage, f, 1),
            lower,
        )

    def send_halo(stage, f):
        pl.when(has_up)(lambda: halo_up(stage, f).start())
        pl.when(has_down)(lambda: halo_down(stage, f).start())

    def wait_halo(stage, f):
        pl.when(has_down)(lambda: halo_up(stage, f).wait_recv())
        pl.when(has_up)(lambda: halo_down(stage, f).wait_recv())

    def hand_parts(f):
        parts = ((0, margin), (rows - margin, margin), (margin, rows - 2 * margin))
        return [
            remote(
                bottom.at[f, :, span(row, count), :],
                starts.at[LEVELS, f, :, span(first + row, count), :],
                hand_sems,
                (f, n),
                deeper,
            )
            for n, (row, count) in enumerate(parts)
        ]

    lane = lax.broadcasted_iota(jnp.int32, (SUB, LANES), 1)
    sub = lax.broadcasted_iota(jnp.int32, (SUB, LANES), 0)
    at_first = lane == 0
    at_last = lane == LANES - 1
    keep_first = sub > 0
    keep_last = sub < SUB - 1

    def across(u):
        right = pltpu.roll(u, 1, 1)
        right_fix = jnp.where(keep_first, pltpu.roll(right, 1, 0), 0.0)
        left = pltpu.roll(u, LANES - 1, 1)
        left_fix = jnp.where(keep_last, pltpu.roll(left, SUB - 1, 0), 0.0)
        return jnp.where(at_first, right_fix, right) + jnp.where(at_last, left_fix, left)

    def reach(k):
        return ((margin - k + UNROLL - 1) // UNROLL) * UNROLL

    def apply(k, present, before, target):
        extra = reach(k)
        low = first - up * extra
        count = (rows + (up + down) * extra) // UNROLL

        def block(i, carry):
            base = low + i * UNROLL
            v = [
                [present[c, at_row(base - 1 + n), :] for n in range(UNROLL + 2)]
                for c in range(2)
            ]
            old = None
            if before is not None:
                old = [
                    [before[c, at_row(base + n), :] for n in range(UNROLL)] for c in range(2)
                ]
            values = []
            for c in range(2):
                q = [v[c][n] + v[c][n + 1] for n in range(UNROLL + 1)]
                for n in range(UNROLL):
                    u = q[n] + q[n + 1]
                    w = across(u) + (u + u)
                    centre = v[c][n + 1]
                    if old is None:
                        value = 0.125 * w - centre
                    else:
                        value = 0.25 * w - (centre + centre + old[c][n])
                    values.append(value)
            for c in range(2):
                for n in range(UNROLL):
                    target[c, at_row(base + n), :] = values[c * UNROLL + n]
            return carry

        lax.fori_loop(0, count, block, 0)

    def unit(tick, level, f, meanwhile=None):
        stage = tick * LEVELS + level
        start = starts.at[stage, f]
        apply(1, start, None, work.at[0])
        apply(2, work.at[0], start, work.at[1])

        def step(k, carry):
            apply(k, work.at[k - 2], work.at[k - 3], work.at[k - 1])
            return carry

        lax.fori_loop(3, ORDER + 1, step, 0)
        if meanwhile is not None:
            meanwhile()
        batch = section if tick == 0 else jnp.maximum(section - 1, 0)
        entry = entry_ref[batch, half * nfh + f]

        def combine(i, carry):
            spots = [TOGETHER * i + n for n in range(TOGETHER)]
            bins = [map_all[level, at_row(r), :] for r in spots]
            real = [None] * TOGETHER
            imag = [None] * TOGETHER
            for n, r in enumerate(spots):
                for k in range(ORDER + 1):
                    cr, ci = (
                        jnp.take_along_axis(
                            jnp.broadcast_to(
                                table_ref[entry, pl.ds(2 * k + c, 1), :], (SUB, LANES)
                            ),
                            bins[n],
                            axis=1,
                            mode="promise_in_bounds",
                        )
                        for c in range(2)
                    )
                    source = start if k == 0 else work.at[k - 1]
                    tr = source[0, at_row(first + r), :]
                    ti = source[1, at_row(first + r), :]
                    re = cr * tr - ci * ti
                    im = cr * ti + ci * tr
                    real[n] = re if k == 0 else real[n] + re
                    imag[n] = im if k == 0 else imag[n] + im
            for n, r in enumerate(spots):
                re, im = real[n], imag[n]
                if tick == 0 and f == 0:
                    raw[level, at_row(r), :] = re
                else:
                    part = re if tick == 0 else jnp.where(has_before, re, 0.0)
                    raw[level, at_row(r), :] = raw[level, at_row(r), :] + part
                for c, value in enumerate((re, im)):
                    if level < LEVELS - 1:
                        starts[stage + 1, f, c, at_row(first + r), :] = value
                    elif tick == 0:
                        bottom[f, c, at_row(r), :] = value
                    else:
                        last[f, c, at_row(r), :] = jnp.where(
                            has_before, value, bottom[f, c, at_row(r), :]
                        )
            return carry

        lax.fori_loop(0, rows // TOGETHER, combine, 0)

    def finish_wave(f):
        return remote(
            last.at[f, :, span(other * length, length), :],
            last_in.at[f],
            fin_sems,
            (f,),
            partner,
        )

    def finish_raw(l):
        return remote(
            raw.at[l, span(other * length, length), :], raw_in.at[l], raw_sems, (l,), partner
        )

    for f in range(nfh):
        swaps[f].wait_recv()
        send_halo(0, f)
    swaps[nfh].wait_recv()
    for level in range(LEVELS):
        for f in range(nfh):
            wait_halo(level, f)
            unit(0, level, f)
            if level < LEVELS - 1:
                send_halo(level + 1, f)
            else:

                @pl.when(has_after)
                def _():
                    for copy in hand_parts(f):
                        copy.start()

    def forward(f):
        @pl.when(has_before)
        def _():
            high, low, mid = hand_parts(f)
            high.wait_recv()
            pl.when(has_up)(lambda: halo_up(LEVELS, f).start())
            low.wait_recv()
            pl.when(has_down)(lambda: halo_down(LEVELS, f).start())
            mid.wait_recv()

    def skip_or(fn):
        pl.when(has_before)(fn)

    forward(0)
    for level in range(LEVELS):
        for f in range(nfh):

            @pl.when(has_before)
            def _():
                wait_halo(LEVELS + level, f)

            later = f + 1 if level == 0 and f + 1 < nfh else None
            unit(1, level, f, None if later is None else lambda: forward(later))
            if level < LEVELS - 1:

                @pl.when(has_before)
                def _():
                    send_halo(LEVELS + level + 1, f)

            else:
                finish_wave(f).start()
        finish_raw(level).start()

    for l in range(LEVELS):
        finish_raw(l).wait_recv()

        def merge(i, carry):
            value = raw[l, at_row(own_row + i), :] + raw_in[l, at_row(i), :]
            raw_in[l, at_row(i), :] = value
            return carry + value * value

        sum_own[pl.ds(l * SUB, SUB), :] = lax.fori_loop(0, length, merge, zero)
    for d in range(1, lateral):
        mate = device(section * lateral + lax.rem(place + d, lateral))
        remote(sum_own, sum_in.at[d], sum_sems, (d,), mate).start()

    for f in range(nfh):
        for c in range(2):
            rearrange(
                lambda g, j: last[f, c, strided(own_row, g, j), :],
                lambda g, j, x: out_store(handed_ref, half * nfh + f, c, g, j, x),
            )
    for f in range(nfh):
        finish_wave(f).wait_recv()
        for c in range(2):
            rearrange(
                lambda g, j: last_in[f, c, strided(0, g, j), :],
                lambda g, j, x: out_store(handed_ref, other * nfh + f, c, g, j, x),
            )

    total = sum_own[...]
    for d in range(1, lateral):
        mate = device(section * lateral + lax.rem(place + d, lateral))
        remote(sum_own, sum_in.at[d], sum_sems, (d,), mate).wait_recv()
        total = total + sum_in[d]
    cells = length * lateral * blocks * LANES
    for l in range(LEVELS):
        mean = jnp.sum(total[l * SUB : (l + 1) * SUB], axis=(0, 1), keepdims=True) / cells
        scale = jnp.broadcast_to(1.0 / jnp.sqrt(mean + 1e-06), (SUB, LANES))

        def put(g, j, x):
            image_ref[l, pl.ds(g * SUB, SUB), pl.ds(j * LANES, LANES)] = x * scale

        rearrange(lambda g, j: raw_in[l, strided(0, g, j), :], put)

    for copy in swaps:
        copy.wait_send()
    for f in range(nfh):
        send_done = lambda make, stage: make(stage, f).wait_send()
        for stage in range(2 * LEVELS):
            live_up = has_up if stage < LEVELS else has_up & has_before
            live_down = has_down if stage < LEVELS else has_down & has_before
            pl.when(live_up)(lambda: send_done(halo_up, stage))
            pl.when(live_down)(lambda: send_done(halo_down, stage))

        @pl.when(has_after)
        def _():
            for copy in hand_parts(f):
                copy.wait_send()

        finish_wave(f).wait_send()
    for l in range(LEVELS):
        finish_raw(l).wait_send()
    for d in range(1, lateral):
        mate = device(section * lateral + lax.rem(place + d, lateral))
        remote(sum_own, sum_in.at[d], sum_sems, (d,), mate).wait_send()


def pltpu_store(ref, where, x):
    ref[where, :] = x


def out_store(ref, f, c, g, j, x):
    ref[f, c, pl.ds(g * SUB, SUB), pl.ds(j * LANES, LANES)] = x


def paired(
    incoming_wave,
    speed_class_map,
    spectral_entry_index,
    filter_weights,
    scaled_pulsations,
    inverse_speed_classes,
):
    strip_count = lax.axis_size("strip")
    lateral = strip_count // SECTIONS
    length = incoming_wave.shape[2]
    nfh = NFREQ // 2
    rows = 2 * length
    tall = (rows + 2 * ORDER + 2 * PAD) * SUB
    table = phase_table(filter_weights, scaled_pulsations, inverse_speed_classes)
    f32 = jnp.float32
    vmem = pl.BlockSpec(memory_space=pltpu.VMEM)

    def dma(*shape):
        return pltpu.SemaphoreType.DMA((2,) + shape)

    return pl.pallas_call(
        functools.partial(kernel, strip_count),
        out_shape=(
            jax.ShapeDtypeStruct(speed_class_map.shape, f32),
            jax.ShapeDtypeStruct(incoming_wave.shape, f32),
        ),
        in_specs=[pl.BlockSpec(memory_space=pltpu.SMEM), vmem, vmem, vmem],
        out_specs=(vmem, vmem),
        scratch_shapes=[
            pltpu.VMEM((2 * LEVELS, nfh, 2, tall, LANES), f32),
            pltpu.VMEM((ORDER, 2, tall, LANES), f32),
            pltpu.VMEM((nfh, 2, rows * SUB, LANES), f32),
            pltpu.VMEM((nfh, 2, rows * SUB, LANES), f32),
            pltpu.VMEM((nfh, 2, length * SUB, LANES), f32),
            pltpu.VMEM((nfh, 2, length * SUB, LANES), f32),
            pltpu.VMEM((LEVELS, length * SUB, LANES), jnp.int32),
            pltpu.VMEM((LEVELS, rows * SUB, LANES), jnp.int32),
            pltpu.VMEM((LEVELS, rows * SUB, LANES), f32),
            pltpu.VMEM((LEVELS, length * SUB, LANES), f32),
            pltpu.VMEM((LEVELS * SUB, LANES), f32),
            pltpu.VMEM((lateral, LEVELS * SUB, LANES), f32),
            dma(nfh + 1),
            dma(2 * LEVELS, nfh, 2),
            dma(nfh, 3),
            dma(nfh),
            dma(LEVELS),
            dma(lateral),
        ],
        compiler_params=pltpu.CompilerParams(
            collective_id=0, has_side_effects=True, vmem_limit_bytes=48 * 1024 * 1024
        ),
    )(spectral_entry_index, incoming_wave, speed_class_map, table)


ROWS = 2 * (ORDER + 1)
TICKS = 2


def lane_pick(x, index):
    return jnp.take_along_axis(
        x, index, axis=1, mode="promise_in_bounds", wrap_negative_indices=False
    )


def transposed(x):
    lane = lax.broadcasted_iota(jnp.int32, (SUB, LANES), 1)
    low = lane % SUB
    bits = [(step, (lane // step) % 2 == 1) for step in (1, 2, 4)]
    x = list(x)
    for step, bit in bits:
        x = [jnp.where(bit, x[(a + step) % SUB], x[a]) for a in range(SUB)]
    for a in range(1, SUB):
        x[a] = lane_pick(x[a], lane - low + (low + SUB - a) % SUB)
    x = [x[-n % SUB] for n in range(SUB)]
    for step, bit in bits:
        x = [jnp.where(bit, x[(m - step) % SUB], x[m]) for m in range(SUB)]
    return x


def chain_kernel(
    count,
    entry_ref,
    pulsation_ref,
    slowness_ref,
    weight_ref,
    wave_ref,
    map_ref,
    image_ref,
    handed_ref,
    entries,
    pulsations,
    slownesses,
    weights,
    rows,
    hop,
    starts,
    last,
    even,
    odd,
    paired_sum,
    running,
    coeffs,
    spread_table,
    wave_in,
    map_in,
    bins,
    raw,
    wave_out,
    raw_out,
    raw_in,
    sum_own,
    sum_in,
    small_sems,
    wave_sems,
    hop_sems,
    map_sems,
    relay_sems,
    fin_sems,
    raw_sems,
    sum_sems,
    own_sems,
    own_raw_sems,
):
    length = wave_ref.shape[2]
    groups = length // SUB
    lateral = count // SECTIONS
    half = lateral // 2
    me = lax.axis_index("strip")
    plane = me // lateral
    place = lax.rem(me, lateral)
    side = place // 2
    core = lax.rem(place, 2)
    chain = lax.rem(plane + SECTIONS - 1, SECTIONS)
    section = lax.rem(chain + side, SECTIONS)
    slab = lax.rem(place + half, lateral)
    home = lax.rem(section + 1, SECTIONS)
    near = side == 0
    has_next = chain < SECTIONS - 1
    is_deep = section > 0

    def wrapped(index):
        return lax.rem(index + count, count)

    def device(index):
        return {"strip": wrapped(index)}

    def worker(plane_, f):
        return wrapped(plane_ * lateral + f)

    def owner(section_, d):
        return wrapped(section_ * lateral + half + d)

    partner = device(me + 1 - 2 * core)

    def remote(src, dst, sems, index, target, arrival=None):
        return pltpu.make_async_remote_copy(
            src_ref=src,
            dst_ref=dst,
            send_sem=sems.at[(0,) + index],
            recv_sem=sems.at[(1,) + (index if arrival is None else arrival)],
            device_id=target,
            device_id_type=MESH,
        )

    barrier = pltpu.get_barrier_semaphore()
    base = (plane - 1) * lateral
    for n in range(3 * lateral):
        mate = wrapped(base + n)

        @pl.when(mate != me)
        def _():
            pl.semaphore_signal(barrier, inc=1, device_id=device(mate), device_id_type=MESH)

    small = [
        pltpu.make_async_copy(source, target, small_sems.at[n])
        for n, (source, target) in enumerate(
            (
                (entry_ref, entries),
                (pulsation_ref, pulsations),
                (slowness_ref, slownesses),
                (weight_ref, weights),
            )
        )
    ]
    for copy in small:
        copy.start()
    own_wave = pltpu.make_async_copy(wave_ref.at[place], wave_in.at[slab], own_sems.at[0])
    own_map = pltpu.make_async_copy(map_ref, map_in.at[side, slab], own_sems.at[1])
    pl.when(near)(own_wave.start)
    pl.when(near | has_next)(own_map.start)

    lane = lax.broadcasted_iota(jnp.int32, (SUB, LANES), 1)
    sub = lax.broadcasted_iota(jnp.int32, (SUB, LANES), 0)
    high_lane, low_lane = lane // SUB, lane % SUB
    to_left = jnp.where(high_lane > 0, lane - SUB, jnp.where(low_lane > 0, 119 + low_lane, 0))
    to_right = jnp.where(
        high_lane < 15, lane + SUB, jnp.where(low_lane < 7, low_lane + 1, LANES - 1)
    )
    not_first_lane = lane > 0
    not_last_lane = lane < LANES - 1
    not_first_sub = sub > 0
    not_last_sub = sub < SUB - 1

    pl.semaphore_wait(barrier, 3 * lateral - 1)

    def wave_copy(f):
        return remote(
            wave_ref.at[f],
            wave_in.at[slab],
            wave_sems,
            (f,),
            device(worker(home, f)),
            (slab,),
        )

    def wave_arrival(d):
        return remote(
            wave_ref.at[0], wave_in.at[d], wave_sems, (d,), device(owner(chain, d))
        )

    def map_copy(tick, y):
        to = worker(home if tick == 0 else section, 2 * y + core)
        copy = remote(
            map_ref,
            map_in.at[tick, slab],
            map_sems,
            (tick, y),
            device(to),
            (tick, slab // 2),
        )
        live = to != me
        return copy, live if tick == 0 else live & is_deep

    def map_arrival(tick, h):
        d = core + 2 * h
        source = owner(chain + tick, d)
        copy = remote(map_ref, map_in.at[tick, d], map_sems, (tick, h), device(source))
        return copy, source != me

    def map_relay(tick, h):
        part = map_in.at[tick, core + 2 * h]
        return remote(part, part, relay_sems, (tick, h), partner)

    def pass_map_on(tick):
        for h in range(2):
            copy, foreign = map_arrival(tick, h)
            pl.when(foreign)(copy.wait_recv)
            pl.when(jnp.logical_not(foreign))(own_map.wait)
            map_relay(tick, h).start()

    def start_map(tick):
        for y in range(2):
            copy, live = map_copy(tick, y)
            pl.when(live)(copy.start)

    far = side == 1

    def hop_in(f):
        return pltpu.make_async_remote_copy(
            src_ref=wave_ref.at[f],
            dst_ref=hop.at[f],
            send_sem=wave_sems.at[0, f],
            recv_sem=hop_sems.at[1, f],
            device_id=device(worker(plane, core)),
            device_id_type=MESH,
        )

    def hop_on(f):
        return pltpu.make_async_remote_copy(
            src_ref=hop.at[f],
            dst_ref=wave_in.at[core],
            send_sem=hop_sems.at[0, f],
            recv_sem=wave_sems.at[1, core],
            device_id=device(worker(plane + 1, f)),
            device_id_type=MESH,
        )

    start_map(0)
    for f in range(half):
        pl.when(far)(hop_in(f).start)
    for f in range(half, lateral):
        wave_copy(f).start()
    for f in range(half):
        pl.when(near & (worker(home, f) != me))(wave_copy(f).start)
    start_map(1)

    for copy in small:
        copy.wait()
    entry = entries[chain, place]
    angle = pulsations[entry] * slownesses[...]
    cosine, sine = jnp.cos(angle), jnp.sin(angle)
    for k in range(ORDER + 1):
        fr, fi = (weights[entry, k, pl.ds(c, 1), :] for c in range(2))
        rows[pl.ds(k, 1), pl.ds(0, NBIN)] = fr * cosine - fi * sine
        rows[pl.ds(ORDER + 1 + k, 1), pl.ds(0, NBIN)] = fr * sine + fi * cosine
    for n in range(ROWS):
        row = jnp.broadcast_to(rows[pl.ds(n, 1), :], (SUB, LANES))
        for part in range(NBIN // SUB):
            spread_table[part, n] = lane_pick(row, sub + part * SUB)

    @pl.when(near)
    def _():
        for f in range(half):
            hop_in(f).wait_recv()
            hop_on(f).start()


    def cell(m, r):
        return pl.ds((m * SUB + r) * SUB, SUB)

    def column(m, slot):
        return pl.ds(m * SUB * SUB + slot, SUB, stride=SUB)

    def gather_back(source, d, g):
        return transposed([source[column(m, groups * d + g), :] for m in range(SUB)])

    def tile(g, j):
        return pl.ds(g * SUB, SUB), pl.ds(j * LANES, LANES)

    def spread(load, ref, d):
        for g in range(groups):
            for m, x in enumerate(transposed([load(*tile(g, j)) for j in range(SUB)])):
                ref[column(m, groups * d + g), :] = x

    def fill(tick, level):
        for d in range(lateral):
            spread(lambda row, col: map_in[tick, d, level, row, col], bins, d)
        n_cells = 2

        def some(i, carry):
            for n in range(n_cells):
                where = pl.ds(pl.multiple_of((i * n_cells + n) * SUB, SUB), SUB)
                bin_ = bins[where, :]
                high = bin_ >= SUB
                low_bits = bin_ % SUB
                for row in range(ROWS):
                    a, b = (
                        jnp.take_along_axis(
                            spread_table[part, row],
                            low_bits,
                            axis=0,
                            mode="promise_in_bounds",
                            wrap_negative_indices=False,
                        )
                        for part in range(NBIN // SUB)
                    )
                    coeffs[level, row, where, :] = jnp.where(high, b, a)
            return carry

        lax.fori_loop(0, SUB * SUB // n_cells, some, 0)

    def stencil(present, target, first=False, last=False):
        def channel(c, carry):
            below = []
            for m in range(8):
                edge = pltpu.roll(present[c, cell(m, 7), :], 1, 0)
                edge = jnp.where(not_first_sub, edge, 0.0)
                below.append(edge + present[c, cell(m, 0), :])
            for r in range(8):
                u = []
                for m in range(8):
                    here = present[c, cell(m, r), :]
                    if r < 7:
                        above = present[c, cell(m, r + 1), :]
                    else:
                        above = pltpu.roll(present[c, cell(m, 0), :], SUB - 1, 0)
                        above = jnp.where(not_last_sub, above, 0.0)
                    q = here + above
                    u.append(below[m] + q)
                    below[m] = q
                left = jnp.where(not_first_lane, lane_pick(u[7], to_left), 0.0)
                right = jnp.where(not_last_lane, lane_pick(u[0], to_right), 0.0)
                u = [left] + u + [right]
                h = [u[m] + u[m + 1] for m in range(9)]
                for m in range(8):
                    w = h[m] + h[m + 1]
                    here = present[c, cell(m, r), :]
                    if first:
                        both = 0.125 * w
                    else:
                        both = 0.25 * w - paired_sum[c, cell(m, r), :]
                    if not last:
                        paired_sum[c, cell(m, r), :] = both
                    target[c, cell(m, r), :] = both - here
            return carry

        lax.fori_loop(0, 2, channel, 0)

    def add_orders(tick, level, terms, where, total):
        re, im = (None, None) if total is None else total
        for order, ref in terms:
            tr, ti = (ref[c, where, :] for c in range(2))
            br = coeffs[level, order, where, :]
            bi = coeffs[level, ORDER + 1 + order, where, :]
            dr = br * tr - bi * ti
            di = br * ti + bi * tr
            re, im = (dr, di) if re is None else (re + dr, im + di)
        return re, im

    def sum_so_far(where):
        return [running[c, where, :] for c in range(2)]

    def unit(tick, level, output):
        start = starts.at[tick * LEVELS + level]
        stencil(start, odd, first=True)
        for i in range(SUB * SUB):
            where = pl.ds(i * SUB, SUB)
            total = add_orders(tick, level, [(0, start), (1, odd)], where, None)
            for c in range(2):
                running[c, where, :] = total[c]

        def steps(i, carry):
            stencil(odd, even)
            stencil(even, odd)
            for n in range(SUB * SUB):
                where = pl.ds(n * SUB, SUB)
                terms = [(2 * i + 2, even), (2 * i + 3, odd)]
                total = add_orders(tick, level, terms, where, sum_so_far(where))
                for c in range(2):
                    running[c, where, :] = total[c]
            return carry

        lax.fori_loop(0, ORDER // 2 - 1, steps, 0)
        stencil(odd, even, last=True)
        for i in range(SUB * SUB):
            where = pl.ds(i * SUB, SUB)
            total = add_orders(tick, level, [(ORDER, even)], where, sum_so_far(where))
            for c in range(2):
                output[c, where, :] = total[c]
            raw[tick, level, where, :] = total[0]

    def raw_copy(tick, level, d):
        to = owner(chain + tick, d)
        copy = remote(
            raw_out.at[tick, level, d],
            raw_in.at[tick, level, place],
            raw_sems,
            (tick, level, d),
            device(to),
            (tick, level, place),
        )
        return copy, to != me

    def own_raw(tick, level):
        return pltpu.make_async_copy(
            raw_out.at[tick, level, slab],
            raw_in.at[tick, level, place],
            own_raw_sems.at[tick, level],
        )

    def raw_arrival(tick, level, f):
        source = worker(home if tick == 0 else section, f)
        copy = remote(
            raw_out.at[tick, level, f],
            raw_in.at[tick, level, f],
            raw_sems,
            (tick, level, f),
            device(source),
        )
        return copy, source != me

    def send_raw(tick, level):
        for d in range(lateral):
            for g in range(groups):
                for j, x in enumerate(gather_back(raw.at[tick, level], d, g)):
                    raw_out[(tick, level, d) + tile(g, j)] = x
            copy, foreign = raw_copy(tick, level, d)
            pl.when(foreign)(copy.start)
            pl.when(jnp.logical_not(foreign))(own_raw(tick, level).start)

    def wave_back(which, d):
        to = owner(chain + which, d)
        copy = remote(
            wave_out.at[which, d],
            handed_ref.at[place],
            fin_sems,
            (which, d),
            device(to),
            (1, place),
        )
        return copy, to != me

    def own_back(which):
        return pltpu.make_async_copy(
            wave_out.at[which, slab], handed_ref.at[place], own_sems.at[0]
        )

    def handed_arrival(f):
        source = worker(jnp.maximum(section, 1), f)
        copy = remote(
            wave_out.at[1, f], handed_ref.at[f], fin_sems, (1, f), device(source)
        )
        return copy, source != me

    def send_wave(which, source):
        for d in range(lateral):
            for c in range(2):
                for g in range(groups):
                    for j, x in enumerate(gather_back(source.at[c], d, g)):
                        wave_out[(which, d, c) + tile(g, j)] = x
            copy, foreign = wave_back(which, d)
            pl.when(foreign)(copy.start)
            pl.when(jnp.logical_not(foreign))(own_back(which).start)

    pass_map_on(0)
    for h in range(2):
        map_relay(0, h).wait_recv()
    fill(0, 0)
    fill(0, 1)
    def take_waves(order):
        for d in order:
            foreign = owner(chain, d) != me
            pl.when(foreign)(wave_arrival(d).wait_recv)
            pl.when(jnp.logical_not(foreign))(own_wave.wait)
            for c in range(2):
                spread(lambda row, col: wave_in[d, c, row, col], starts.at[0, c], d)

    pl.when(near)(lambda: take_waves((2, 3, 0, 1)))
    pl.when(far)(lambda: take_waves((0, 1, 2, 3)))
    unit(0, 0, starts.at[1])
    pl.when(has_next)(lambda: pass_map_on(1))
    send_raw(0, 0)
    unit(0, 1, starts.at[2])
    send_raw(0, 1)

    @pl.when(chain == 0)
    def _():
        send_wave(0, starts.at[2])

    @pl.when(has_next)
    def _():
        for h in range(2):
            map_relay(1, h).wait_recv()
        fill(1, 0)
        fill(1, 1)
        unit(1, 0, starts.at[3])
        send_raw(1, 0)
        unit(1, 1, last)
        send_raw(1, 1)
        send_wave(1, last)

    for level in range(LEVELS):
        for tick in range(TICKS):
            for f in range(lateral):
                copy, foreign = raw_arrival(tick, level, f)
                own = jnp.logical_not(foreign)
                if tick == 1:
                    foreign, own = foreign & is_deep, own & is_deep
                pl.when(foreign)(copy.wait_recv)
                pl.when(own)(own_raw(tick, level).wait)
        total = jnp.zeros((SUB, LANES), jnp.float32)
        for g in range(groups):
            for j in range(SUB):
                value = second = None
                for f in range(lateral):
                    a, b = (raw_in[(t, level, f) + tile(g, j)] for t in range(TICKS))
                    value = a if value is None else value + a
                    second = b if second is None else second + b
                value = value + jnp.where(is_deep, second, 0.0)
                image_ref[(level,) + tile(g, j)] = value
                total = total + value * value
        sum_own[pl.ds(level * SUB, SUB), :] = total

    def sum_copy(x):
        mate = lax.rem(slab + x, lateral)
        return remote(sum_own, sum_in.at[x], sum_sems, (x,), device(owner(section, mate)))

    for x in range(1, lateral):
        sum_copy(x).start()
    total = sum_own[...]
    for x in range(1, lateral):
        sum_copy(x).wait_recv()
        total = total + sum_in[x]
    cells = length * lateral * SUB * LANES
    for level in range(LEVELS):
        mean = (
            jnp.sum(total[level * SUB : (level + 1) * SUB], axis=(0, 1), keepdims=True) / cells
        )
        scale = jnp.broadcast_to(1.0 / jnp.sqrt(mean + 1e-06), (SUB, LANES))
        for g in range(groups):
            for j in range(SUB):
                where = (level,) + tile(g, j)
                image_ref[where] = image_ref[where] * scale
    for f in range(lateral):
        copy, foreign = handed_arrival(f)
        pl.when(foreign)(copy.wait_recv)
        pl.when(jnp.logical_not(foreign))(own_back(0).wait)
    for x in range(1, lateral):
        sum_copy(x).wait_send()
    for tick in range(TICKS):
        for y in range(2):
            copy, live = map_copy(tick, y)
            pl.when(live)(copy.wait_send)
    for h in range(2):
        map_relay(0, h).wait_send()
        pl.when(has_next)(map_relay(1, h).wait_send)
    for n in range(lateral):
        pl.when(worker(home, n) != me)(wave_copy(n).wait_send)
        if n < half:
            pl.when(near)(hop_on(n).wait_send)
        for which, live in ((0, chain == 0), (1, has_next)):
            copy, foreign = wave_back(which, n)
            pl.when(foreign & live)(copy.wait_send)
        for level in range(LEVELS):
            for tick in range(TICKS):
                copy, foreign = raw_copy(tick, level, n)
                pl.when(foreign if tick == 0 else foreign & has_next)(copy.wait_send)


def phase_table(filter_weights, scaled_pulsations, inverse_speed_classes):
    angle = scaled_pulsations[:, None] * inverse_speed_classes[None, :]
    cosine = jnp.cos(angle)[:, None, :]
    sine = jnp.sin(angle)[:, None, :]
    by_order = jnp.transpose(filter_weights, (2, 0, 3, 1))
    real = by_order[0] * cosine - by_order[1] * sine
    imag = by_order[0] * sine + by_order[1] * cosine
    table = jnp.stack([real, imag], axis=2).reshape(NW, 2 * (ORDER + 1), NBIN)
    return jnp.pad(table, ((0, 0), (0, 0), (0, LANES - NBIN)))


def chains(
    incoming_wave,
    speed_class_map,
    spectral_entry_index,
    filter_weights,
    scaled_pulsations,
    inverse_speed_classes,
):
    count = lax.axis_size("strip")
    lateral = count // SECTIONS
    length, across = incoming_wave.shape[2:]
    tall = length * lateral * SUB
    f32 = jnp.float32
    vmem = pl.BlockSpec(memory_space=pltpu.VMEM)
    anywhere = pl.BlockSpec(memory_space=pltpu.HBM)
    def dma(*shape):
        return pltpu.SemaphoreType.DMA((2,) + shape)

    return pl.pallas_call(
        functools.partial(chain_kernel, count),
        out_shape=(
            jax.ShapeDtypeStruct(speed_class_map.shape, f32),
            jax.ShapeDtypeStruct(incoming_wave.shape, f32),
        ),
        in_specs=[anywhere] * 6,
        out_specs=(vmem, vmem),
        scratch_shapes=[
            pltpu.SMEM(spectral_entry_index.shape, jnp.int32),
            pltpu.SMEM((NW,), f32),
            pltpu.VMEM((1, NBIN), f32),
            pltpu.VMEM((NW, ORDER + 1, 2, NBIN), f32),
            pltpu.VMEM((ROWS, LANES), f32),
            pltpu.VMEM((lateral // 2, 2, length, across), f32),
            pltpu.VMEM((TICKS * LEVELS, 2, tall, LANES), f32),
            pltpu.VMEM((2, tall, LANES), f32),
            pltpu.VMEM((2, tall, LANES), f32),
            pltpu.VMEM((2, tall, LANES), f32),
            pltpu.VMEM((2, tall, LANES), f32),
            pltpu.VMEM((2, tall, LANES), f32),
            pltpu.VMEM((LEVELS, ROWS, tall, LANES), f32),
            pltpu.VMEM((NBIN // SUB, ROWS, SUB, LANES), f32),
            pltpu.VMEM((lateral, 2, length, across), f32),
            pltpu.VMEM((TICKS, lateral, LEVELS, length, across), jnp.int32),
            pltpu.VMEM((tall, LANES), jnp.int32),
            pltpu.VMEM((TICKS, LEVELS, tall, LANES), f32),
            pltpu.VMEM((2, lateral, 2, length, across), f32),
            pltpu.VMEM((TICKS, LEVELS, lateral, length, across), f32),
            pltpu.VMEM((TICKS, LEVELS, lateral, length, across), f32),
            pltpu.VMEM((LEVELS * SUB, LANES), f32),
            pltpu.VMEM((lateral, LEVELS * SUB, LANES), f32),
            pltpu.SemaphoreType.DMA((4,)),
            dma(lateral),
            dma(lateral // 2),
            dma(TICKS, 2),
            dma(TICKS, 2),
            dma(2, lateral),
            dma(TICKS, LEVELS, lateral),
            dma(lateral),
            pltpu.SemaphoreType.DMA((2,)),
            pltpu.SemaphoreType.DMA((TICKS, LEVELS)),
        ],
        compiler_params=pltpu.CompilerParams(
            collective_id=0, has_side_effects=True, vmem_limit_bytes=32 * 1024 * 1024
        ),
    )(
        spectral_entry_index,
        scaled_pulsations,
        inverse_speed_classes[None],
        jnp.transpose(filter_weights, (0, 3, 2, 1)),
        incoming_wave,
        speed_class_map,
    )


def fits(mesh):
    lateral = mesh.shape["strip"] // SECTIONS
    return NFREQ % 2 == 0 and lateral % 4 == 0


def whole_section(mesh, wave):
    lateral = mesh.shape["strip"] // SECTIONS
    full = lateral * wave.shape[2] == SUB * SUB and wave.shape[3] == SUB * LANES
    return lateral == NFREQ == 4 and wave.shape[2] % SUB == 0 and full


def body_for(mesh):
    def body(wave, *rest):
        whole = wave.shape[3] == SUB * LANES and wave.shape[2] % SUB == 0
        if whole_section(mesh, wave):
            return chains(wave, *rest)
        if fits(mesh) and whole and wave.shape[2] >= ORDER:
            return paired(wave, *rest)
        return shards(wave, *rest)

    return body


def solution(mesh):
    return jax.shard_map(
        body_for(mesh),
        mesh=mesh,
        in_specs=(
            P("groups", None, "strip", None),
            P("groups", "strip", None),
            P("groups", None),
            P(),
            P(),
            P(),
        ),
        out_specs=(P("groups", "strip", None), P("groups", None, "strip", None)),
        check_vma=False,
    )
```

```python
import functools
import jax
import jax.numpy as jnp
from jax import lax
from jax.experimental import pallas as pl
from jax.experimental.pallas import tpu as pltpu
from jax.sharding import PartitionSpec as P

SECTIONS = 4
LEVELS = 2
ORDER = 12
NFREQ = 4
NBIN = 16
NW = 16


def extended_2(shard, sides, width):
    for axis, dim in sides:
        devices, length = (lax.axis_size(axis), shard.shape[dim])
        up = [(i, (i + 1) % devices) for i in range(devices)]
        down = [(j, i) for i, j in up]
        last = lax.slice_in_dim(shard, length - width, length, axis=dim)
        initial = lax.slice_in_dim(shard, 0, width, axis=dim)
        before = lax.ppermute(last, axis, up)
        after = lax.ppermute(initial, axis, down)
        shard = jnp.concatenate([before, shard, after], axis=dim)
    return shard


def from_behind(shard, axis, by):
    devices = lax.axis_size(axis)
    return lax.ppermute(shard, axis, [(i, (i + by) % devices) for i in range(devices)])


def stencil_padded(padded):
    vertical = padded[:, :, :-2, :] + padded[:, :, 2:, :]
    middle = padded[:, :, 1:-1, :]
    return (
        -0.5 * middle[..., 1:-1]
        + 0.25 * (vertical[..., 1:-1] + middle[..., :-2] + middle[..., 2:])
        + 0.125 * (vertical[..., :-2] + vertical[..., 2:])
    )


def complex_times(coeff, field):
    real_part = coeff[:, 0] * field[:, 0] - coeff[:, 1] * field[:, 1]
    imag_part = coeff[:, 0] * field[:, 1] + coeff[:, 1] * field[:, 0]
    return jnp.stack([real_part, imag_part], axis=1)


def shards(
    incoming_wave,
    speed_class_map,
    spectral_entry_index,
    filter_weights,
    scaled_pulsations,
    inverse_speed_classes,
):
    highest = lax.Precision.HIGHEST
    summed_along = incoming_wave.shape[2]
    summed_across = incoming_wave.shape[3]
    strip_count = lax.axis_size("strip")
    lateral_count = strip_count // SECTIONS
    position = (lax.axis_index("strip") - lateral_count // 2) % strip_count
    vertical_slab = position // lateral_count
    lateral_place = position % lateral_count
    section_rows = summed_along * lateral_count
    section_cells = section_rows * summed_across
    margin = ORDER
    extended_rows = summed_along + 2 * margin
    lateral_rows = (
        lateral_place * summed_along - margin + jnp.arange(extended_rows, dtype=jnp.int32)
    )
    inside = ((lateral_rows >= 0) & (lateral_rows < section_rows)).astype(jnp.float32)[
        None, None, :, None
    ]

    def mcclellan_step(field):
        padded = jnp.pad(field, ((0, 0), (0, 0), (1, 1), (0, 0)))
        padded = jnp.pad(padded, ((0, 0), (0, 0), (0, 0), (1, 1)))
        result = stencil_padded(padded)
        result = result * inside
        return result

    def interior(field):
        return field[:, :, margin : margin + summed_along, :]

    def image_downward(field, batch_index):
        freq_row = lax.dynamic_index_in_dim(spectral_entry_index, batch_index, 0, keepdims=False)
        freq_select = (freq_row[:, None] == jnp.arange(NW, dtype=jnp.int32)[None, :]).astype(
            jnp.float32
        )
        freq_coeffs = jnp.einsum("fw,wbck->fbck", freq_select, filter_weights, precision=highest)
        freq_omega = jnp.dot(freq_select, scaled_pulsations, precision=highest)
        wavefield = field
        raws = []
        for level in range(LEVELS):
            cells = speed_class_map[level].reshape(-1)
            bin_onehot = (cells[None, :] == jnp.arange(NBIN, dtype=jnp.int32)[:, None]).astype(
                jnp.float32
            )
            cell_slowness = jnp.dot(inverse_speed_classes, bin_onehot, precision=highest).reshape(
                summed_along, summed_across
            )
            table = jnp.einsum("fbck,bn->kfcn", freq_coeffs, bin_onehot, precision=highest).reshape(
                ORDER + 1, NFREQ, 2, summed_along, summed_across
            )
            extended = extended_2(wavefield, (("strip", 2),), ORDER) * inside
            previous = extended
            current = mcclellan_step(extended)
            accumulated = complex_times(table[0], interior(previous)) + complex_times(
                table[1], interior(current)
            )

            def recursion_step(order_index, state_tuple):
                before, present, running = state_tuple
                following = 2.0 * mcclellan_step(present) - before
                coeff = lax.dynamic_index_in_dim(table, order_index, 0, keepdims=False)
                running = running + complex_times(coeff, interior(following))
                return (present, following, running)

            previous, current, accumulated = lax.fori_loop(
                2, ORDER + 1, recursion_step, (previous, current, accumulated)
            )
            phase_angle = freq_omega[:, None, None] * cell_slowness[None]
            cosine = jnp.cos(phase_angle)
            sine_part = jnp.sin(phase_angle)
            real_part = accumulated[:, 0] * cosine - accumulated[:, 1] * sine_part
            imag_part = accumulated[:, 0] * sine_part + accumulated[:, 1] * cosine
            wavefield = jnp.stack([real_part, imag_part], axis=1)
            raws.append(jnp.sum(real_part, axis=0))
        return (wavefield, raws)

    above_floor_lines, above_unscaled_waves = image_downward(incoming_wave, vertical_slab)
    arriving = from_behind(above_floor_lines, "strip", lateral_count)
    second_bottom, second_raws = image_downward(arriving, jnp.maximum(vertical_slab - 1, 0))
    handed = jnp.where(vertical_slab == 0, above_floor_lines, second_bottom)
    first_section = (vertical_slab > 0).astype(jnp.float32)
    totals = [
        above_unscaled_waves[level] + first_section * second_raws[level] for level in range(LEVELS)
    ]
    selector = (jnp.arange(SECTIONS, dtype=jnp.int32) == vertical_slab).astype(jnp.float32)
    images = []
    for level in range(LEVELS):
        raw_image = totals[level]
        spread = lax.psum(selector * jnp.sum(raw_image * raw_image), "strip")
        mean_square = jnp.sum(spread * selector) / section_cells
        images.append(raw_image / jnp.sqrt(mean_square + 1e-06))
    return (jnp.stack(images, axis=0), handed)


SUB = 8
LANES = 128
PAD = 5
UNROLL = 8
TOGETHER = 4
MESH = pl.DeviceIdType.MESH


def at_row(row):
    return pl.ds(pl.multiple_of(row * SUB, SUB), SUB)


def kernel(
    strip_count,
    entry_ref,
    wave_ref,
    map_ref,
    table_ref,
    image_ref,
    handed_ref,
    starts,
    work,
    bottom,
    last,
    last_in,
    wave_out,
    map_out,
    map_all,
    raw,
    raw_in,
    sum_own,
    sum_in,
    swap_sems,
    halo_sems,
    hand_sems,
    fin_sems,
    raw_sems,
    sum_sems,
):
    nfh = wave_ref.shape[0] // 2
    length = wave_ref.shape[2]
    rows = 2 * length
    blocks = wave_ref.shape[3] // LANES
    lateral = strip_count // SECTIONS
    shift = lateral // 2
    pairs = lateral // 2
    margin = ORDER
    first = PAD + margin
    me = lax.axis_index("strip")
    position = lax.rem(me + strip_count - shift, strip_count)
    section = position // lateral
    place = lax.rem(position, lateral)
    pair = place // 2
    half = lax.rem(place, 2)
    up = jnp.where(pair > 0, 1, 0)
    down = jnp.where(pair < pairs - 1, 1, 0)
    has_up = pair > 0
    has_down = pair < pairs - 1
    has_before = section > 0
    has_after = section < SECTIONS - 1
    other = 1 - half

    def device(pos):
        return {"strip": lax.rem(pos + shift + strip_count, strip_count)}

    partner = device(position + 1 - 2 * half)
    upper = device(position - 2)
    lower = device(position + 2)
    deeper = device(position + lateral)
    shallower = device(position + strip_count - lateral)

    def remote(src, dst, sems, index, target):
        return pltpu.make_async_remote_copy(
            src_ref=src,
            dst_ref=dst,
            send_sem=sems.at[(0,) + index],
            recv_sem=sems.at[(1,) + index],
            device_id=target,
            device_id_type=MESH,
        )

    def span(row, count):
        return pl.ds(pl.multiple_of(row * SUB, SUB), count * SUB)

    zero = jnp.zeros((SUB, LANES), jnp.float32)
    for edge in (first - 1, first + rows):
        for f in range(nfh):
            for c in range(2):
                for s in range(2 * LEVELS):
                    starts[s, f, c, at_row(edge), :] = zero
        for c in range(2):
            for k in range(ORDER):
                work[k, c, at_row(edge), :] = zero

    barrier = pltpu.get_barrier_semaphore()
    for d in range(1, lateral):
        mate = device(section * lateral + lax.rem(place + d, lateral))
        pl.semaphore_signal(barrier, inc=1, device_id=mate, device_id_type=MESH)
    for target in (deeper, shallower):
        pl.semaphore_signal(barrier, inc=1, device_id=target, device_id_type=MESH)

    def rearrange(load, store):
        for g in range(length // SUB):
            for j in range(blocks):
                store(g, j, load(g, j))

    def strided(row, g, j):
        return pl.ds((row + g * SUB) * SUB + j, SUB, stride=SUB)

    own_row = half * length
    swaps = []
    for f in range(nfh):
        for c in range(2):
            rearrange(
                lambda g, j: wave_ref[other * nfh + f, c, pl.ds(g * SUB, SUB), pl.ds(j * LANES, LANES)],
                lambda g, j, x: pltpu_store(wave_out.at[f, c], strided(0, g, j), x),
            )
        if f == 0:
            pl.semaphore_wait(barrier, lateral + 1)
        copy = remote(
            wave_out.at[f],
            starts.at[0, f, :, span(first + own_row, length), :],
            swap_sems,
            (f,),
            partner,
        )
        copy.start()
        swaps.append(copy)
    for l in range(LEVELS):
        rearrange(
            lambda g, j: map_ref[l, pl.ds(g * SUB, SUB), pl.ds(j * LANES, LANES)],
            lambda g, j, x: pltpu_store(map_out.at[l], strided(0, g, j), x),
        )
    copy = remote(
        map_out, map_all.at[:, span(own_row, length), :], swap_sems, (nfh,), partner
    )
    copy.start()
    swaps.append(copy)
    for f in range(nfh):
        for c in range(2):
            rearrange(
                lambda g, j: wave_ref[half * nfh + f, c, pl.ds(g * SUB, SUB), pl.ds(j * LANES, LANES)],
                lambda g, j, x: pltpu_store(
                    starts.at[0, f, c], strided(first + own_row, g, j), x
                ),
            )
    for l in range(LEVELS):
        rearrange(
            lambda g, j: map_ref[l, pl.ds(g * SUB, SUB), pl.ds(j * LANES, LANES)],
            lambda g, j, x: pltpu_store(map_all.at[l], strided(own_row, g, j), x),
        )

    def halo_up(stage, f):
        ref = starts.at[stage, f]
        return remote(
            ref.at[:, span(first, margin), :],
            ref.at[:, span(first + rows, margin), :],
            halo_sems,
            (stage, f, 0),
            upper,
        )

    def halo_down(stage, f):
        ref = starts.at[stage, f]
        return remote(
            ref.at[:, span(first + rows - margin, margin), :],
            ref.at[:, span(first - margin, margin), :],
            halo_sems,
            (stage, f, 1),
            lower,
        )

    def send_halo(stage, f):
        pl.when(has_up)(lambda: halo_up(stage, f).start())
        pl.when(has_down)(lambda: halo_down(stage, f).start())

    def wait_halo(stage, f):
        pl.when(has_down)(lambda: halo_up(stage, f).wait_recv())
        pl.when(has_up)(lambda: halo_down(stage, f).wait_recv())

    def hand_parts(f):
        parts = ((0, margin), (rows - margin, margin), (margin, rows - 2 * margin))
        return [
            remote(
                bottom.at[f, :, span(row, count), :],
                starts.at[LEVELS, f, :, span(first + row, count), :],
                hand_sems,
                (f, n),
                deeper,
            )
            for n, (row, count) in enumerate(parts)
        ]

    lane = lax.broadcasted_iota(jnp.int32, (SUB, LANES), 1)
    sub = lax.broadcasted_iota(jnp.int32, (SUB, LANES), 0)
    at_first = lane == 0
    at_last = lane == LANES - 1
    keep_first = sub > 0
    keep_last = sub < SUB - 1

    def across(u):
        right = pltpu.roll(u, 1, 1)
        right_fix = jnp.where(keep_first, pltpu.roll(right, 1, 0), 0.0)
        left = pltpu.roll(u, LANES - 1, 1)
        left_fix = jnp.where(keep_last, pltpu.roll(left, SUB - 1, 0), 0.0)
        return jnp.where(at_first, right_fix, right) + jnp.where(at_last, left_fix, left)

    def reach(k):
        return ((margin - k + UNROLL - 1) // UNROLL) * UNROLL

    def apply(k, present, before, target):
        extra = reach(k)
        low = first - up * extra
        count = (rows + (up + down) * extra) // UNROLL

        def block(i, carry):
            base = low + i * UNROLL
            v = [
                [present[c, at_row(base - 1 + n), :] for n in range(UNROLL + 2)]
                for c in range(2)
            ]
            old = None
            if before is not None:
                old = [
                    [before[c, at_row(base + n), :] for n in range(UNROLL)] for c in range(2)
                ]
            values = []
            for c in range(2):
                q = [v[c][n] + v[c][n + 1] for n in range(UNROLL + 1)]
                for n in range(UNROLL):
                    u = q[n] + q[n + 1]
                    w = across(u) + (u + u)
                    centre = v[c][n + 1]
                    if old is None:
                        value = 0.125 * w - centre
                    else:
                        value = 0.25 * w - (centre + centre + old[c][n])
                    values.append(value)
            for c in range(2):
                for n in range(UNROLL):
                    target[c, at_row(base + n), :] = values[c * UNROLL + n]
            return carry

        lax.fori_loop(0, count, block, 0)

    def unit(tick, level, f, meanwhile=None):
        stage = tick * LEVELS + level
        start = starts.at[stage, f]
        apply(1, start, None, work.at[0])
        apply(2, work.at[0], start, work.at[1])

        def step(k, carry):
            apply(k, work.at[k - 2], work.at[k - 3], work.at[k - 1])
            return carry

        lax.fori_loop(3, ORDER + 1, step, 0)
        if meanwhile is not None:
            meanwhile()
        batch = section if tick == 0 else jnp.maximum(section - 1, 0)
        entry = entry_ref[batch, half * nfh + f]

        def combine(i, carry):
            spots = [TOGETHER * i + n for n in range(TOGETHER)]
            bins = [map_all[level, at_row(r), :] for r in spots]
            real = [None] * TOGETHER
            imag = [None] * TOGETHER
            for n, r in enumerate(spots):
                for k in range(ORDER + 1):
                    cr, ci = (
                        jnp.take_along_axis(
                            jnp.broadcast_to(
                                table_ref[entry, pl.ds(2 * k + c, 1), :], (SUB, LANES)
                            ),
                            bins[n],
                            axis=1,
                            mode="promise_in_bounds",
                        )
                        for c in range(2)
                    )
                    source = start if k == 0 else work.at[k - 1]
                    tr = source[0, at_row(first + r), :]
                    ti = source[1, at_row(first + r), :]
                    re = cr * tr - ci * ti
                    im = cr * ti + ci * tr
                    real[n] = re if k == 0 else real[n] + re
                    imag[n] = im if k == 0 else imag[n] + im
            for n, r in enumerate(spots):
                re, im = real[n], imag[n]
                if tick == 0 and f == 0:
                    raw[level, at_row(r), :] = re
                else:
                    part = re if tick == 0 else jnp.where(has_before, re, 0.0)
                    raw[level, at_row(r), :] = raw[level, at_row(r), :] + part
                for c, value in enumerate((re, im)):
                    if level < LEVELS - 1:
                        starts[stage + 1, f, c, at_row(first + r), :] = value
                    elif tick == 0:
                        bottom[f, c, at_row(r), :] = value
                    else:
                        last[f, c, at_row(r), :] = jnp.where(
                            has_before, value, bottom[f, c, at_row(r), :]
                        )
            return carry

        lax.fori_loop(0, rows // TOGETHER, combine, 0)

    def finish_wave(f):
        return remote(
            last.at[f, :, span(other * length, length), :],
            last_in.at[f],
            fin_sems,
            (f,),
            partner,
        )

    def finish_raw(l):
        return remote(
            raw.at[l, span(other * length, length), :], raw_in.at[l], raw_sems, (l,), partner
        )

    for f in range(nfh):
        swaps[f].wait_recv()
        send_halo(0, f)
    swaps[nfh].wait_recv()
    for level in range(LEVELS):
        for f in range(nfh):
            wait_halo(level, f)
            unit(0, level, f)
            if level < LEVELS - 1:
                send_halo(level + 1, f)
            else:

                @pl.when(has_after)
                def _():
                    for copy in hand_parts(f):
                        copy.start()

    def forward(f):
        @pl.when(has_before)
        def _():
            high, low, mid = hand_parts(f)
            high.wait_recv()
            pl.when(has_up)(lambda: halo_up(LEVELS, f).start())
            low.wait_recv()
            pl.when(has_down)(lambda: halo_down(LEVELS, f).start())
            mid.wait_recv()

    def skip_or(fn):
        pl.when(has_before)(fn)

    forward(0)
    for level in range(LEVELS):
        for f in range(nfh):

            @pl.when(has_before)
            def _():
                wait_halo(LEVELS + level, f)

            later = f + 1 if level == 0 and f + 1 < nfh else None
            unit(1, level, f, None if later is None else lambda: forward(later))
            if level < LEVELS - 1:

                @pl.when(has_before)
                def _():
                    send_halo(LEVELS + level + 1, f)

            else:
                finish_wave(f).start()
        finish_raw(level).start()

    for l in range(LEVELS):
        finish_raw(l).wait_recv()

        def merge(i, carry):
            value = raw[l, at_row(own_row + i), :] + raw_in[l, at_row(i), :]
            raw_in[l, at_row(i), :] = value
            return carry + value * value

        sum_own[pl.ds(l * SUB, SUB), :] = lax.fori_loop(0, length, merge, zero)
    for d in range(1, lateral):
        mate = device(section * lateral + lax.rem(place + d, lateral))
        remote(sum_own, sum_in.at[d], sum_sems, (d,), mate).start()

    for f in range(nfh):
        for c in range(2):
            rearrange(
                lambda g, j: last[f, c, strided(own_row, g, j), :],
                lambda g, j, x: out_store(handed_ref, half * nfh + f, c, g, j, x),
            )
    for f in range(nfh):
        finish_wave(f).wait_recv()
        for c in range(2):
            rearrange(
                lambda g, j: last_in[f, c, strided(0, g, j), :],
                lambda g, j, x: out_store(handed_ref, other * nfh + f, c, g, j, x),
            )

    total = sum_own[...]
    for d in range(1, lateral):
        mate = device(section * lateral + lax.rem(place + d, lateral))
        remote(sum_own, sum_in.at[d], sum_sems, (d,), mate).wait_recv()
        total = total + sum_in[d]
    cells = length * lateral * blocks * LANES
    for l in range(LEVELS):
        mean = jnp.sum(total[l * SUB : (l + 1) * SUB], axis=(0, 1), keepdims=True) / cells
        scale = jnp.broadcast_to(1.0 / jnp.sqrt(mean + 1e-06), (SUB, LANES))

        def put(g, j, x):
            image_ref[l, pl.ds(g * SUB, SUB), pl.ds(j * LANES, LANES)] = x * scale

        rearrange(lambda g, j: raw_in[l, strided(0, g, j), :], put)

    for copy in swaps:
        copy.wait_send()
    for f in range(nfh):
        send_done = lambda make, stage: make(stage, f).wait_send()
        for stage in range(2 * LEVELS):
            live_up = has_up if stage < LEVELS else has_up & has_before
            live_down = has_down if stage < LEVELS else has_down & has_before
            pl.when(live_up)(lambda: send_done(halo_up, stage))
            pl.when(live_down)(lambda: send_done(halo_down, stage))

        @pl.when(has_after)
        def _():
            for copy in hand_parts(f):
                copy.wait_send()

        finish_wave(f).wait_send()
    for l in range(LEVELS):
        finish_raw(l).wait_send()
    for d in range(1, lateral):
        mate = device(section * lateral + lax.rem(place + d, lateral))
        remote(sum_own, sum_in.at[d], sum_sems, (d,), mate).wait_send()


def pltpu_store(ref, where, x):
    ref[where, :] = x


def out_store(ref, f, c, g, j, x):
    ref[f, c, pl.ds(g * SUB, SUB), pl.ds(j * LANES, LANES)] = x


def paired(
    incoming_wave,
    speed_class_map,
    spectral_entry_index,
    filter_weights,
    scaled_pulsations,
    inverse_speed_classes,
):
    strip_count = lax.axis_size("strip")
    lateral = strip_count // SECTIONS
    length = incoming_wave.shape[2]
    nfh = NFREQ // 2
    rows = 2 * length
    tall = (rows + 2 * ORDER + 2 * PAD) * SUB
    table = phase_table(filter_weights, scaled_pulsations, inverse_speed_classes)
    f32 = jnp.float32
    vmem = pl.BlockSpec(memory_space=pltpu.VMEM)

    def dma(*shape):
        return pltpu.SemaphoreType.DMA((2,) + shape)

    return pl.pallas_call(
        functools.partial(kernel, strip_count),
        out_shape=(
            jax.ShapeDtypeStruct(speed_class_map.shape, f32),
            jax.ShapeDtypeStruct(incoming_wave.shape, f32),
        ),
        in_specs=[pl.BlockSpec(memory_space=pltpu.SMEM), vmem, vmem, vmem],
        out_specs=(vmem, vmem),
        scratch_shapes=[
            pltpu.VMEM((2 * LEVELS, nfh, 2, tall, LANES), f32),
            pltpu.VMEM((ORDER, 2, tall, LANES), f32),
            pltpu.VMEM((nfh, 2, rows * SUB, LANES), f32),
            pltpu.VMEM((nfh, 2, rows * SUB, LANES), f32),
            pltpu.VMEM((nfh, 2, length * SUB, LANES), f32),
            pltpu.VMEM((nfh, 2, length * SUB, LANES), f32),
            pltpu.VMEM((LEVELS, length * SUB, LANES), jnp.int32),
            pltpu.VMEM((LEVELS, rows * SUB, LANES), jnp.int32),
            pltpu.VMEM((LEVELS, rows * SUB, LANES), f32),
            pltpu.VMEM((LEVELS, length * SUB, LANES), f32),
            pltpu.VMEM((LEVELS * SUB, LANES), f32),
            pltpu.VMEM((lateral, LEVELS * SUB, LANES), f32),
            dma(nfh + 1),
            dma(2 * LEVELS, nfh, 2),
            dma(nfh, 3),
            dma(nfh),
            dma(LEVELS),
            dma(lateral),
        ],
        compiler_params=pltpu.CompilerParams(
            collective_id=0, has_side_effects=True, vmem_limit_bytes=48 * 1024 * 1024
        ),
    )(spectral_entry_index, incoming_wave, speed_class_map, table)


ROWS = 2 * (ORDER + 1)
TICKS = 2


def lane_pick(x, index):
    return jnp.take_along_axis(
        x, index, axis=1, mode="promise_in_bounds", wrap_negative_indices=False
    )


def transposed(x):
    lane = lax.broadcasted_iota(jnp.int32, (SUB, LANES), 1)
    low = lane % SUB
    bits = [(step, (lane // step) % 2 == 1) for step in (1, 2, 4)]
    x = list(x)
    for step, bit in bits:
        x = [jnp.where(bit, x[(a + step) % SUB], x[a]) for a in range(SUB)]
    for a in range(1, SUB):
        x[a] = lane_pick(x[a], lane - low + (low + SUB - a) % SUB)
    x = [x[-n % SUB] for n in range(SUB)]
    for step, bit in bits:
        x = [jnp.where(bit, x[(m - step) % SUB], x[m]) for m in range(SUB)]
    return x


def chain_kernel(
    count,
    entry_ref,
    pulsation_ref,
    slowness_ref,
    weight_ref,
    wave_ref,
    map_ref,
    image_ref,
    handed_ref,
    entries,
    pulsations,
    slownesses,
    weights,
    rows,
    hop,
    starts,
    last,
    even,
    odd,
    paired_sum,
    running,
    coeffs,
    spread_table,
    wave_in,
    map_in,
    bins,
    raw,
    wave_out,
    raw_out,
    raw_in,
    sum_own,
    sum_in,
    small_sems,
    wave_sems,
    hop_sems,
    on_sems,
    map_sems,
    relay_sems,
    fin_sems,
    raw_sems,
    sum_sems,
    own_sems,
    own_raw_sems,
):
    length = wave_ref.shape[2]
    groups = length // SUB
    lateral = count // SECTIONS
    half = lateral // 2
    me = lax.axis_index("strip")
    plane = me // lateral
    place = lax.rem(me, lateral)
    side = place // 2
    core = lax.rem(place, 2)
    chain = lax.rem(plane + SECTIONS - 1, SECTIONS)
    section = lax.rem(chain + side, SECTIONS)
    slab = lax.rem(place + half, lateral)
    home = lax.rem(section + 1, SECTIONS)
    near = side == 0
    has_next = chain < SECTIONS - 1
    is_deep = section > 0

    def wrapped(index):
        return lax.rem(index + count, count)

    def device(index):
        return {"strip": wrapped(index)}

    def worker(plane_, f):
        return wrapped(plane_ * lateral + f)

    def owner(section_, d):
        return wrapped(section_ * lateral + half + d)

    partner = device(me + 1 - 2 * core)

    def remote(src, dst, sems, index, target, arrival=None):
        return pltpu.make_async_remote_copy(
            src_ref=src,
            dst_ref=dst,
            send_sem=sems.at[(0,) + index],
            recv_sem=sems.at[(1,) + (index if arrival is None else arrival)],
            device_id=target,
            device_id_type=MESH,
        )

    barrier = pltpu.get_barrier_semaphore()
    base = (plane - 1) * lateral
    for n in range(3 * lateral):
        mate = wrapped(base + n)

        @pl.when(mate != me)
        def _():
            pl.semaphore_signal(barrier, inc=1, device_id=device(mate), device_id_type=MESH)

    small = [
        pltpu.make_async_copy(source, target, small_sems.at[n])
        for n, (source, target) in enumerate(
            (
                (entry_ref, entries),
                (pulsation_ref, pulsations),
                (slowness_ref, slownesses),
                (weight_ref, weights),
            )
        )
    ]
    for copy in small:
        copy.start()
    own_wave = pltpu.make_async_copy(wave_ref.at[place], wave_in.at[slab], own_sems.at[0])
    own_map = pltpu.make_async_copy(map_ref, map_in.at[side, slab], own_sems.at[1])
    pl.when(near)(own_wave.start)
    pl.when(near | has_next)(own_map.start)

    lane = lax.broadcasted_iota(jnp.int32, (SUB, LANES), 1)
    sub = lax.broadcasted_iota(jnp.int32, (SUB, LANES), 0)
    high_lane, low_lane = lane // SUB, lane % SUB
    to_left = jnp.where(high_lane > 0, lane - SUB, jnp.where(low_lane > 0, 119 + low_lane, 0))
    to_right = jnp.where(
        high_lane < 15, lane + SUB, jnp.where(low_lane < 7, low_lane + 1, LANES - 1)
    )
    not_first_lane = lane > 0
    not_last_lane = lane < LANES - 1
    not_first_sub = sub > 0
    not_last_sub = sub < SUB - 1

    pl.semaphore_wait(barrier, 3 * lateral - 1)

    def wave_copy(f):
        return remote(
            wave_ref.at[f],
            wave_in.at[slab],
            wave_sems,
            (f,),
            device(worker(home, f)),
            (slab,),
        )

    def wave_arrival(d):
        return remote(
            wave_ref.at[0], wave_in.at[d], wave_sems, (d,), device(owner(chain, d))
        )

    def map_copy(tick, y):
        to = worker(home if tick == 0 else section, 2 * y + core)
        copy = remote(
            map_ref,
            map_in.at[tick, slab],
            map_sems,
            (tick, y),
            device(to),
            (tick, slab // 2),
        )
        live = to != me
        return copy, live if tick == 0 else live & is_deep

    def map_arrival(tick, h):
        d = core + 2 * h
        source = owner(chain + tick, d)
        copy = remote(map_ref, map_in.at[tick, d], map_sems, (tick, h), device(source))
        return copy, source != me

    def map_relay(tick, h):
        part = map_in.at[tick, core + 2 * h]
        return remote(part, part, relay_sems, (tick, h), partner)

    def pass_map_on(tick):
        for h in range(2):
            copy, foreign = map_arrival(tick, h)
            pl.when(foreign)(copy.wait_recv)
            pl.when(jnp.logical_not(foreign))(own_map.wait)
            map_relay(tick, h).start()

    def start_map(tick):
        for y in (1, 0):
            copy, live = map_copy(tick, y)
            pl.when(live)(copy.start)

    far = side == 1

    def hop_in(i):
        return pltpu.make_async_remote_copy(
            src_ref=wave_ref.at[i // 2, i % 2],
            dst_ref=hop.at[i // 2, i % 2],
            send_sem=hop_sems.at[0, i],
            recv_sem=hop_sems.at[1, i],
            device_id=device(worker(plane, core)),
            device_id_type=MESH,
        )

    def hop_on(i):
        return remote(
            hop.at[i // 2, i % 2],
            wave_in.at[core, i % 2],
            on_sems,
            (i,),
            device(worker(plane + 1, i // 2)),
            (2 * core + i % 2,),
        )

    def hop_arrival(d, c):
        return remote(
            hop.at[0, c],
            wave_in.at[d, c],
            on_sems,
            (2 * d + c,),
            device(worker(chain, d)),
        )

    start_map(0)

    @pl.when(far)
    def _():
        for i in range(lateral):
            hop_in(i).start()

    for f in range(half, lateral):
        wave_copy(f).start()

    @pl.when(near)
    def _():
        for f in range(half):
            pl.when(worker(home, f) != me)(wave_copy(f).start)
        start_map(1)

    for copy in small:
        copy.wait()
    entry = entries[chain, place]
    angle = pulsations[entry] * slownesses[...]
    cosine, sine = jnp.cos(angle), jnp.sin(angle)
    for k in range(ORDER + 1):
        fr, fi = (weights[entry, k, pl.ds(c, 1), :] for c in range(2))
        rows[pl.ds(k, 1), pl.ds(0, NBIN)] = fr * cosine - fi * sine
        rows[pl.ds(ORDER + 1 + k, 1), pl.ds(0, NBIN)] = fr * sine + fi * cosine
    for n in range(ROWS):
        row = jnp.broadcast_to(rows[pl.ds(n, 1), :], (SUB, LANES))
        for part in range(NBIN // SUB):
            spread_table[part, n] = lane_pick(row, sub + part * SUB)

    def pass_waves_on(some):
        for i in some:
            hop_in(i).wait_recv()
            hop_on(i).start()

    pl.when(near)(lambda: pass_waves_on(range(lateral - 1)))


    def cell(m, r):
        return pl.ds((m * SUB + r) * SUB, SUB)

    def column(m, slot):
        return pl.ds(m * SUB * SUB + slot, SUB, stride=SUB)

    def gather_back(source, d, g):
        return transposed([source[column(m, groups * d + g), :] for m in range(SUB)])

    def tile(g, j):
        return pl.ds(g * SUB, SUB), pl.ds(j * LANES, LANES)

    def spread(load, ref, d):
        for g in range(groups):
            for m, x in enumerate(transposed([load(*tile(g, j)) for j in range(SUB)])):
                ref[column(m, groups * d + g), :] = x

    def fill(tick, level):
        for d in range(lateral):
            spread(lambda row, col: map_in[tick, d, level, row, col], bins, d)
        n_cells = 4

        def some(i, carry):
            for n in range(n_cells):
                where = pl.ds(pl.multiple_of((i * n_cells + n) * SUB, SUB), SUB)
                bin_ = bins[where, :]
                high = bin_ >= SUB
                low_bits = bin_ % SUB
                for row in range(ROWS):
                    a, b = (
                        jnp.take_along_axis(
                            spread_table[part, row],
                            low_bits,
                            axis=0,
                            mode="promise_in_bounds",
                            wrap_negative_indices=False,
                        )
                        for part in range(NBIN // SUB)
                    )
                    coeffs[level, row, where, :] = jnp.where(high, b, a)
            return carry

        lax.fori_loop(0, SUB * SUB // n_cells, some, 0)

    def stencil(present, target, first=False, last=False):
        def channel(c, carry):
            below = []
            for m in range(8):
                edge = pltpu.roll(present[c, cell(m, 7), :], 1, 0)
                edge = jnp.where(not_first_sub, edge, 0.0)
                below.append(edge + present[c, cell(m, 0), :])
            for r in range(8):
                u = []
                for m in range(8):
                    here = present[c, cell(m, r), :]
                    if r < 7:
                        above = present[c, cell(m, r + 1), :]
                    else:
                        above = pltpu.roll(present[c, cell(m, 0), :], SUB - 1, 0)
                        above = jnp.where(not_last_sub, above, 0.0)
                    q = here + above
                    u.append(below[m] + q)
                    below[m] = q
                left = jnp.where(not_first_lane, lane_pick(u[7], to_left), 0.0)
                right = jnp.where(not_last_lane, lane_pick(u[0], to_right), 0.0)
                u = [left] + u + [right]
                h = [u[m] + u[m + 1] for m in range(9)]
                for m in range(8):
                    w = h[m] + h[m + 1]
                    here = present[c, cell(m, r), :]
                    if first:
                        both = 0.125 * w
                    else:
                        both = 0.25 * w - paired_sum[c, cell(m, r), :]
                    if not last:
                        paired_sum[c, cell(m, r), :] = both
                    target[c, cell(m, r), :] = both - here
            return carry

        lax.fori_loop(0, 2, channel, 0)

    def add_orders(tick, level, terms, where, total):
        re, im = (None, None) if total is None else total
        for order, ref in terms:
            tr, ti = (ref[c, where, :] for c in range(2))
            br = coeffs[level, order, where, :]
            bi = coeffs[level, ORDER + 1 + order, where, :]
            dr = br * tr - bi * ti
            di = br * ti + bi * tr
            re, im = (dr, di) if re is None else (re + dr, im + di)
        return re, im

    def sum_so_far(where):
        return [running[c, where, :] for c in range(2)]

    def unit(tick, level, output):
        start = starts.at[tick * LEVELS + level]
        stencil(start, odd, first=True)
        for i in range(SUB * SUB):
            where = pl.ds(i * SUB, SUB)
            total = add_orders(tick, level, [(0, start), (1, odd)], where, None)
            for c in range(2):
                running[c, where, :] = total[c]

        def steps(i, carry):
            stencil(odd, even)
            stencil(even, odd)
            for n in range(SUB * SUB):
                where = pl.ds(n * SUB, SUB)
                terms = [(2 * i + 2, even), (2 * i + 3, odd)]
                total = add_orders(tick, level, terms, where, sum_so_far(where))
                for c in range(2):
                    running[c, where, :] = total[c]
            return carry

        lax.fori_loop(0, ORDER // 2 - 1, steps, 0)
        stencil(odd, even, last=True)
        for i in range(SUB * SUB):
            where = pl.ds(i * SUB, SUB)
            total = add_orders(tick, level, [(ORDER, even)], where, sum_so_far(where))
            for c in range(2):
                output[c, where, :] = total[c]
            raw[tick, level, where, :] = total[0]

    def raw_copy(tick, level, d):
        to = owner(chain + tick, d)
        copy = remote(
            raw_out.at[tick, level, d],
            raw_in.at[tick, level, place],
            raw_sems,
            (tick, level, d),
            device(to),
            (tick, level, place),
        )
        return copy, to != me

    def own_raw(tick, level):
        return pltpu.make_async_copy(
            raw_out.at[tick, level, slab],
            raw_in.at[tick, level, place],
            own_raw_sems.at[tick, level],
        )

    def raw_arrival(tick, level, f):
        source = worker(home if tick == 0 else section, f)
        copy = remote(
            raw_out.at[tick, level, f],
            raw_in.at[tick, level, f],
            raw_sems,
            (tick, level, f),
            device(source),
        )
        return copy, source != me

    def send_raw(tick, level):
        for d in range(lateral):
            for g in range(groups):
                for j, x in enumerate(gather_back(raw.at[tick, level], d, g)):
                    raw_out[(tick, level, d) + tile(g, j)] = x
            copy, foreign = raw_copy(tick, level, d)
            pl.when(foreign)(copy.start)
            pl.when(jnp.logical_not(foreign))(own_raw(tick, level).start)

    def wave_back(which, d):
        to = owner(chain + which, d)
        copy = remote(
            wave_out.at[which, d],
            handed_ref.at[place],
            fin_sems,
            (which, d),
            device(to),
            (1, place),
        )
        return copy, to != me

    def own_back(which):
        return pltpu.make_async_copy(
            wave_out.at[which, slab], handed_ref.at[place], own_sems.at[0]
        )

    def handed_arrival(f):
        source = worker(jnp.maximum(section, 1), f)
        copy = remote(
            wave_out.at[1, f], handed_ref.at[f], fin_sems, (1, f), device(source)
        )
        return copy, source != me

    def send_wave(which, source):
        for d in range(lateral):
            for c in range(2):
                for g in range(groups):
                    for j, x in enumerate(gather_back(source.at[c], d, g)):
                        wave_out[(which, d, c) + tile(g, j)] = x
            copy, foreign = wave_back(which, d)
            pl.when(foreign)(copy.start)
            pl.when(jnp.logical_not(foreign))(own_back(which).start)

    pass_map_on(0)
    for h in range(2):
        map_relay(0, h).wait_recv()
    pl.when(far)(lambda: start_map(1))
    fill(0, 0)
    pl.when(near)(lambda: pass_waves_on((lateral - 1,)))
    fill(0, 1)
    def take_waves(order):
        for d in order:
            foreign = owner(chain, d) != me
            pl.when(foreign)(wave_arrival(d).wait_recv)
            pl.when(jnp.logical_not(foreign))(own_wave.wait)
            for c in range(2):
                spread(lambda row, col: wave_in[d, c, row, col], starts.at[0, c], d)

    @pl.when(near)
    def _():
        take_waves((2, 3))
        for d in range(half):
            for c in range(2):
                hop_arrival(d, c).wait_recv()
                spread(lambda row, col: wave_in[d, c, row, col], starts.at[0, c], d)

    pl.when(far)(lambda: take_waves((0, 1, 2, 3)))
    unit(0, 0, starts.at[1])
    send_raw(0, 0)
    pl.when(has_next)(lambda: pass_map_on(1))
    unit(0, 1, starts.at[2])
    send_raw(0, 1)

    @pl.when(chain == 0)
    def _():
        send_wave(0, starts.at[2])

    @pl.when(has_next)
    def _():
        for h in range(2):
            map_relay(1, h).wait_recv()
        fill(1, 0)
        fill(1, 1)
        unit(1, 0, starts.at[3])
        send_raw(1, 0)
        unit(1, 1, last)
        send_raw(1, 1)
        send_wave(1, last)

    for level in range(LEVELS):
        for tick in range(TICKS):
            for f in range(lateral):
                copy, foreign = raw_arrival(tick, level, f)
                own = jnp.logical_not(foreign)
                if tick == 1:
                    foreign, own = foreign & is_deep, own & is_deep
                pl.when(foreign)(copy.wait_recv)
                pl.when(own)(own_raw(tick, level).wait)
        total = jnp.zeros((SUB, LANES), jnp.float32)
        for g in range(groups):
            for j in range(SUB):
                value = second = None
                for f in range(lateral):
                    a, b = (raw_in[(t, level, f) + tile(g, j)] for t in range(TICKS))
                    value = a if value is None else value + a
                    second = b if second is None else second + b
                value = value + jnp.where(is_deep, second, 0.0)
                image_ref[(level,) + tile(g, j)] = value
                total = total + value * value
        sum_own[pl.ds(level * SUB, SUB), :] = total

    def sum_copy(x):
        mate = lax.rem(slab + x, lateral)
        return remote(sum_own, sum_in.at[x], sum_sems, (x,), device(owner(section, mate)))

    for x in range(1, lateral):
        sum_copy(x).start()
    for tick in range(TICKS):
        for y in range(2):
            copy, live = map_copy(tick, y)
            pl.when(live)(copy.wait_send)
    for h in range(2):
        map_relay(0, h).wait_send()
        pl.when(has_next)(map_relay(1, h).wait_send)
    for n in range(lateral):
        if n < half:
            pl.when(near & (worker(home, n) != me))(wave_copy(n).wait_send)
        else:
            wave_copy(n).wait_send()
        pl.when(near)(hop_on(n).wait_send)
        pl.when(far)(hop_in(n).wait_send)
        for which, live in ((0, chain == 0), (1, has_next)):
            copy, foreign = wave_back(which, n)
            pl.when(foreign & live)(copy.wait_send)
        for level in range(LEVELS):
            for tick in range(TICKS):
                copy, foreign = raw_copy(tick, level, n)
                pl.when(foreign if tick == 0 else foreign & has_next)(copy.wait_send)
    total = sum_own[...]
    for x in range(1, lateral):
        sum_copy(x).wait_recv()
        total = total + sum_in[x]
    cells = length * lateral * SUB * LANES
    for level in range(LEVELS):
        mean = (
            jnp.sum(total[level * SUB : (level + 1) * SUB], axis=(0, 1), keepdims=True) / cells
        )
        scale = jnp.broadcast_to(1.0 / jnp.sqrt(mean + 1e-06), (SUB, LANES))
        for g in range(groups):
            for j in range(SUB):
                where = (level,) + tile(g, j)
                image_ref[where] = image_ref[where] * scale
    for f in range(lateral):
        copy, foreign = handed_arrival(f)
        pl.when(foreign)(copy.wait_recv)
        pl.when(jnp.logical_not(foreign))(own_back(0).wait)
    for x in range(1, lateral):
        sum_copy(x).wait_send()


def phase_table(filter_weights, scaled_pulsations, inverse_speed_classes):
    angle = scaled_pulsations[:, None] * inverse_speed_classes[None, :]
    cosine = jnp.cos(angle)[:, None, :]
    sine = jnp.sin(angle)[:, None, :]
    by_order = jnp.transpose(filter_weights, (2, 0, 3, 1))
    real = by_order[0] * cosine - by_order[1] * sine
    imag = by_order[0] * sine + by_order[1] * cosine
    table = jnp.stack([real, imag], axis=2).reshape(NW, 2 * (ORDER + 1), NBIN)
    return jnp.pad(table, ((0, 0), (0, 0), (0, LANES - NBIN)))


def chains(
    incoming_wave,
    speed_class_map,
    spectral_entry_index,
    filter_weights,
    scaled_pulsations,
    inverse_speed_classes,
):
    count = lax.axis_size("strip")
    lateral = count // SECTIONS
    length, across = incoming_wave.shape[2:]
    tall = length * lateral * SUB
    f32 = jnp.float32
    vmem = pl.BlockSpec(memory_space=pltpu.VMEM)
    anywhere = pl.BlockSpec(memory_space=pl.ANY)
    def dma(*shape):
        return pltpu.SemaphoreType.DMA((2,) + shape)

    return pl.pallas_call(
        functools.partial(chain_kernel, count),
        out_shape=(
            jax.ShapeDtypeStruct(speed_class_map.shape, f32),
            jax.ShapeDtypeStruct(incoming_wave.shape, f32),
        ),
        in_specs=[anywhere] * 6,
        out_specs=(vmem, vmem),
        scratch_shapes=[
            pltpu.SMEM(spectral_entry_index.shape, jnp.int32),
            pltpu.SMEM((NW,), f32),
            pltpu.VMEM((1, NBIN), f32),
            pltpu.VMEM((NW, ORDER + 1, 2, NBIN), f32),
            pltpu.VMEM((ROWS, LANES), f32),
            pltpu.VMEM((lateral // 2, 2, length, across), f32),
            pltpu.VMEM((TICKS * LEVELS, 2, tall, LANES), f32),
            pltpu.VMEM((2, tall, LANES), f32),
            pltpu.VMEM((2, tall, LANES), f32),
            pltpu.VMEM((2, tall, LANES), f32),
            pltpu.VMEM((2, tall, LANES), f32),
            pltpu.VMEM((2, tall, LANES), f32),
            pltpu.VMEM((LEVELS, ROWS, tall, LANES), f32),
            pltpu.VMEM((NBIN // SUB, ROWS, SUB, LANES), f32),
            pltpu.VMEM((lateral, 2, length, across), f32),
            pltpu.VMEM((TICKS, lateral, LEVELS, length, across), jnp.int32),
            pltpu.VMEM((tall, LANES), jnp.int32),
            pltpu.VMEM((TICKS, LEVELS, tall, LANES), f32),
            pltpu.VMEM((2, lateral, 2, length, across), f32),
            pltpu.VMEM((TICKS, LEVELS, lateral, length, across), f32),
            pltpu.VMEM((TICKS, LEVELS, lateral, length, across), f32),
            pltpu.VMEM((LEVELS * SUB, LANES), f32),
            pltpu.VMEM((lateral, LEVELS * SUB, LANES), f32),
            pltpu.SemaphoreType.DMA((4,)),
            dma(lateral),
            dma(lateral),
            dma(lateral),
            dma(TICKS, 2),
            dma(TICKS, 2),
            dma(2, lateral),
            dma(TICKS, LEVELS, lateral),
            dma(lateral),
            pltpu.SemaphoreType.DMA((2,)),
            pltpu.SemaphoreType.DMA((TICKS, LEVELS)),
        ],
        compiler_params=pltpu.CompilerParams(
            collective_id=0, has_side_effects=True, vmem_limit_bytes=32 * 1024 * 1024
        ),
    )(
        *(
            pltpu.with_memory_space_constraint(x, pltpu.HBM)
            for x in (
                spectral_entry_index,
                scaled_pulsations,
                inverse_speed_classes[None],
                jnp.transpose(filter_weights, (0, 3, 2, 1)),
                incoming_wave,
                speed_class_map,
            )
        )
    )


def fits(mesh):
    lateral = mesh.shape["strip"] // SECTIONS
    return NFREQ % 2 == 0 and lateral % 4 == 0


def whole_section(mesh, wave):
    lateral = mesh.shape["strip"] // SECTIONS
    full = lateral * wave.shape[2] == SUB * SUB and wave.shape[3] == SUB * LANES
    return lateral == NFREQ == 4 and wave.shape[2] % SUB == 0 and full


def body_for(mesh):
    def body(wave, *rest):
        whole = wave.shape[3] == SUB * LANES and wave.shape[2] % SUB == 0
        if whole_section(mesh, wave):
            return chains(wave, *rest)
        if fits(mesh) and whole and wave.shape[2] >= ORDER:
            return paired(wave, *rest)
        return shards(wave, *rest)

    return body


def solution(mesh):
    return jax.shard_map(
        body_for(mesh),
        mesh=mesh,
        in_specs=(
            P("groups", None, "strip", None),
            P("groups", "strip", None),
            P("groups", None),
            P(),
            P(),
            P(),
        ),
        out_specs=(P("groups", "strip", None), P("groups", None, "strip", None)),
        check_vma=False,
    )
```

```python
import functools
import jax
import jax.numpy as jnp
from jax import lax
from jax.experimental import pallas as pl
from jax.experimental.pallas import tpu as pltpu
from jax.sharding import PartitionSpec as P

SECTIONS = 4
LEVELS = 2
ORDER = 12
NFREQ = 4
NBIN = 16
NW = 16


def extended_2(shard, sides, width):
    for axis, dim in sides:
        devices, length = (lax.axis_size(axis), shard.shape[dim])
        up = [(i, (i + 1) % devices) for i in range(devices)]
        down = [(j, i) for i, j in up]
        last = lax.slice_in_dim(shard, length - width, length, axis=dim)
        initial = lax.slice_in_dim(shard, 0, width, axis=dim)
        before = lax.ppermute(last, axis, up)
        after = lax.ppermute(initial, axis, down)
        shard = jnp.concatenate([before, shard, after], axis=dim)
    return shard


def from_behind(shard, axis, by):
    devices = lax.axis_size(axis)
    return lax.ppermute(shard, axis, [(i, (i + by) % devices) for i in range(devices)])


def stencil_padded(padded):
    vertical = padded[:, :, :-2, :] + padded[:, :, 2:, :]
    middle = padded[:, :, 1:-1, :]
    return (
        -0.5 * middle[..., 1:-1]
        + 0.25 * (vertical[..., 1:-1] + middle[..., :-2] + middle[..., 2:])
        + 0.125 * (vertical[..., :-2] + vertical[..., 2:])
    )


def complex_times(coeff, field):
    real_part = coeff[:, 0] * field[:, 0] - coeff[:, 1] * field[:, 1]
    imag_part = coeff[:, 0] * field[:, 1] + coeff[:, 1] * field[:, 0]
    return jnp.stack([real_part, imag_part], axis=1)


def shards(
    incoming_wave,
    speed_class_map,
    spectral_entry_index,
    filter_weights,
    scaled_pulsations,
    inverse_speed_classes,
):
    highest = lax.Precision.HIGHEST
    summed_along = incoming_wave.shape[2]
    summed_across = incoming_wave.shape[3]
    strip_count = lax.axis_size("strip")
    lateral_count = strip_count // SECTIONS
    position = (lax.axis_index("strip") - lateral_count // 2) % strip_count
    vertical_slab = position // lateral_count
    lateral_place = position % lateral_count
    section_rows = summed_along * lateral_count
    section_cells = section_rows * summed_across
    margin = ORDER
    extended_rows = summed_along + 2 * margin
    lateral_rows = (
        lateral_place * summed_along - margin + jnp.arange(extended_rows, dtype=jnp.int32)
    )
    inside = ((lateral_rows >= 0) & (lateral_rows < section_rows)).astype(jnp.float32)[
        None, None, :, None
    ]

    def mcclellan_step(field):
        padded = jnp.pad(field, ((0, 0), (0, 0), (1, 1), (0, 0)))
        padded = jnp.pad(padded, ((0, 0), (0, 0), (0, 0), (1, 1)))
        result = stencil_padded(padded)
        result = result * inside
        return result

    def interior(field):
        return field[:, :, margin : margin + summed_along, :]

    def image_downward(field, batch_index):
        freq_row = lax.dynamic_index_in_dim(spectral_entry_index, batch_index, 0, keepdims=False)
        freq_select = (freq_row[:, None] == jnp.arange(NW, dtype=jnp.int32)[None, :]).astype(
            jnp.float32
        )
        freq_coeffs = jnp.einsum("fw,wbck->fbck", freq_select, filter_weights, precision=highest)
        freq_omega = jnp.dot(freq_select, scaled_pulsations, precision=highest)
        wavefield = field
        raws = []
        for level in range(LEVELS):
            cells = speed_class_map[level].reshape(-1)
            bin_onehot = (cells[None, :] == jnp.arange(NBIN, dtype=jnp.int32)[:, None]).astype(
                jnp.float32
            )
            cell_slowness = jnp.dot(inverse_speed_classes, bin_onehot, precision=highest).reshape(
                summed_along, summed_across
            )
            table = jnp.einsum("fbck,bn->kfcn", freq_coeffs, bin_onehot, precision=highest).reshape(
                ORDER + 1, NFREQ, 2, summed_along, summed_across
            )
            extended = extended_2(wavefield, (("strip", 2),), ORDER) * inside
            previous = extended
            current = mcclellan_step(extended)
            accumulated = complex_times(table[0], interior(previous)) + complex_times(
                table[1], interior(current)
            )

            def recursion_step(order_index, state_tuple):
                before, present, running = state_tuple
                following = 2.0 * mcclellan_step(present) - before
                coeff = lax.dynamic_index_in_dim(table, order_index, 0, keepdims=False)
                running = running + complex_times(coeff, interior(following))
                return (present, following, running)

            previous, current, accumulated = lax.fori_loop(
                2, ORDER + 1, recursion_step, (previous, current, accumulated)
            )
            phase_angle = freq_omega[:, None, None] * cell_slowness[None]
            cosine = jnp.cos(phase_angle)
            sine_part = jnp.sin(phase_angle)
            real_part = accumulated[:, 0] * cosine - accumulated[:, 1] * sine_part
            imag_part = accumulated[:, 0] * sine_part + accumulated[:, 1] * cosine
            wavefield = jnp.stack([real_part, imag_part], axis=1)
            raws.append(jnp.sum(real_part, axis=0))
        return (wavefield, raws)

    above_floor_lines, above_unscaled_waves = image_downward(incoming_wave, vertical_slab)
    arriving = from_behind(above_floor_lines, "strip", lateral_count)
    second_bottom, second_raws = image_downward(arriving, jnp.maximum(vertical_slab - 1, 0))
    handed = jnp.where(vertical_slab == 0, above_floor_lines, second_bottom)
    first_section = (vertical_slab > 0).astype(jnp.float32)
    totals = [
        above_unscaled_waves[level] + first_section * second_raws[level] for level in range(LEVELS)
    ]
    selector = (jnp.arange(SECTIONS, dtype=jnp.int32) == vertical_slab).astype(jnp.float32)
    images = []
    for level in range(LEVELS):
        raw_image = totals[level]
        spread = lax.psum(selector * jnp.sum(raw_image * raw_image), "strip")
        mean_square = jnp.sum(spread * selector) / section_cells
        images.append(raw_image / jnp.sqrt(mean_square + 1e-06))
    return (jnp.stack(images, axis=0), handed)


SUB = 8
LANES = 128
PAD = 5
UNROLL = 8
TOGETHER = 4
MESH = pl.DeviceIdType.MESH


def at_row(row):
    return pl.ds(pl.multiple_of(row * SUB, SUB), SUB)


def kernel(
    strip_count,
    entry_ref,
    wave_ref,
    map_ref,
    table_ref,
    image_ref,
    handed_ref,
    starts,
    work,
    bottom,
    last,
    last_in,
    wave_out,
    map_out,
    map_all,
    raw,
    raw_in,
    sum_own,
    sum_in,
    swap_sems,
    halo_sems,
    hand_sems,
    fin_sems,
    raw_sems,
    sum_sems,
):
    nfh = wave_ref.shape[0] // 2
    length = wave_ref.shape[2]
    rows = 2 * length
    blocks = wave_ref.shape[3] // LANES
    lateral = strip_count // SECTIONS
    shift = lateral // 2
    pairs = lateral // 2
    margin = ORDER
    first = PAD + margin
    me = lax.axis_index("strip")
    position = lax.rem(me + strip_count - shift, strip_count)
    section = position // lateral
    place = lax.rem(position, lateral)
    pair = place // 2
    half = lax.rem(place, 2)
    up = jnp.where(pair > 0, 1, 0)
    down = jnp.where(pair < pairs - 1, 1, 0)
    has_up = pair > 0
    has_down = pair < pairs - 1
    has_before = section > 0
    has_after = section < SECTIONS - 1
    other = 1 - half

    def device(pos):
        return {"strip": lax.rem(pos + shift + strip_count, strip_count)}

    partner = device(position + 1 - 2 * half)
    upper = device(position - 2)
    lower = device(position + 2)
    deeper = device(position + lateral)
    shallower = device(position + strip_count - lateral)

    def remote(src, dst, sems, index, target):
        return pltpu.make_async_remote_copy(
            src_ref=src,
            dst_ref=dst,
            send_sem=sems.at[(0,) + index],
            recv_sem=sems.at[(1,) + index],
            device_id=target,
            device_id_type=MESH,
        )

    def span(row, count):
        return pl.ds(pl.multiple_of(row * SUB, SUB), count * SUB)

    zero = jnp.zeros((SUB, LANES), jnp.float32)
    for edge in (first - 1, first + rows):
        for f in range(nfh):
            for c in range(2):
                for s in range(2 * LEVELS):
                    starts[s, f, c, at_row(edge), :] = zero
        for c in range(2):
            for k in range(ORDER):
                work[k, c, at_row(edge), :] = zero

    barrier = pltpu.get_barrier_semaphore()
    for d in range(1, lateral):
        mate = device(section * lateral + lax.rem(place + d, lateral))
        pl.semaphore_signal(barrier, inc=1, device_id=mate, device_id_type=MESH)
    for target in (deeper, shallower):
        pl.semaphore_signal(barrier, inc=1, device_id=target, device_id_type=MESH)

    def rearrange(load, store):
        for g in range(length // SUB):
            for j in range(blocks):
                store(g, j, load(g, j))

    def strided(row, g, j):
        return pl.ds((row + g * SUB) * SUB + j, SUB, stride=SUB)

    own_row = half * length
    swaps = []
    for f in range(nfh):
        for c in range(2):
            rearrange(
                lambda g, j: wave_ref[other * nfh + f, c, pl.ds(g * SUB, SUB), pl.ds(j * LANES, LANES)],
                lambda g, j, x: pltpu_store(wave_out.at[f, c], strided(0, g, j), x),
            )
        if f == 0:
            pl.semaphore_wait(barrier, lateral + 1)
        copy = remote(
            wave_out.at[f],
            starts.at[0, f, :, span(first + own_row, length), :],
            swap_sems,
            (f,),
            partner,
        )
        copy.start()
        swaps.append(copy)
    for l in range(LEVELS):
        rearrange(
            lambda g, j: map_ref[l, pl.ds(g * SUB, SUB), pl.ds(j * LANES, LANES)],
            lambda g, j, x: pltpu_store(map_out.at[l], strided(0, g, j), x),
        )
    copy = remote(
        map_out, map_all.at[:, span(own_row, length), :], swap_sems, (nfh,), partner
    )
    copy.start()
    swaps.append(copy)
    for f in range(nfh):
        for c in range(2):
            rearrange(
                lambda g, j: wave_ref[half * nfh + f, c, pl.ds(g * SUB, SUB), pl.ds(j * LANES, LANES)],
                lambda g, j, x: pltpu_store(
                    starts.at[0, f, c], strided(first + own_row, g, j), x
                ),
            )
    for l in range(LEVELS):
        rearrange(
            lambda g, j: map_ref[l, pl.ds(g * SUB, SUB), pl.ds(j * LANES, LANES)],
            lambda g, j, x: pltpu_store(map_all.at[l], strided(own_row, g, j), x),
        )

    def halo_up(stage, f):
        ref = starts.at[stage, f]
        return remote(
            ref.at[:, span(first, margin), :],
            ref.at[:, span(first + rows, margin), :],
            halo_sems,
            (stage, f, 0),
            upper,
        )

    def halo_down(stage, f):
        ref = starts.at[stage, f]
        return remote(
            ref.at[:, span(first + rows - margin, margin), :],
            ref.at[:, span(first - margin, margin), :],
            halo_sems,
            (stage, f, 1),
            lower,
        )

    def send_halo(stage, f):
        pl.when(has_up)(lambda: halo_up(stage, f).start())
        pl.when(has_down)(lambda: halo_down(stage, f).start())

    def wait_halo(stage, f):
        pl.when(has_down)(lambda: halo_up(stage, f).wait_recv())
        pl.when(has_up)(lambda: halo_down(stage, f).wait_recv())

    def hand_parts(f):
        parts = ((0, margin), (rows - margin, margin), (margin, rows - 2 * margin))
        return [
            remote(
                bottom.at[f, :, span(row, count), :],
                starts.at[LEVELS, f, :, span(first + row, count), :],
                hand_sems,
                (f, n),
                deeper,
            )
            for n, (row, count) in enumerate(parts)
        ]

    lane = lax.broadcasted_iota(jnp.int32, (SUB, LANES), 1)
    sub = lax.broadcasted_iota(jnp.int32, (SUB, LANES), 0)
    at_first = lane == 0
    at_last = lane == LANES - 1
    keep_first = sub > 0
    keep_last = sub < SUB - 1

    def across(u):
        right = pltpu.roll(u, 1, 1)
        right_fix = jnp.where(keep_first, pltpu.roll(right, 1, 0), 0.0)
        left = pltpu.roll(u, LANES - 1, 1)
        left_fix = jnp.where(keep_last, pltpu.roll(left, SUB - 1, 0), 0.0)
        return jnp.where(at_first, right_fix, right) + jnp.where(at_last, left_fix, left)

    def reach(k):
        return ((margin - k + UNROLL - 1) // UNROLL) * UNROLL

    def apply(k, present, before, target):
        extra = reach(k)
        low = first - up * extra
        count = (rows + (up + down) * extra) // UNROLL

        def block(i, carry):
            base = low + i * UNROLL
            v = [
                [present[c, at_row(base - 1 + n), :] for n in range(UNROLL + 2)]
                for c in range(2)
            ]
            old = None
            if before is not None:
                old = [
                    [before[c, at_row(base + n), :] for n in range(UNROLL)] for c in range(2)
                ]
            values = []
            for c in range(2):
                q = [v[c][n] + v[c][n + 1] for n in range(UNROLL + 1)]
                for n in range(UNROLL):
                    u = q[n] + q[n + 1]
                    w = across(u) + (u + u)
                    centre = v[c][n + 1]
                    if old is None:
                        value = 0.125 * w - centre
                    else:
                        value = 0.25 * w - (centre + centre + old[c][n])
                    values.append(value)
            for c in range(2):
                for n in range(UNROLL):
                    target[c, at_row(base + n), :] = values[c * UNROLL + n]
            return carry

        lax.fori_loop(0, count, block, 0)

    def unit(tick, level, f, meanwhile=None):
        stage = tick * LEVELS + level
        start = starts.at[stage, f]
        apply(1, start, None, work.at[0])
        apply(2, work.at[0], start, work.at[1])

        def step(k, carry):
            apply(k, work.at[k - 2], work.at[k - 3], work.at[k - 1])
            return carry

        lax.fori_loop(3, ORDER + 1, step, 0)
        if meanwhile is not None:
            meanwhile()
        batch = section if tick == 0 else jnp.maximum(section - 1, 0)
        entry = entry_ref[batch, half * nfh + f]

        def combine(i, carry):
            spots = [TOGETHER * i + n for n in range(TOGETHER)]
            bins = [map_all[level, at_row(r), :] for r in spots]
            real = [None] * TOGETHER
            imag = [None] * TOGETHER
            for n, r in enumerate(spots):
                for k in range(ORDER + 1):
                    cr, ci = (
                        jnp.take_along_axis(
                            jnp.broadcast_to(
                                table_ref[entry, pl.ds(2 * k + c, 1), :], (SUB, LANES)
                            ),
                            bins[n],
                            axis=1,
                            mode="promise_in_bounds",
                        )
                        for c in range(2)
                    )
                    source = start if k == 0 else work.at[k - 1]
                    tr = source[0, at_row(first + r), :]
                    ti = source[1, at_row(first + r), :]
                    re = cr * tr - ci * ti
                    im = cr * ti + ci * tr
                    real[n] = re if k == 0 else real[n] + re
                    imag[n] = im if k == 0 else imag[n] + im
            for n, r in enumerate(spots):
                re, im = real[n], imag[n]
                if tick == 0 and f == 0:
                    raw[level, at_row(r), :] = re
                else:
                    part = re if tick == 0 else jnp.where(has_before, re, 0.0)
                    raw[level, at_row(r), :] = raw[level, at_row(r), :] + part
                for c, value in enumerate((re, im)):
                    if level < LEVELS - 1:
                        starts[stage + 1, f, c, at_row(first + r), :] = value
                    elif tick == 0:
                        bottom[f, c, at_row(r), :] = value
                    else:
                        last[f, c, at_row(r), :] = jnp.where(
                            has_before, value, bottom[f, c, at_row(r), :]
                        )
            return carry

        lax.fori_loop(0, rows // TOGETHER, combine, 0)

    def finish_wave(f):
        return remote(
            last.at[f, :, span(other * length, length), :],
            last_in.at[f],
            fin_sems,
            (f,),
            partner,
        )

    def finish_raw(l):
        return remote(
            raw.at[l, span(other * length, length), :], raw_in.at[l], raw_sems, (l,), partner
        )

    for f in range(nfh):
        swaps[f].wait_recv()
        send_halo(0, f)
    swaps[nfh].wait_recv()
    for level in range(LEVELS):
        for f in range(nfh):
            wait_halo(level, f)
            unit(0, level, f)
            if level < LEVELS - 1:
                send_halo(level + 1, f)
            else:

                @pl.when(has_after)
                def _():
                    for copy in hand_parts(f):
                        copy.start()

    def forward(f):
        @pl.when(has_before)
        def _():
            high, low, mid = hand_parts(f)
            high.wait_recv()
            pl.when(has_up)(lambda: halo_up(LEVELS, f).start())
            low.wait_recv()
            pl.when(has_down)(lambda: halo_down(LEVELS, f).start())
            mid.wait_recv()

    def skip_or(fn):
        pl.when(has_before)(fn)

    forward(0)
    for level in range(LEVELS):
        for f in range(nfh):

            @pl.when(has_before)
            def _():
                wait_halo(LEVELS + level, f)

            later = f + 1 if level == 0 and f + 1 < nfh else None
            unit(1, level, f, None if later is None else lambda: forward(later))
            if level < LEVELS - 1:

                @pl.when(has_before)
                def _():
                    send_halo(LEVELS + level + 1, f)

            else:
                finish_wave(f).start()
        finish_raw(level).start()

    for l in range(LEVELS):
        finish_raw(l).wait_recv()

        def merge(i, carry):
            value = raw[l, at_row(own_row + i), :] + raw_in[l, at_row(i), :]
            raw_in[l, at_row(i), :] = value
            return carry + value * value

        sum_own[pl.ds(l * SUB, SUB), :] = lax.fori_loop(0, length, merge, zero)
    for d in range(1, lateral):
        mate = device(section * lateral + lax.rem(place + d, lateral))
        remote(sum_own, sum_in.at[d], sum_sems, (d,), mate).start()

    for f in range(nfh):
        for c in range(2):
            rearrange(
                lambda g, j: last[f, c, strided(own_row, g, j), :],
                lambda g, j, x: out_store(handed_ref, half * nfh + f, c, g, j, x),
            )
    for f in range(nfh):
        finish_wave(f).wait_recv()
        for c in range(2):
            rearrange(
                lambda g, j: last_in[f, c, strided(0, g, j), :],
                lambda g, j, x: out_store(handed_ref, other * nfh + f, c, g, j, x),
            )

    total = sum_own[...]
    for d in range(1, lateral):
        mate = device(section * lateral + lax.rem(place + d, lateral))
        remote(sum_own, sum_in.at[d], sum_sems, (d,), mate).wait_recv()
        total = total + sum_in[d]
    cells = length * lateral * blocks * LANES
    for l in range(LEVELS):
        mean = jnp.sum(total[l * SUB : (l + 1) * SUB], axis=(0, 1), keepdims=True) / cells
        scale = jnp.broadcast_to(1.0 / jnp.sqrt(mean + 1e-06), (SUB, LANES))

        def put(g, j, x):
            image_ref[l, pl.ds(g * SUB, SUB), pl.ds(j * LANES, LANES)] = x * scale

        rearrange(lambda g, j: raw_in[l, strided(0, g, j), :], put)

    for copy in swaps:
        copy.wait_send()
    for f in range(nfh):
        send_done = lambda make, stage: make(stage, f).wait_send()
        for stage in range(2 * LEVELS):
            live_up = has_up if stage < LEVELS else has_up & has_before
            live_down = has_down if stage < LEVELS else has_down & has_before
            pl.when(live_up)(lambda: send_done(halo_up, stage))
            pl.when(live_down)(lambda: send_done(halo_down, stage))

        @pl.when(has_after)
        def _():
            for copy in hand_parts(f):
                copy.wait_send()

        finish_wave(f).wait_send()
    for l in range(LEVELS):
        finish_raw(l).wait_send()
    for d in range(1, lateral):
        mate = device(section * lateral + lax.rem(place + d, lateral))
        remote(sum_own, sum_in.at[d], sum_sems, (d,), mate).wait_send()


def pltpu_store(ref, where, x):
    ref[where, :] = x


def out_store(ref, f, c, g, j, x):
    ref[f, c, pl.ds(g * SUB, SUB), pl.ds(j * LANES, LANES)] = x


def paired(
    incoming_wave,
    speed_class_map,
    spectral_entry_index,
    filter_weights,
    scaled_pulsations,
    inverse_speed_classes,
):
    strip_count = lax.axis_size("strip")
    lateral = strip_count // SECTIONS
    length = incoming_wave.shape[2]
    nfh = NFREQ // 2
    rows = 2 * length
    tall = (rows + 2 * ORDER + 2 * PAD) * SUB
    table = phase_table(filter_weights, scaled_pulsations, inverse_speed_classes)
    f32 = jnp.float32
    vmem = pl.BlockSpec(memory_space=pltpu.VMEM)

    def dma(*shape):
        return pltpu.SemaphoreType.DMA((2,) + shape)

    return pl.pallas_call(
        functools.partial(kernel, strip_count),
        out_shape=(
            jax.ShapeDtypeStruct(speed_class_map.shape, f32),
            jax.ShapeDtypeStruct(incoming_wave.shape, f32),
        ),
        in_specs=[pl.BlockSpec(memory_space=pltpu.SMEM), vmem, vmem, vmem],
        out_specs=(vmem, vmem),
        scratch_shapes=[
            pltpu.VMEM((2 * LEVELS, nfh, 2, tall, LANES), f32),
            pltpu.VMEM((ORDER, 2, tall, LANES), f32),
            pltpu.VMEM((nfh, 2, rows * SUB, LANES), f32),
            pltpu.VMEM((nfh, 2, rows * SUB, LANES), f32),
            pltpu.VMEM((nfh, 2, length * SUB, LANES), f32),
            pltpu.VMEM((nfh, 2, length * SUB, LANES), f32),
            pltpu.VMEM((LEVELS, length * SUB, LANES), jnp.int32),
            pltpu.VMEM((LEVELS, rows * SUB, LANES), jnp.int32),
            pltpu.VMEM((LEVELS, rows * SUB, LANES), f32),
            pltpu.VMEM((LEVELS, length * SUB, LANES), f32),
            pltpu.VMEM((LEVELS * SUB, LANES), f32),
            pltpu.VMEM((lateral, LEVELS * SUB, LANES), f32),
            dma(nfh + 1),
            dma(2 * LEVELS, nfh, 2),
            dma(nfh, 3),
            dma(nfh),
            dma(LEVELS),
            dma(lateral),
        ],
        compiler_params=pltpu.CompilerParams(
            collective_id=0, has_side_effects=True, vmem_limit_bytes=48 * 1024 * 1024
        ),
    )(spectral_entry_index, incoming_wave, speed_class_map, table)


ROWS = 2 * (ORDER + 1)
TICKS = 2


def lane_pick(x, index):
    return jnp.take_along_axis(
        x, index, axis=1, mode="promise_in_bounds", wrap_negative_indices=False
    )


def transposed(x):
    lane = lax.broadcasted_iota(jnp.int32, (SUB, LANES), 1)
    low = lane % SUB
    bits = [(step, (lane // step) % 2 == 1) for step in (1, 2, 4)]
    x = list(x)
    for step, bit in bits:
        x = [jnp.where(bit, x[(a + step) % SUB], x[a]) for a in range(SUB)]
    for a in range(1, SUB):
        x[a] = lane_pick(x[a], lane - low + (low + SUB - a) % SUB)
    x = [x[-n % SUB] for n in range(SUB)]
    for step, bit in bits:
        x = [jnp.where(bit, x[(m - step) % SUB], x[m]) for m in range(SUB)]
    return x


def chain_kernel(
    count,
    entry_ref,
    pulsation_ref,
    slowness_ref,
    weight_ref,
    wave_ref,
    map_ref,
    image_ref,
    handed_ref,
    entries,
    pulsations,
    slownesses,
    weights,
    rows,
    hop,
    starts,
    last,
    even,
    odd,
    paired_sum,
    running,
    coeffs,
    spread_table,
    wave_in,
    map_in,
    bins,
    raw,
    wave_out,
    summed,
    raw_in,
    sum_own,
    sum_in,
    small_sems,
    wave_sems,
    hop_sems,
    on_sems,
    map_sems,
    relay_sems,
    fin_sems,
    raw_sems,
    sum_sems,
    own_sems,
    own_raw_sems,
):
    length = wave_ref.shape[2]
    groups = length // SUB
    lateral = count // SECTIONS
    half = lateral // 2
    me = lax.axis_index("strip")
    plane = me // lateral
    place = lax.rem(me, lateral)
    side = place // 2
    core = lax.rem(place, 2)
    chain = lax.rem(plane + SECTIONS - 1, SECTIONS)
    section = lax.rem(chain + side, SECTIONS)
    slab = lax.rem(place + half, lateral)
    home = lax.rem(section + 1, SECTIONS)
    near = side == 0
    slab_home = side
    has_next = chain < SECTIONS - 1
    is_deep = section > 0

    def wrapped(index):
        return lax.rem(index + count, count)

    def device(index):
        return {"strip": wrapped(index)}

    def worker(plane_, f):
        return wrapped(plane_ * lateral + f)

    def owner(section_, d):
        return wrapped(section_ * lateral + half + d)

    partner = device(me + 1 - 2 * core)

    def remote(src, dst, sems, index, target, arrival=None):
        return pltpu.make_async_remote_copy(
            src_ref=src,
            dst_ref=dst,
            send_sem=sems.at[(0,) + index],
            recv_sem=sems.at[(1,) + (index if arrival is None else arrival)],
            device_id=target,
            device_id_type=MESH,
        )

    barrier = pltpu.get_barrier_semaphore()
    base = (plane - 1) * lateral
    for n in range(3 * lateral):
        mate = wrapped(base + n)

        @pl.when(mate != me)
        def _():
            pl.semaphore_signal(barrier, inc=1, device_id=device(mate), device_id_type=MESH)

    small = [
        pltpu.make_async_copy(source, target, small_sems.at[n])
        for n, (source, target) in enumerate(
            (
                (entry_ref, entries),
                (pulsation_ref, pulsations),
                (slowness_ref, slownesses),
                (weight_ref, weights),
            )
        )
    ]
    for copy in small:
        copy.start()
    own_wave = pltpu.make_async_copy(wave_ref.at[place], wave_in.at[slab], own_sems.at[0])
    own_map = pltpu.make_async_copy(map_ref, map_in.at[side, slab], own_sems.at[1])
    pl.when(near)(own_wave.start)
    pl.when(near | has_next)(own_map.start)

    lane = lax.broadcasted_iota(jnp.int32, (SUB, LANES), 1)
    sub = lax.broadcasted_iota(jnp.int32, (SUB, LANES), 0)
    high_lane, low_lane = lane // SUB, lane % SUB
    to_left = jnp.where(high_lane > 0, lane - SUB, jnp.where(low_lane > 0, 119 + low_lane, 0))
    to_right = jnp.where(
        high_lane < 15, lane + SUB, jnp.where(low_lane < 7, low_lane + 1, LANES - 1)
    )
    not_first_lane = lane > 0
    not_last_lane = lane < LANES - 1
    not_first_sub = sub > 0
    not_last_sub = sub < SUB - 1

    pl.semaphore_wait(barrier, 3 * lateral - 1)

    def wave_copy(f):
        return remote(
            wave_ref.at[f],
            wave_in.at[slab],
            wave_sems,
            (f,),
            device(worker(home, f)),
            (slab,),
        )

    def wave_arrival(d):
        return remote(
            wave_ref.at[0], wave_in.at[d], wave_sems, (d,), device(owner(chain, d))
        )

    def map_copy(tick, y):
        to = worker(home if tick == 0 else section, 2 * y + core)
        copy = remote(
            map_ref,
            map_in.at[tick, slab],
            map_sems,
            (tick, y),
            device(to),
            (tick, slab // 2),
        )
        live = to != me
        return copy, live if tick == 0 else live & is_deep

    def map_arrival(tick, h):
        d = core + 2 * h
        source = owner(chain + tick, d)
        copy = remote(map_ref, map_in.at[tick, d], map_sems, (tick, h), device(source))
        return copy, source != me

    def map_relay(tick, h):
        part = map_in.at[tick, core + 2 * h]
        return remote(part, part, relay_sems, (tick, h), partner)

    def pass_map_on(tick):
        for h in range(2):
            copy, foreign = map_arrival(tick, h)
            pl.when(foreign)(copy.wait_recv)
            pl.when(jnp.logical_not(foreign))(own_map.wait)
            map_relay(tick, h).start()

    def start_map(tick):
        for y in (1, 0):
            copy, live = map_copy(tick, y)
            pl.when(live)(copy.start)

    far = side == 1

    def hop_in(i):
        return pltpu.make_async_remote_copy(
            src_ref=wave_ref.at[i // 2, i % 2],
            dst_ref=hop.at[i // 2, i % 2],
            send_sem=hop_sems.at[0, i],
            recv_sem=hop_sems.at[1, i],
            device_id=device(worker(plane, core)),
            device_id_type=MESH,
        )

    def hop_on(i):
        return remote(
            hop.at[i // 2, i % 2],
            wave_in.at[core, i % 2],
            on_sems,
            (i,),
            device(worker(plane + 1, i // 2)),
            (2 * core + i % 2,),
        )

    def hop_arrival(d, c):
        return remote(
            hop.at[0, c],
            wave_in.at[d, c],
            on_sems,
            (2 * d + c,),
            device(worker(chain, d)),
        )

    start_map(0)

    @pl.when(far)
    def _():
        for i in range(lateral):
            hop_in(i).start()

    for f in range(half, lateral):
        wave_copy(f).start()

    @pl.when(near)
    def _():
        for f in range(half):
            pl.when(worker(home, f) != me)(wave_copy(f).start)
        start_map(1)

    for copy in small:
        copy.wait()
    entry = entries[chain, place]
    angle = pulsations[entry] * slownesses[...]
    cosine, sine = jnp.cos(angle), jnp.sin(angle)
    for k in range(ORDER + 1):
        fr, fi = (weights[entry, k, pl.ds(c, 1), :] for c in range(2))
        rows[pl.ds(k, 1), pl.ds(0, NBIN)] = fr * cosine - fi * sine
        rows[pl.ds(ORDER + 1 + k, 1), pl.ds(0, NBIN)] = fr * sine + fi * cosine
    for n in range(ROWS):
        row = jnp.broadcast_to(rows[pl.ds(n, 1), :], (SUB, LANES))
        for part in range(NBIN // SUB):
            spread_table[part, n] = lane_pick(row, sub + part * SUB)

    def pass_waves_on(some):
        for i in some:
            hop_in(i).wait_recv()
            hop_on(i).start()

    pl.when(near)(lambda: pass_waves_on(range(lateral - 1)))


    def cell(m, r):
        return pl.ds((m * SUB + r) * SUB, SUB)

    def column(m, slot):
        return pl.ds(m * SUB * SUB + slot, SUB, stride=SUB)

    def gather_back(source, d, g):
        return transposed([source[column(m, groups * d + g), :] for m in range(SUB)])

    def tile(g, j):
        return pl.ds(g * SUB, SUB), pl.ds(j * LANES, LANES)

    def spread(load, ref, d):
        for g in range(groups):
            for m, x in enumerate(transposed([load(*tile(g, j)) for j in range(SUB)])):
                ref[column(m, groups * d + g), :] = x

    def fill(tick, level):
        for d in range(lateral):
            spread(lambda row, col: map_in[tick, d, level, row, col], bins, d)
        n_cells = 16

        def some(i, carry):
            for n in range(n_cells):
                where = pl.ds(pl.multiple_of((i * n_cells + n) * SUB, SUB), SUB)
                bin_ = bins[where, :]
                high = bin_ >= SUB
                low_bits = bin_ % SUB
                for row in range(ROWS):
                    a, b = (
                        jnp.take_along_axis(
                            spread_table[part, row],
                            low_bits,
                            axis=0,
                            mode="promise_in_bounds",
                            wrap_negative_indices=False,
                        )
                        for part in range(NBIN // SUB)
                    )
                    coeffs[level, row, where, :] = jnp.where(high, b, a)
            return carry

        lax.fori_loop(0, SUB * SUB // n_cells, some, 0)

    def stencil(present, target, first=False, last=False):
        def channel(c, carry):
            below = []
            for m in range(8):
                edge = pltpu.roll(present[c, cell(m, 7), :], 1, 0)
                edge = jnp.where(not_first_sub, edge, 0.0)
                below.append(edge + present[c, cell(m, 0), :])
            for r in range(8):
                u = []
                for m in range(8):
                    here = present[c, cell(m, r), :]
                    if r < 7:
                        above = present[c, cell(m, r + 1), :]
                    else:
                        above = pltpu.roll(present[c, cell(m, 0), :], SUB - 1, 0)
                        above = jnp.where(not_last_sub, above, 0.0)
                    q = here + above
                    u.append(below[m] + q)
                    below[m] = q
                left = jnp.where(not_first_lane, lane_pick(u[7], to_left), 0.0)
                right = jnp.where(not_last_lane, lane_pick(u[0], to_right), 0.0)
                u = [left] + u + [right]
                h = [u[m] + u[m + 1] for m in range(9)]
                for m in range(8):
                    w = h[m] + h[m + 1]
                    here = present[c, cell(m, r), :]
                    if first:
                        both = 0.125 * w
                    else:
                        both = 0.25 * w - paired_sum[c, cell(m, r), :]
                    if not last:
                        paired_sum[c, cell(m, r), :] = both
                    target[c, cell(m, r), :] = both - here
            return carry

        lax.fori_loop(0, 2, channel, 0)

    def add_orders(tick, level, terms, where, total):
        re, im = (None, None) if total is None else total
        for order, ref in terms:
            tr, ti = (ref[c, where, :] for c in range(2))
            br = coeffs[level, order, where, :]
            bi = coeffs[level, ORDER + 1 + order, where, :]
            dr = br * tr - bi * ti
            di = br * ti + bi * tr
            re, im = (dr, di) if re is None else (re + dr, im + di)
        return re, im

    def sum_so_far(where):
        return [running[c, where, :] for c in range(2)]

    def unit(tick, level, output):
        start = starts.at[tick * LEVELS + level]
        stencil(start, odd, first=True)
        for i in range(SUB * SUB):
            where = pl.ds(i * SUB, SUB)
            total = add_orders(tick, level, [(0, start), (1, odd)], where, None)
            for c in range(2):
                running[c, where, :] = total[c]

        def steps(i, carry):
            stencil(odd, even)
            stencil(even, odd)
            for n in range(SUB * SUB):
                where = pl.ds(n * SUB, SUB)
                terms = [(2 * i + 2, even), (2 * i + 3, odd)]
                total = add_orders(tick, level, terms, where, sum_so_far(where))
                for c in range(2):
                    running[c, where, :] = total[c]
            return carry

        lax.fori_loop(0, ORDER // 2 - 1, steps, 0)
        stencil(odd, even, last=True)
        for i in range(SUB * SUB):
            where = pl.ds(i * SUB, SUB)
            total = add_orders(tick, level, [(ORDER, even)], where, sum_so_far(where))
            for c in range(2):
                output[c, where, :] = total[c]
            raw[tick, level, i] = total[0]

    def slot(n):
        return pl.ds(groups * n, groups)

    def raw_part(tick, level, d):
        return raw.at[tick, level, :, slot(d), :]

    def raw_copy(tick, level, d):
        to = owner(chain + tick, d)
        copy = remote(
            raw_part(tick, level, d),
            raw_in.at[tick, level, place],
            raw_sems,
            (tick, level, d),
            device(to),
            (tick, level, place),
        )
        return copy, to != me

    def own_raw(tick, level):
        return pltpu.make_async_copy(
            raw_part(tick, level, slab),
            raw_in.at[tick, level, place],
            own_raw_sems.at[tick, level],
        )

    def raw_arrival(tick, level, f):
        source = worker(home if tick == 0 else section, f)
        copy = remote(
            raw_part(tick, level, f),
            raw_in.at[tick, level, f],
            raw_sems,
            (tick, level, f),
            device(source),
        )
        return copy, source != me

    def send_raw(tick, level):
        for d in range(lateral):
            copy, foreign = raw_copy(tick, level, d)
            pl.when(foreign)(copy.start)
        pl.when((slab_home == tick))(own_raw(tick, level).start)

    def wave_back(which, d):
        to = owner(chain + which, d)
        copy = remote(
            wave_out.at[which, d],
            handed_ref.at[place],
            fin_sems,
            (which, d),
            device(to),
            (1, place),
        )
        return copy, to != me

    def own_back(which):
        return pltpu.make_async_copy(
            wave_out.at[which, slab], handed_ref.at[place], own_sems.at[0]
        )

    def handed_arrival(f):
        source = worker(jnp.maximum(section, 1), f)
        copy = remote(
            wave_out.at[1, f], handed_ref.at[f], fin_sems, (1, f), device(source)
        )
        return copy, source != me

    def send_wave(which, source):
        for d in range(lateral):
            for c in range(2):
                for g in range(groups):
                    for j, x in enumerate(gather_back(source.at[c], d, g)):
                        wave_out[(which, d, c) + tile(g, j)] = x
            copy, foreign = wave_back(which, d)
            pl.when(foreign)(copy.start)
            pl.when(jnp.logical_not(foreign))(own_back(which).start)

    pass_map_on(0)
    for h in range(2):
        map_relay(0, h).wait_recv()
    pl.when(far)(lambda: start_map(1))
    fill(0, 0)
    pl.when(near)(lambda: pass_waves_on((lateral - 1,)))
    fill(0, 1)
    def take_waves(order):
        for d in order:
            foreign = owner(chain, d) != me
            pl.when(foreign)(wave_arrival(d).wait_recv)
            pl.when(jnp.logical_not(foreign))(own_wave.wait)
            for c in range(2):
                spread(lambda row, col: wave_in[d, c, row, col], starts.at[0, c], d)

    @pl.when(near)
    def _():
        take_waves((2, 3))
        for d in range(half):
            for c in range(2):
                hop_arrival(d, c).wait_recv()
                spread(lambda row, col: wave_in[d, c, row, col], starts.at[0, c], d)

    pl.when(far)(lambda: take_waves((0, 1, 2, 3)))
    unit(0, 0, starts.at[1])
    send_raw(0, 0)
    pl.when(has_next)(lambda: pass_map_on(1))
    unit(0, 1, starts.at[2])
    send_raw(0, 1)

    @pl.when(chain == 0)
    def _():
        send_wave(0, starts.at[2])

    @pl.when(has_next)
    def _():
        for h in range(2):
            map_relay(1, h).wait_recv()
        fill(1, 0)
        fill(1, 1)
        unit(1, 0, starts.at[3])
        send_raw(1, 0)
        unit(1, 1, last)
        send_raw(1, 1)
        send_wave(1, last)

    for level in range(LEVELS):
        for tick in range(TICKS):
            for f in range(lateral):
                copy, foreign = raw_arrival(tick, level, f)
                own = jnp.logical_not(foreign)
                if tick == 1:
                    foreign, own = foreign & is_deep, own & is_deep
                pl.when(foreign)(copy.wait_recv)
                pl.when(own)(own_raw(tick, level).wait)
        total = jnp.zeros((groups, LANES), jnp.float32)
        for i in range(SUB * SUB):
            value = second = None
            for f in range(lateral):
                a, b = (raw_in[t, level, f, i] for t in range(TICKS))
                value = a if value is None else value + a
                second = b if second is None else second + b
            value = value + jnp.where(is_deep, second, 0.0)
            summed[level, pl.ds(i * groups, groups), :] = value
            total = total + value * value
        sum_own[pl.ds(level * SUB, groups), :] = total
        sum_own[pl.ds(level * SUB + groups, SUB - groups), :] = jnp.zeros(
            (SUB - groups, LANES), jnp.float32
        )

    def sum_copy(x):
        mate = lax.rem(slab + x, lateral)
        return remote(sum_own, sum_in.at[x], sum_sems, (x,), device(owner(section, mate)))

    for x in range(1, lateral):
        sum_copy(x).start()
    for tick in range(TICKS):
        for y in range(2):
            copy, live = map_copy(tick, y)
            pl.when(live)(copy.wait_send)
    for h in range(2):
        map_relay(0, h).wait_send()
        pl.when(has_next)(map_relay(1, h).wait_send)
    for n in range(lateral):
        if n < half:
            pl.when(near & (worker(home, n) != me))(wave_copy(n).wait_send)
        else:
            wave_copy(n).wait_send()
        pl.when(near)(hop_on(n).wait_send)
        pl.when(far)(hop_in(n).wait_send)
        for which, live in ((0, chain == 0), (1, has_next)):
            copy, foreign = wave_back(which, n)
            pl.when(foreign & live)(copy.wait_send)
        for level in range(LEVELS):
            for tick in range(TICKS):
                copy, foreign = raw_copy(tick, level, n)
                pl.when(foreign if tick == 0 else foreign & has_next)(copy.wait_send)
    for level in range(LEVELS):
        for g in range(groups):
            part = [
                summed[level, pl.ds(m * SUB * groups + g, SUB, stride=groups), :]
                for m in range(SUB)
            ]
            for j, x in enumerate(transposed(part)):
                image_ref[(level,) + tile(g, j)] = x
    total = sum_own[...]
    for x in range(1, lateral):
        sum_copy(x).wait_recv()
        total = total + sum_in[x]
    cells = length * lateral * SUB * LANES
    for level in range(LEVELS):
        mean = (
            jnp.sum(total[level * SUB : (level + 1) * SUB], axis=(0, 1), keepdims=True) / cells
        )
        scale = jnp.broadcast_to(1.0 / jnp.sqrt(mean + 1e-06), (SUB, LANES))
        for g in range(groups):
            for j in range(SUB):
                where = (level,) + tile(g, j)
                image_ref[where] = image_ref[where] * scale
    for f in range(lateral):
        copy, foreign = handed_arrival(f)
        pl.when(foreign)(copy.wait_recv)
        pl.when(jnp.logical_not(foreign))(own_back(0).wait)
    for x in range(1, lateral):
        sum_copy(x).wait_send()


def phase_table(filter_weights, scaled_pulsations, inverse_speed_classes):
    angle = scaled_pulsations[:, None] * inverse_speed_classes[None, :]
    cosine = jnp.cos(angle)[:, None, :]
    sine = jnp.sin(angle)[:, None, :]
    by_order = jnp.transpose(filter_weights, (2, 0, 3, 1))
    real = by_order[0] * cosine - by_order[1] * sine
    imag = by_order[0] * sine + by_order[1] * cosine
    table = jnp.stack([real, imag], axis=2).reshape(NW, 2 * (ORDER + 1), NBIN)
    return jnp.pad(table, ((0, 0), (0, 0), (0, LANES - NBIN)))


def chains(
    incoming_wave,
    speed_class_map,
    spectral_entry_index,
    filter_weights,
    scaled_pulsations,
    inverse_speed_classes,
):
    count = lax.axis_size("strip")
    lateral = count // SECTIONS
    length, across = incoming_wave.shape[2:]
    tall = length * lateral * SUB
    f32 = jnp.float32
    vmem = pl.BlockSpec(memory_space=pltpu.VMEM)
    anywhere = pl.BlockSpec(memory_space=pl.ANY)
    def dma(*shape):
        return pltpu.SemaphoreType.DMA((2,) + shape)

    return pl.pallas_call(
        functools.partial(chain_kernel, count),
        out_shape=(
            jax.ShapeDtypeStruct(speed_class_map.shape, f32),
            jax.ShapeDtypeStruct(incoming_wave.shape, f32),
        ),
        in_specs=[anywhere] * 6,
        out_specs=(vmem, vmem),
        scratch_shapes=[
            pltpu.SMEM(spectral_entry_index.shape, jnp.int32),
            pltpu.SMEM((NW,), f32),
            pltpu.VMEM((1, NBIN), f32),
            pltpu.VMEM((NW, ORDER + 1, 2, NBIN), f32),
            pltpu.VMEM((ROWS, LANES), f32),
            pltpu.VMEM((lateral // 2, 2, length, across), f32),
            pltpu.VMEM((TICKS * LEVELS, 2, tall, LANES), f32),
            pltpu.VMEM((2, tall, LANES), f32),
            pltpu.VMEM((2, tall, LANES), f32),
            pltpu.VMEM((2, tall, LANES), f32),
            pltpu.VMEM((2, tall, LANES), f32),
            pltpu.VMEM((2, tall, LANES), f32),
            pltpu.VMEM((LEVELS, ROWS, tall, LANES), f32),
            pltpu.VMEM((NBIN // SUB, ROWS, SUB, LANES), f32),
            pltpu.VMEM((lateral, 2, length, across), f32),
            pltpu.VMEM((TICKS, lateral, LEVELS, length, across), jnp.int32),
            pltpu.VMEM((tall, LANES), jnp.int32),
            pltpu.VMEM((TICKS, LEVELS, SUB * SUB, SUB, LANES), f32),
            pltpu.VMEM((2, lateral, 2, length, across), f32),
            pltpu.VMEM((LEVELS, SUB * SUB * length // SUB, LANES), f32),
            pltpu.VMEM((TICKS, LEVELS, lateral, SUB * SUB, length // SUB, LANES), f32),
            pltpu.VMEM((LEVELS * SUB, LANES), f32),
            pltpu.VMEM((lateral, LEVELS * SUB, LANES), f32),
            pltpu.SemaphoreType.DMA((4,)),
            dma(lateral),
            dma(lateral),
            dma(lateral),
            dma(TICKS, 2),
            dma(TICKS, 2),
            dma(2, lateral),
            dma(TICKS, LEVELS, lateral),
            dma(lateral),
            pltpu.SemaphoreType.DMA((2,)),
            pltpu.SemaphoreType.DMA((TICKS, LEVELS)),
        ],
        compiler_params=pltpu.CompilerParams(
            collective_id=0, has_side_effects=True, vmem_limit_bytes=32 * 1024 * 1024
        ),
    )(
        *(
            pltpu.with_memory_space_constraint(x, pltpu.HBM)
            for x in (
                spectral_entry_index,
                scaled_pulsations,
                inverse_speed_classes[None],
                jnp.transpose(filter_weights, (0, 3, 2, 1)),
                incoming_wave,
                speed_class_map,
            )
        )
    )


def fits(mesh):
    lateral = mesh.shape["strip"] // SECTIONS
    return NFREQ % 2 == 0 and lateral % 4 == 0


def whole_section(mesh, wave):
    lateral = mesh.shape["strip"] // SECTIONS
    full = lateral * wave.shape[2] == SUB * SUB and wave.shape[3] == SUB * LANES
    return lateral == NFREQ == 4 and wave.shape[2] % SUB == 0 and full


def body_for(mesh):
    def body(wave, *rest):
        whole = wave.shape[3] == SUB * LANES and wave.shape[2] % SUB == 0
        if whole_section(mesh, wave):
            return chains(wave, *rest)
        if fits(mesh) and whole and wave.shape[2] >= ORDER:
            return paired(wave, *rest)
        return shards(wave, *rest)

    return body


def solution(mesh):
    return jax.shard_map(
        body_for(mesh),
        mesh=mesh,
        in_specs=(
            P("groups", None, "strip", None),
            P("groups", "strip", None),
            P("groups", None),
            P(),
            P(),
            P(),
        ),
        out_specs=(P("groups", "strip", None), P("groups", None, "strip", None)),
        check_vma=False,
    )
```

```python
import functools
import jax
import jax.numpy as jnp
from jax import lax
from jax.experimental import pallas as pl
from jax.experimental.pallas import tpu as pltpu
from jax.sharding import PartitionSpec as P

SECTIONS = 4
LEVELS = 2
ORDER = 12
NFREQ = 4
NBIN = 16
NW = 16


def extended_2(shard, sides, width):
    for axis, dim in sides:
        devices, length = (lax.axis_size(axis), shard.shape[dim])
        up = [(i, (i + 1) % devices) for i in range(devices)]
        down = [(j, i) for i, j in up]
        last = lax.slice_in_dim(shard, length - width, length, axis=dim)
        initial = lax.slice_in_dim(shard, 0, width, axis=dim)
        before = lax.ppermute(last, axis, up)
        after = lax.ppermute(initial, axis, down)
        shard = jnp.concatenate([before, shard, after], axis=dim)
    return shard


def from_behind(shard, axis, by):
    devices = lax.axis_size(axis)
    return lax.ppermute(shard, axis, [(i, (i + by) % devices) for i in range(devices)])


def stencil_padded(padded):
    vertical = padded[:, :, :-2, :] + padded[:, :, 2:, :]
    middle = padded[:, :, 1:-1, :]
    return (
        -0.5 * middle[..., 1:-1]
        + 0.25 * (vertical[..., 1:-1] + middle[..., :-2] + middle[..., 2:])
        + 0.125 * (vertical[..., :-2] + vertical[..., 2:])
    )


def complex_times(coeff, field):
    real_part = coeff[:, 0] * field[:, 0] - coeff[:, 1] * field[:, 1]
    imag_part = coeff[:, 0] * field[:, 1] + coeff[:, 1] * field[:, 0]
    return jnp.stack([real_part, imag_part], axis=1)


def shards(
    incoming_wave,
    speed_class_map,
    spectral_entry_index,
    filter_weights,
    scaled_pulsations,
    inverse_speed_classes,
):
    highest = lax.Precision.HIGHEST
    summed_along = incoming_wave.shape[2]
    summed_across = incoming_wave.shape[3]
    strip_count = lax.axis_size("strip")
    lateral_count = strip_count // SECTIONS
    position = (lax.axis_index("strip") - lateral_count // 2) % strip_count
    vertical_slab = position // lateral_count
    lateral_place = position % lateral_count
    section_rows = summed_along * lateral_count
    section_cells = section_rows * summed_across
    margin = ORDER
    extended_rows = summed_along + 2 * margin
    lateral_rows = (
        lateral_place * summed_along - margin + jnp.arange(extended_rows, dtype=jnp.int32)
    )
    inside = ((lateral_rows >= 0) & (lateral_rows < section_rows)).astype(jnp.float32)[
        None, None, :, None
    ]

    def mcclellan_step(field):
        padded = jnp.pad(field, ((0, 0), (0, 0), (1, 1), (0, 0)))
        padded = jnp.pad(padded, ((0, 0), (0, 0), (0, 0), (1, 1)))
        result = stencil_padded(padded)
        result = result * inside
        return result

    def interior(field):
        return field[:, :, margin : margin + summed_along, :]

    def image_downward(field, batch_index):
        freq_row = lax.dynamic_index_in_dim(spectral_entry_index, batch_index, 0, keepdims=False)
        freq_select = (freq_row[:, None] == jnp.arange(NW, dtype=jnp.int32)[None, :]).astype(
            jnp.float32
        )
        freq_coeffs = jnp.einsum("fw,wbck->fbck", freq_select, filter_weights, precision=highest)
        freq_omega = jnp.dot(freq_select, scaled_pulsations, precision=highest)
        wavefield = field
        raws = []
        for level in range(LEVELS):
            cells = speed_class_map[level].reshape(-1)
            bin_onehot = (cells[None, :] == jnp.arange(NBIN, dtype=jnp.int32)[:, None]).astype(
                jnp.float32
            )
            cell_slowness = jnp.dot(inverse_speed_classes, bin_onehot, precision=highest).reshape(
                summed_along, summed_across
            )
            table = jnp.einsum("fbck,bn->kfcn", freq_coeffs, bin_onehot, precision=highest).reshape(
                ORDER + 1, NFREQ, 2, summed_along, summed_across
            )
            extended = extended_2(wavefield, (("strip", 2),), ORDER) * inside
            previous = extended
            current = mcclellan_step(extended)
            accumulated = complex_times(table[0], interior(previous)) + complex_times(
                table[1], interior(current)
            )

            def recursion_step(order_index, state_tuple):
                before, present, running = state_tuple
                following = 2.0 * mcclellan_step(present) - before
                coeff = lax.dynamic_index_in_dim(table, order_index, 0, keepdims=False)
                running = running + complex_times(coeff, interior(following))
                return (present, following, running)

            previous, current, accumulated = lax.fori_loop(
                2, ORDER + 1, recursion_step, (previous, current, accumulated)
            )
            phase_angle = freq_omega[:, None, None] * cell_slowness[None]
            cosine = jnp.cos(phase_angle)
            sine_part = jnp.sin(phase_angle)
            real_part = accumulated[:, 0] * cosine - accumulated[:, 1] * sine_part
            imag_part = accumulated[:, 0] * sine_part + accumulated[:, 1] * cosine
            wavefield = jnp.stack([real_part, imag_part], axis=1)
            raws.append(jnp.sum(real_part, axis=0))
        return (wavefield, raws)

    above_floor_lines, above_unscaled_waves = image_downward(incoming_wave, vertical_slab)
    arriving = from_behind(above_floor_lines, "strip", lateral_count)
    second_bottom, second_raws = image_downward(arriving, jnp.maximum(vertical_slab - 1, 0))
    handed = jnp.where(vertical_slab == 0, above_floor_lines, second_bottom)
    first_section = (vertical_slab > 0).astype(jnp.float32)
    totals = [
        above_unscaled_waves[level] + first_section * second_raws[level] for level in range(LEVELS)
    ]
    selector = (jnp.arange(SECTIONS, dtype=jnp.int32) == vertical_slab).astype(jnp.float32)
    images = []
    for level in range(LEVELS):
        raw_image = totals[level]
        spread = lax.psum(selector * jnp.sum(raw_image * raw_image), "strip")
        mean_square = jnp.sum(spread * selector) / section_cells
        images.append(raw_image / jnp.sqrt(mean_square + 1e-06))
    return (jnp.stack(images, axis=0), handed)


SUB = 8
LANES = 128
PAD = 5
UNROLL = 8
TOGETHER = 4
MESH = pl.DeviceIdType.MESH


def at_row(row):
    return pl.ds(pl.multiple_of(row * SUB, SUB), SUB)


def kernel(
    strip_count,
    entry_ref,
    wave_ref,
    map_ref,
    table_ref,
    image_ref,
    handed_ref,
    starts,
    work,
    bottom,
    last,
    last_in,
    wave_out,
    map_out,
    map_all,
    raw,
    raw_in,
    sum_own,
    sum_in,
    swap_sems,
    halo_sems,
    hand_sems,
    fin_sems,
    raw_sems,
    sum_sems,
):
    nfh = wave_ref.shape[0] // 2
    length = wave_ref.shape[2]
    rows = 2 * length
    blocks = wave_ref.shape[3] // LANES
    lateral = strip_count // SECTIONS
    shift = lateral // 2
    pairs = lateral // 2
    margin = ORDER
    first = PAD + margin
    me = lax.axis_index("strip")
    position = lax.rem(me + strip_count - shift, strip_count)
    section = position // lateral
    place = lax.rem(position, lateral)
    pair = place // 2
    half = lax.rem(place, 2)
    up = jnp.where(pair > 0, 1, 0)
    down = jnp.where(pair < pairs - 1, 1, 0)
    has_up = pair > 0
    has_down = pair < pairs - 1
    has_before = section > 0
    has_after = section < SECTIONS - 1
    other = 1 - half

    def device(pos):
        return {"strip": lax.rem(pos + shift + strip_count, strip_count)}

    partner = device(position + 1 - 2 * half)
    upper = device(position - 2)
    lower = device(position + 2)
    deeper = device(position + lateral)
    shallower = device(position + strip_count - lateral)

    def remote(src, dst, sems, index, target):
        return pltpu.make_async_remote_copy(
            src_ref=src,
            dst_ref=dst,
            send_sem=sems.at[(0,) + index],
            recv_sem=sems.at[(1,) + index],
            device_id=target,
            device_id_type=MESH,
        )

    def span(row, count):
        return pl.ds(pl.multiple_of(row * SUB, SUB), count * SUB)

    zero = jnp.zeros((SUB, LANES), jnp.float32)
    for edge in (first - 1, first + rows):
        for f in range(nfh):
            for c in range(2):
                for s in range(2 * LEVELS):
                    starts[s, f, c, at_row(edge), :] = zero
        for c in range(2):
            for k in range(ORDER):
                work[k, c, at_row(edge), :] = zero

    barrier = pltpu.get_barrier_semaphore()
    for d in range(1, lateral):
        mate = device(section * lateral + lax.rem(place + d, lateral))
        pl.semaphore_signal(barrier, inc=1, device_id=mate, device_id_type=MESH)
    for target in (deeper, shallower):
        pl.semaphore_signal(barrier, inc=1, device_id=target, device_id_type=MESH)

    def rearrange(load, store):
        for g in range(length // SUB):
            for j in range(blocks):
                store(g, j, load(g, j))

    def strided(row, g, j):
        return pl.ds((row + g * SUB) * SUB + j, SUB, stride=SUB)

    own_row = half * length
    swaps = []
    for f in range(nfh):
        for c in range(2):
            rearrange(
                lambda g, j: wave_ref[other * nfh + f, c, pl.ds(g * SUB, SUB), pl.ds(j * LANES, LANES)],
                lambda g, j, x: pltpu_store(wave_out.at[f, c], strided(0, g, j), x),
            )
        if f == 0:
            pl.semaphore_wait(barrier, lateral + 1)
        copy = remote(
            wave_out.at[f],
            starts.at[0, f, :, span(first + own_row, length), :],
            swap_sems,
            (f,),
            partner,
        )
        copy.start()
        swaps.append(copy)
    for l in range(LEVELS):
        rearrange(
            lambda g, j: map_ref[l, pl.ds(g * SUB, SUB), pl.ds(j * LANES, LANES)],
            lambda g, j, x: pltpu_store(map_out.at[l], strided(0, g, j), x),
        )
    copy = remote(
        map_out, map_all.at[:, span(own_row, length), :], swap_sems, (nfh,), partner
    )
    copy.start()
    swaps.append(copy)
    for f in range(nfh):
        for c in range(2):
            rearrange(
                lambda g, j: wave_ref[half * nfh + f, c, pl.ds(g * SUB, SUB), pl.ds(j * LANES, LANES)],
                lambda g, j, x: pltpu_store(
                    starts.at[0, f, c], strided(first + own_row, g, j), x
                ),
            )
    for l in range(LEVELS):
        rearrange(
            lambda g, j: map_ref[l, pl.ds(g * SUB, SUB), pl.ds(j * LANES, LANES)],
            lambda g, j, x: pltpu_store(map_all.at[l], strided(own_row, g, j), x),
        )

    def halo_up(stage, f):
        ref = starts.at[stage, f]
        return remote(
            ref.at[:, span(first, margin), :],
            ref.at[:, span(first + rows, margin), :],
            halo_sems,
            (stage, f, 0),
            upper,
        )

    def halo_down(stage, f):
        ref = starts.at[stage, f]
        return remote(
            ref.at[:, span(first + rows - margin, margin), :],
            ref.at[:, span(first - margin, margin), :],
            halo_sems,
            (stage, f, 1),
            lower,
        )

    def send_halo(stage, f):
        pl.when(has_up)(lambda: halo_up(stage, f).start())
        pl.when(has_down)(lambda: halo_down(stage, f).start())

    def wait_halo(stage, f):
        pl.when(has_down)(lambda: halo_up(stage, f).wait_recv())
        pl.when(has_up)(lambda: halo_down(stage, f).wait_recv())

    def hand_parts(f):
        parts = ((0, margin), (rows - margin, margin), (margin, rows - 2 * margin))
        return [
            remote(
                bottom.at[f, :, span(row, count), :],
                starts.at[LEVELS, f, :, span(first + row, count), :],
                hand_sems,
                (f, n),
                deeper,
            )
            for n, (row, count) in enumerate(parts)
        ]

    lane = lax.broadcasted_iota(jnp.int32, (SUB, LANES), 1)
    sub = lax.broadcasted_iota(jnp.int32, (SUB, LANES), 0)
    at_first = lane == 0
    at_last = lane == LANES - 1
    keep_first = sub > 0
    keep_last = sub < SUB - 1

    def across(u):
        right = pltpu.roll(u, 1, 1)
        right_fix = jnp.where(keep_first, pltpu.roll(right, 1, 0), 0.0)
        left = pltpu.roll(u, LANES - 1, 1)
        left_fix = jnp.where(keep_last, pltpu.roll(left, SUB - 1, 0), 0.0)
        return jnp.where(at_first, right_fix, right) + jnp.where(at_last, left_fix, left)

    def reach(k):
        return ((margin - k + UNROLL - 1) // UNROLL) * UNROLL

    def apply(k, present, before, target):
        extra = reach(k)
        low = first - up * extra
        count = (rows + (up + down) * extra) // UNROLL

        def block(i, carry):
            base = low + i * UNROLL
            v = [
                [present[c, at_row(base - 1 + n), :] for n in range(UNROLL + 2)]
                for c in range(2)
            ]
            old = None
            if before is not None:
                old = [
                    [before[c, at_row(base + n), :] for n in range(UNROLL)] for c in range(2)
                ]
            values = []
            for c in range(2):
                q = [v[c][n] + v[c][n + 1] for n in range(UNROLL + 1)]
                for n in range(UNROLL):
                    u = q[n] + q[n + 1]
                    w = across(u) + (u + u)
                    centre = v[c][n + 1]
                    if old is None:
                        value = 0.125 * w - centre
                    else:
                        value = 0.25 * w - (centre + centre + old[c][n])
                    values.append(value)
            for c in range(2):
                for n in range(UNROLL):
                    target[c, at_row(base + n), :] = values[c * UNROLL + n]
            return carry

        lax.fori_loop(0, count, block, 0)

    def unit(tick, level, f, meanwhile=None):
        stage = tick * LEVELS + level
        start = starts.at[stage, f]
        apply(1, start, None, work.at[0])
        apply(2, work.at[0], start, work.at[1])

        def step(k, carry):
            apply(k, work.at[k - 2], work.at[k - 3], work.at[k - 1])
            return carry

        lax.fori_loop(3, ORDER + 1, step, 0)
        if meanwhile is not None:
            meanwhile()
        batch = section if tick == 0 else jnp.maximum(section - 1, 0)
        entry = entry_ref[batch, half * nfh + f]

        def combine(i, carry):
            spots = [TOGETHER * i + n for n in range(TOGETHER)]
            bins = [map_all[level, at_row(r), :] for r in spots]
            real = [None] * TOGETHER
            imag = [None] * TOGETHER
            for n, r in enumerate(spots):
                for k in range(ORDER + 1):
                    cr, ci = (
                        jnp.take_along_axis(
                            jnp.broadcast_to(
                                table_ref[entry, pl.ds(2 * k + c, 1), :], (SUB, LANES)
                            ),
                            bins[n],
                            axis=1,
                            mode="promise_in_bounds",
                        )
                        for c in range(2)
                    )
                    source = start if k == 0 else work.at[k - 1]
                    tr = source[0, at_row(first + r), :]
                    ti = source[1, at_row(first + r), :]
                    re = cr * tr - ci * ti
                    im = cr * ti + ci * tr
                    real[n] = re if k == 0 else real[n] + re
                    imag[n] = im if k == 0 else imag[n] + im
            for n, r in enumerate(spots):
                re, im = real[n], imag[n]
                if tick == 0 and f == 0:
                    raw[level, at_row(r), :] = re
                else:
                    part = re if tick == 0 else jnp.where(has_before, re, 0.0)
                    raw[level, at_row(r), :] = raw[level, at_row(r), :] + part
                for c, value in enumerate((re, im)):
                    if level < LEVELS - 1:
                        starts[stage + 1, f, c, at_row(first + r), :] = value
                    elif tick == 0:
                        bottom[f, c, at_row(r), :] = value
                    else:
                        last[f, c, at_row(r), :] = jnp.where(
                            has_before, value, bottom[f, c, at_row(r), :]
                        )
            return carry

        lax.fori_loop(0, rows // TOGETHER, combine, 0)

    def finish_wave(f):
        return remote(
            last.at[f, :, span(other * length, length), :],
            last_in.at[f],
            fin_sems,
            (f,),
            partner,
        )

    def finish_raw(l):
        return remote(
            raw.at[l, span(other * length, length), :], raw_in.at[l], raw_sems, (l,), partner
        )

    for f in range(nfh):
        swaps[f].wait_recv()
        send_halo(0, f)
    swaps[nfh].wait_recv()
    for level in range(LEVELS):
        for f in range(nfh):
            wait_halo(level, f)
            unit(0, level, f)
            if level < LEVELS - 1:
                send_halo(level + 1, f)
            else:

                @pl.when(has_after)
                def _():
                    for copy in hand_parts(f):
                        copy.start()

    def forward(f):
        @pl.when(has_before)
        def _():
            high, low, mid = hand_parts(f)
            high.wait_recv()
            pl.when(has_up)(lambda: halo_up(LEVELS, f).start())
            low.wait_recv()
            pl.when(has_down)(lambda: halo_down(LEVELS, f).start())
            mid.wait_recv()

    def skip_or(fn):
        pl.when(has_before)(fn)

    forward(0)
    for level in range(LEVELS):
        for f in range(nfh):

            @pl.when(has_before)
            def _():
                wait_halo(LEVELS + level, f)

            later = f + 1 if level == 0 and f + 1 < nfh else None
            unit(1, level, f, None if later is None else lambda: forward(later))
            if level < LEVELS - 1:

                @pl.when(has_before)
                def _():
                    send_halo(LEVELS + level + 1, f)

            else:
                finish_wave(f).start()
        finish_raw(level).start()

    for l in range(LEVELS):
        finish_raw(l).wait_recv()

        def merge(i, carry):
            value = raw[l, at_row(own_row + i), :] + raw_in[l, at_row(i), :]
            raw_in[l, at_row(i), :] = value
            return carry + value * value

        sum_own[pl.ds(l * SUB, SUB), :] = lax.fori_loop(0, length, merge, zero)
    for d in range(1, lateral):
        mate = device(section * lateral + lax.rem(place + d, lateral))
        remote(sum_own, sum_in.at[d], sum_sems, (d,), mate).start()

    for f in range(nfh):
        for c in range(2):
            rearrange(
                lambda g, j: last[f, c, strided(own_row, g, j), :],
                lambda g, j, x: out_store(handed_ref, half * nfh + f, c, g, j, x),
            )
    for f in range(nfh):
        finish_wave(f).wait_recv()
        for c in range(2):
            rearrange(
                lambda g, j: last_in[f, c, strided(0, g, j), :],
                lambda g, j, x: out_store(handed_ref, other * nfh + f, c, g, j, x),
            )

    total = sum_own[...]
    for d in range(1, lateral):
        mate = device(section * lateral + lax.rem(place + d, lateral))
        remote(sum_own, sum_in.at[d], sum_sems, (d,), mate).wait_recv()
        total = total + sum_in[d]
    cells = length * lateral * blocks * LANES
    for l in range(LEVELS):
        mean = jnp.sum(total[l * SUB : (l + 1) * SUB], axis=(0, 1), keepdims=True) / cells
        scale = jnp.broadcast_to(1.0 / jnp.sqrt(mean + 1e-06), (SUB, LANES))

        def put(g, j, x):
            image_ref[l, pl.ds(g * SUB, SUB), pl.ds(j * LANES, LANES)] = x * scale

        rearrange(lambda g, j: raw_in[l, strided(0, g, j), :], put)

    for copy in swaps:
        copy.wait_send()
    for f in range(nfh):
        send_done = lambda make, stage: make(stage, f).wait_send()
        for stage in range(2 * LEVELS):
            live_up = has_up if stage < LEVELS else has_up & has_before
            live_down = has_down if stage < LEVELS else has_down & has_before
            pl.when(live_up)(lambda: send_done(halo_up, stage))
            pl.when(live_down)(lambda: send_done(halo_down, stage))

        @pl.when(has_after)
        def _():
            for copy in hand_parts(f):
                copy.wait_send()

        finish_wave(f).wait_send()
    for l in range(LEVELS):
        finish_raw(l).wait_send()
    for d in range(1, lateral):
        mate = device(section * lateral + lax.rem(place + d, lateral))
        remote(sum_own, sum_in.at[d], sum_sems, (d,), mate).wait_send()


def pltpu_store(ref, where, x):
    ref[where, :] = x


def out_store(ref, f, c, g, j, x):
    ref[f, c, pl.ds(g * SUB, SUB), pl.ds(j * LANES, LANES)] = x


def paired(
    incoming_wave,
    speed_class_map,
    spectral_entry_index,
    filter_weights,
    scaled_pulsations,
    inverse_speed_classes,
):
    strip_count = lax.axis_size("strip")
    lateral = strip_count // SECTIONS
    length = incoming_wave.shape[2]
    nfh = NFREQ // 2
    rows = 2 * length
    tall = (rows + 2 * ORDER + 2 * PAD) * SUB
    table = phase_table(filter_weights, scaled_pulsations, inverse_speed_classes)
    f32 = jnp.float32
    vmem = pl.BlockSpec(memory_space=pltpu.VMEM)

    def dma(*shape):
        return pltpu.SemaphoreType.DMA((2,) + shape)

    return pl.pallas_call(
        functools.partial(kernel, strip_count),
        out_shape=(
            jax.ShapeDtypeStruct(speed_class_map.shape, f32),
            jax.ShapeDtypeStruct(incoming_wave.shape, f32),
        ),
        in_specs=[pl.BlockSpec(memory_space=pltpu.SMEM), vmem, vmem, vmem],
        out_specs=(vmem, vmem),
        scratch_shapes=[
            pltpu.VMEM((2 * LEVELS, nfh, 2, tall, LANES), f32),
            pltpu.VMEM((ORDER, 2, tall, LANES), f32),
            pltpu.VMEM((nfh, 2, rows * SUB, LANES), f32),
            pltpu.VMEM((nfh, 2, rows * SUB, LANES), f32),
            pltpu.VMEM((nfh, 2, length * SUB, LANES), f32),
            pltpu.VMEM((nfh, 2, length * SUB, LANES), f32),
            pltpu.VMEM((LEVELS, length * SUB, LANES), jnp.int32),
            pltpu.VMEM((LEVELS, rows * SUB, LANES), jnp.int32),
            pltpu.VMEM((LEVELS, rows * SUB, LANES), f32),
            pltpu.VMEM((LEVELS, length * SUB, LANES), f32),
            pltpu.VMEM((LEVELS * SUB, LANES), f32),
            pltpu.VMEM((lateral, LEVELS * SUB, LANES), f32),
            dma(nfh + 1),
            dma(2 * LEVELS, nfh, 2),
            dma(nfh, 3),
            dma(nfh),
            dma(LEVELS),
            dma(lateral),
        ],
        compiler_params=pltpu.CompilerParams(
            collective_id=0, has_side_effects=True, vmem_limit_bytes=48 * 1024 * 1024
        ),
    )(spectral_entry_index, incoming_wave, speed_class_map, table)


ROWS = 2 * (ORDER + 1)
TICKS = 2


def lane_pick(x, index):
    return jnp.take_along_axis(
        x, index, axis=1, mode="promise_in_bounds", wrap_negative_indices=False
    )


def transposed(x):
    lane = lax.broadcasted_iota(jnp.int32, (SUB, LANES), 1)
    low = lane % SUB
    bits = [(step, (lane // step) % 2 == 1) for step in (1, 2, 4)]
    x = list(x)
    for step, bit in bits:
        x = [jnp.where(bit, x[(a + step) % SUB], x[a]) for a in range(SUB)]
    for a in range(1, SUB):
        x[a] = lane_pick(x[a], lane - low + (low + SUB - a) % SUB)
    x = [x[-n % SUB] for n in range(SUB)]
    for step, bit in bits:
        x = [jnp.where(bit, x[(m - step) % SUB], x[m]) for m in range(SUB)]
    return x


def chain_kernel(
    count,
    entry_ref,
    pulsation_ref,
    slowness_ref,
    weight_ref,
    wave_ref,
    map_ref,
    image_ref,
    handed_ref,
    entries,
    pulsations,
    slownesses,
    weights,
    rows,
    hop,
    starts,
    last,
    even,
    odd,
    paired_sum,
    running,
    coeffs,
    spread_table,
    wave_in,
    map_in,
    bins,
    raw,
    wave_out,
    summed,
    raw_in,
    sum_own,
    sum_in,
    small_sems,
    wave_sems,
    hop_sems,
    on_sems,
    map_sems,
    relay_sems,
    back_sent,
    back_got,
    raw_sent,
    raw_got,
    sum_sems,
    own_sems,
):
    length = wave_ref.shape[2]
    groups = length // SUB
    lateral = count // SECTIONS
    half = lateral // 2
    me = lax.axis_index("strip")
    plane = me // lateral
    place = lax.rem(me, lateral)
    side = place // 2
    core = lax.rem(place, 2)
    chain = lax.rem(plane + SECTIONS - 1, SECTIONS)
    section = lax.rem(chain + side, SECTIONS)
    slab = lax.rem(place + half, lateral)
    home = lax.rem(section + 1, SECTIONS)
    near = side == 0
    slab_home = side
    has_next = chain < SECTIONS - 1
    is_deep = section > 0

    def wrapped(index):
        return lax.rem(index + count, count)

    def device(index):
        return {"strip": wrapped(index)}

    def worker(plane_, f):
        return wrapped(plane_ * lateral + f)

    def owner(section_, d):
        return wrapped(section_ * lateral + half + d)

    partner = device(me + 1 - 2 * core)

    def remote(src, dst, sems, index, target, arrival=None):
        return pltpu.make_async_remote_copy(
            src_ref=src,
            dst_ref=dst,
            send_sem=sems.at[(0,) + index],
            recv_sem=sems.at[(1,) + (index if arrival is None else arrival)],
            device_id=target,
            device_id_type=MESH,
        )

    barrier = pltpu.get_barrier_semaphore()
    base = (plane - 1) * lateral
    for n in range(3 * lateral):
        mate = wrapped(base + n)

        @pl.when(mate != me)
        def _():
            pl.semaphore_signal(barrier, inc=1, device_id=device(mate), device_id_type=MESH)

    small = [
        pltpu.make_async_copy(source, target, small_sems.at[n])
        for n, (source, target) in enumerate(
            (
                (entry_ref, entries),
                (pulsation_ref, pulsations),
                (slowness_ref, slownesses),
                (weight_ref, weights),
            )
        )
    ]
    for copy in small:
        copy.start()
    own_wave = pltpu.make_async_copy(wave_ref.at[place], wave_in.at[slab], own_sems.at[0])
    own_map = pltpu.make_async_copy(map_ref, map_in.at[side, slab], own_sems.at[1])
    pl.when(near)(own_wave.start)
    pl.when(near | has_next)(own_map.start)

    lane = lax.broadcasted_iota(jnp.int32, (SUB, LANES), 1)
    sub = lax.broadcasted_iota(jnp.int32, (SUB, LANES), 0)
    high_lane, low_lane = lane // SUB, lane % SUB
    to_left = jnp.where(high_lane > 0, lane - SUB, jnp.where(low_lane > 0, 119 + low_lane, 0))
    to_right = jnp.where(
        high_lane < 15, lane + SUB, jnp.where(low_lane < 7, low_lane + 1, LANES - 1)
    )
    not_first_lane = lane > 0
    not_last_lane = lane < LANES - 1
    not_first_sub = sub > 0
    not_last_sub = sub < SUB - 1

    pl.semaphore_wait(barrier, 3 * lateral - 1)

    def wave_copy(f):
        return remote(
            wave_ref.at[f],
            wave_in.at[slab],
            wave_sems,
            (f,),
            device(worker(home, f)),
            (slab,),
        )

    def wave_arrival(d):
        return remote(
            wave_ref.at[0], wave_in.at[d], wave_sems, (d,), device(owner(chain, d))
        )

    def map_copy(tick, y):
        to = worker(home if tick == 0 else section, 2 * y + core)
        copy = remote(
            map_ref,
            map_in.at[tick, slab],
            map_sems,
            (tick, y),
            device(to),
            (tick, slab // 2),
        )
        live = to != me
        return copy, live if tick == 0 else live & is_deep

    def map_arrival(tick, h):
        d = core + 2 * h
        source = owner(chain + tick, d)
        copy = remote(map_ref, map_in.at[tick, d], map_sems, (tick, h), device(source))
        return copy, source != me

    def map_relay(tick, h):
        part = map_in.at[tick, core + 2 * h]
        return remote(part, part, relay_sems, (tick, h), partner)

    def pass_map_on(tick):
        for h in range(2):
            copy, foreign = map_arrival(tick, h)
            pl.when(foreign)(copy.wait_recv)
            pl.when(jnp.logical_not(foreign))(own_map.wait)
            map_relay(tick, h).start()

    def start_map(tick):
        for y in (1, 0):
            copy, live = map_copy(tick, y)
            pl.when(live)(copy.start)

    far = side == 1

    def hop_in(i):
        return pltpu.make_async_remote_copy(
            src_ref=wave_ref.at[i // 2, i % 2],
            dst_ref=hop.at[i // 2, i % 2],
            send_sem=hop_sems.at[0, i],
            recv_sem=hop_sems.at[1, i],
            device_id=device(worker(plane, core)),
            device_id_type=MESH,
        )

    def hop_on(i):
        return remote(
            hop.at[i // 2, i % 2],
            wave_in.at[core, i % 2],
            on_sems,
            (i,),
            device(worker(plane + 1, i // 2)),
            (2 * core + i % 2,),
        )

    def hop_arrival(d, c):
        return remote(
            hop.at[0, c],
            wave_in.at[d, c],
            on_sems,
            (2 * d + c,),
            device(worker(chain, d)),
        )

    start_map(0)

    @pl.when(far)
    def _():
        for i in range(lateral):
            hop_in(i).start()

    for f in range(half, lateral):
        wave_copy(f).start()

    @pl.when(near)
    def _():
        for f in range(half):
            pl.when(worker(home, f) != me)(wave_copy(f).start)
        start_map(1)

    for copy in small:
        copy.wait()
    entry = entries[chain, place]
    angle = pulsations[entry] * slownesses[...]
    cosine, sine = jnp.cos(angle), jnp.sin(angle)
    for k in range(ORDER + 1):
        fr, fi = (weights[entry, k, pl.ds(c, 1), :] for c in range(2))
        rows[pl.ds(k, 1), pl.ds(0, NBIN)] = fr * cosine - fi * sine
        rows[pl.ds(ORDER + 1 + k, 1), pl.ds(0, NBIN)] = fr * sine + fi * cosine
    for n in range(ROWS):
        row = jnp.broadcast_to(rows[pl.ds(n, 1), :], (SUB, LANES))
        for part in range(NBIN // SUB):
            spread_table[part, n] = lane_pick(row, sub + part * SUB)

    def pass_waves_on(some):
        for i in some:
            hop_in(i).wait_recv()
            hop_on(i).start()

    pl.when(near)(lambda: pass_waves_on(range(lateral - 1)))


    def cell(m, r):
        return pl.ds((m * SUB + r) * SUB, SUB)

    def column(m, slot):
        return pl.ds(m * SUB * SUB + slot, SUB, stride=SUB)

    def gather_back(source, d, g):
        return transposed([source[column(m, groups * d + g), :] for m in range(SUB)])

    def tile(g, j):
        return pl.ds(g * SUB, SUB), pl.ds(j * LANES, LANES)

    def spread(load, ref, d):
        for g in range(groups):
            for m, x in enumerate(transposed([load(*tile(g, j)) for j in range(SUB)])):
                ref[column(m, groups * d + g), :] = x

    def fill(tick, level):
        for d in range(lateral):
            spread(lambda row, col: map_in[tick, d, level, row, col], bins, d)
        n_cells = 16

        def some(i, carry):
            for n in range(n_cells):
                where = pl.ds(pl.multiple_of((i * n_cells + n) * SUB, SUB), SUB)
                bin_ = bins[where, :]
                high = bin_ >= SUB
                low_bits = bin_ % SUB
                for row in range(ROWS):
                    a, b = (
                        jnp.take_along_axis(
                            spread_table[part, row],
                            low_bits,
                            axis=0,
                            mode="promise_in_bounds",
                            wrap_negative_indices=False,
                        )
                        for part in range(NBIN // SUB)
                    )
                    coeffs[level, row, where, :] = jnp.where(high, b, a)
            return carry

        lax.fori_loop(0, SUB * SUB // n_cells, some, 0)

    def stencil(present, target, first=False, last=False):
        def channel(c, carry):
            below = []
            for m in range(8):
                edge = pltpu.roll(present[c, cell(m, 7), :], 1, 0)
                edge = jnp.where(not_first_sub, edge, 0.0)
                below.append(edge + present[c, cell(m, 0), :])
            for r in range(8):
                u = []
                for m in range(8):
                    here = present[c, cell(m, r), :]
                    if r < 7:
                        above = present[c, cell(m, r + 1), :]
                    else:
                        above = pltpu.roll(present[c, cell(m, 0), :], SUB - 1, 0)
                        above = jnp.where(not_last_sub, above, 0.0)
                    q = here + above
                    u.append(below[m] + q)
                    below[m] = q
                left = jnp.where(not_first_lane, lane_pick(u[7], to_left), 0.0)
                right = jnp.where(not_last_lane, lane_pick(u[0], to_right), 0.0)
                u = [left] + u + [right]
                h = [u[m] + u[m + 1] for m in range(9)]
                for m in range(8):
                    w = h[m] + h[m + 1]
                    here = present[c, cell(m, r), :]
                    if first:
                        both = 0.125 * w
                    else:
                        both = 0.25 * w - paired_sum[c, cell(m, r), :]
                    if not last:
                        paired_sum[c, cell(m, r), :] = both
                    target[c, cell(m, r), :] = both - here
            return carry

        lax.fori_loop(0, 2, channel, 0)

    def add_orders(tick, level, terms, where, total):
        re, im = (None, None) if total is None else total
        for order, ref in terms:
            tr, ti = (ref[c, where, :] for c in range(2))
            br = coeffs[level, order, where, :]
            bi = coeffs[level, ORDER + 1 + order, where, :]
            dr = br * tr - bi * ti
            di = br * ti + bi * tr
            re, im = (dr, di) if re is None else (re + dr, im + di)
        return re, im

    def sum_so_far(where):
        return [running[c, where, :] for c in range(2)]

    def unit(tick, level, output):
        start = starts.at[tick * LEVELS + level]
        stencil(start, odd, first=True)
        for i in range(SUB * SUB):
            where = pl.ds(i * SUB, SUB)
            total = add_orders(tick, level, [(0, start), (1, odd)], where, None)
            for c in range(2):
                running[c, where, :] = total[c]

        def steps(i, carry):
            stencil(odd, even)
            stencil(even, odd)
            for n in range(SUB * SUB):
                where = pl.ds(n * SUB, SUB)
                terms = [(2 * i + 2, even), (2 * i + 3, odd)]
                total = add_orders(tick, level, terms, where, sum_so_far(where))
                for c in range(2):
                    running[c, where, :] = total[c]
            return carry

        lax.fori_loop(0, ORDER // 2 - 1, steps, 0)
        stencil(odd, even, last=True)
        for i in range(SUB * SUB):
            where = pl.ds(i * SUB, SUB)
            total = add_orders(tick, level, [(ORDER, even)], where, sum_so_far(where))
            for c in range(2):
                output[c, where, :] = total[c]
            raw[tick, level, i] = total[0]

    def slot(n):
        return pl.ds(groups * n, groups)

    def raw_part(tick, level, d):
        return raw.at[tick, level, :, slot(d), :]

    def raw_copy(tick, level, d):
        to = owner(chain + tick, d)
        copy = pltpu.make_async_remote_copy(
            src_ref=raw_part(tick, level, d),
            dst_ref=raw_in.at[tick, level, place],
            send_sem=raw_sent.at[tick, level],
            recv_sem=raw_got.at[tick, level],
            device_id=device(to),
            device_id_type=MESH,
        )
        return copy, to != me

    def own_raw(tick, level):
        return pltpu.make_async_copy(
            raw_part(tick, level, slab), raw_in.at[tick, level, place], raw_got.at[tick, level]
        )

    def raw_arrivals(tick, level):
        every = raw_in.at[tick, level]
        return pltpu.make_async_copy(every, every, raw_got.at[tick, level])

    def raw_departures(tick, level, n):
        some = raw.at[tick, level, :, pl.ds(0, groups * n), :]
        return pltpu.make_async_copy(some, some, raw_sent.at[tick, level])

    def send_raw(tick, level):
        for d in range(lateral):
            copy, foreign = raw_copy(tick, level, d)
            pl.when(foreign)(copy.start)
        pl.when((slab_home == tick))(own_raw(tick, level).start)

    def wave_back(which, d):
        to = owner(chain + which, d)
        copy = pltpu.make_async_remote_copy(
            src_ref=wave_out.at[which, d],
            dst_ref=handed_ref.at[place],
            send_sem=back_sent.at[which, d],
            recv_sem=back_got,
            device_id=device(to),
            device_id_type=MESH,
        )
        return copy, to != me

    def own_back(which):
        return pltpu.make_async_copy(wave_out.at[which, slab], handed_ref.at[place], back_got)

    def send_wave(which, source):
        for d in (2, 0, 3, 1):
            for c in range(2):
                for g in range(groups):
                    for j, x in enumerate(gather_back(source.at[c], d, g)):
                        wave_out[(which, d, c) + tile(g, j)] = x
            copy, foreign = wave_back(which, d)
            pl.when(foreign)(copy.start)
            pl.when(jnp.logical_not(foreign))(own_back(which).start)

    pass_map_on(0)
    for h in range(2):
        map_relay(0, h).wait_recv()
    pl.when(far)(lambda: start_map(1))
    fill(0, 0)
    pl.when(near)(lambda: pass_waves_on((lateral - 1,)))
    fill(0, 1)
    def take_waves(order):
        for d in order:
            foreign = owner(chain, d) != me
            pl.when(foreign)(wave_arrival(d).wait_recv)
            pl.when(jnp.logical_not(foreign))(own_wave.wait)
            for c in range(2):
                spread(lambda row, col: wave_in[d, c, row, col], starts.at[0, c], d)

    @pl.when(near)
    def _():
        take_waves((2, 3))
        for d in range(half):
            for c in range(2):
                hop_arrival(d, c).wait_recv()
                spread(lambda row, col: wave_in[d, c, row, col], starts.at[0, c], d)

    pl.when(far)(lambda: take_waves((0, 1, 2, 3)))
    unit(0, 0, starts.at[1])
    send_raw(0, 0)
    pl.when(has_next)(lambda: pass_map_on(1))
    unit(0, 1, starts.at[2])
    send_raw(0, 1)

    @pl.when(chain == 0)
    def _():
        send_wave(0, starts.at[2])

    @pl.when(has_next)
    def _():
        for h in range(2):
            map_relay(1, h).wait_recv()
        fill(1, 0)
        fill(1, 1)
        unit(1, 0, starts.at[3])
        send_raw(1, 0)
        unit(1, 1, last)
        send_raw(1, 1)
        send_wave(1, last)

    for level in range(LEVELS):
        for tick in range(TICKS):
            arrivals = raw_arrivals(tick, level)
            if tick == 0:
                arrivals.wait()
            else:
                pl.when(is_deep)(arrivals.wait)
        total = jnp.zeros((groups, LANES), jnp.float32)
        for i in range(SUB * SUB):
            value = second = None
            for f in range(lateral):
                a, b = (raw_in[t, level, f, i] for t in range(TICKS))
                value = a if value is None else value + a
                second = b if second is None else second + b
            value = value + jnp.where(is_deep, second, 0.0)
            summed[level, pl.ds(i * groups, groups), :] = value
            total = total + value * value
        sum_own[pl.ds(level * SUB, groups), :] = total
        sum_own[pl.ds(level * SUB + groups, SUB - groups), :] = jnp.zeros(
            (SUB - groups, LANES), jnp.float32
        )

    def sum_copy(x):
        mate = lax.rem(slab + x, lateral)
        return remote(
            sum_own, sum_in.at[x], sum_sems, (x - 1,), device(owner(section, mate))
        )

    for x in range(1, lateral):
        sum_copy(x).start()
    for tick in range(TICKS):
        for y in range(2):
            copy, live = map_copy(tick, y)
            pl.when(live)(copy.wait_send)
    for h in range(2):
        map_relay(0, h).wait_send()
        pl.when(has_next)(map_relay(1, h).wait_send)
    for n in range(lateral):
        if n < half:
            pl.when(near & (worker(home, n) != me))(wave_copy(n).wait_send)
        else:
            wave_copy(n).wait_send()
        pl.when(near)(hop_on(n).wait_send)
        pl.when(far)(hop_in(n).wait_send)
        for which, live in ((0, chain == 0), (1, has_next)):
            copy, foreign = wave_back(which, n)
            pl.when(foreign & live)(copy.wait_send)
    for level in range(LEVELS):
        for tick in range(TICKS):
            live = True if tick == 0 else has_next
            own = side == tick
            pl.when(own & live)(raw_departures(tick, level, lateral - 1).wait)
            pl.when(jnp.logical_not(own) & live)(raw_departures(tick, level, lateral).wait)
    for level in range(LEVELS):
        for g in range(groups):
            part = [
                summed[level, pl.ds(m * SUB * groups + g, SUB, stride=groups), :]
                for m in range(SUB)
            ]
            for j, x in enumerate(transposed(part)):
                image_ref[(level,) + tile(g, j)] = x
    total = sum_own[...]
    for x in range(1, lateral):
        sum_copy(x).wait_recv()
        total = total + sum_in[x]
    cells = length * lateral * SUB * LANES
    for level in range(LEVELS):
        mean = (
            jnp.sum(total[level * SUB : (level + 1) * SUB], axis=(0, 1), keepdims=True) / cells
        )
        scale = jnp.broadcast_to(1.0 / jnp.sqrt(mean + 1e-06), (SUB, LANES))
        for g in range(groups):
            for j in range(SUB):
                where = (level,) + tile(g, j)
                image_ref[where] = image_ref[where] * scale
    pltpu.make_async_copy(handed_ref, handed_ref, back_got).wait()
    for x in range(1, lateral):
        sum_copy(x).wait_send()


def phase_table(filter_weights, scaled_pulsations, inverse_speed_classes):
    angle = scaled_pulsations[:, None] * inverse_speed_classes[None, :]
    cosine = jnp.cos(angle)[:, None, :]
    sine = jnp.sin(angle)[:, None, :]
    by_order = jnp.transpose(filter_weights, (2, 0, 3, 1))
    real = by_order[0] * cosine - by_order[1] * sine
    imag = by_order[0] * sine + by_order[1] * cosine
    table = jnp.stack([real, imag], axis=2).reshape(NW, 2 * (ORDER + 1), NBIN)
    return jnp.pad(table, ((0, 0), (0, 0), (0, LANES - NBIN)))


def chains(
    incoming_wave,
    speed_class_map,
    spectral_entry_index,
    filter_weights,
    scaled_pulsations,
    inverse_speed_classes,
):
    count = lax.axis_size("strip")
    lateral = count // SECTIONS
    length, across = incoming_wave.shape[2:]
    tall = length * lateral * SUB
    f32 = jnp.float32
    vmem = pl.BlockSpec(memory_space=pltpu.VMEM)
    anywhere = pl.BlockSpec(memory_space=pl.ANY)
    def dma(*shape):
        return pltpu.SemaphoreType.DMA((2,) + shape)

    return pl.pallas_call(
        functools.partial(chain_kernel, count),
        out_shape=(
            jax.ShapeDtypeStruct(speed_class_map.shape, f32),
            jax.ShapeDtypeStruct(incoming_wave.shape, f32),
        ),
        in_specs=[anywhere] * 6,
        out_specs=(vmem, vmem),
        scratch_shapes=[
            pltpu.SMEM(spectral_entry_index.shape, jnp.int32),
            pltpu.SMEM((NW,), f32),
            pltpu.VMEM((1, NBIN), f32),
            pltpu.VMEM((NW, ORDER + 1, 2, NBIN), f32),
            pltpu.VMEM((ROWS, LANES), f32),
            pltpu.VMEM((lateral // 2, 2, length, across), f32),
            pltpu.VMEM((TICKS * LEVELS, 2, tall, LANES), f32),
            pltpu.VMEM((2, tall, LANES), f32),
            pltpu.VMEM((2, tall, LANES), f32),
            pltpu.VMEM((2, tall, LANES), f32),
            pltpu.VMEM((2, tall, LANES), f32),
            pltpu.VMEM((2, tall, LANES), f32),
            pltpu.VMEM((LEVELS, ROWS, tall, LANES), f32),
            pltpu.VMEM((NBIN // SUB, ROWS, SUB, LANES), f32),
            pltpu.VMEM((lateral, 2, length, across), f32),
            pltpu.VMEM((TICKS, lateral, LEVELS, length, across), jnp.int32),
            pltpu.VMEM((tall, LANES), jnp.int32),
            pltpu.VMEM((TICKS, LEVELS, SUB * SUB, SUB, LANES), f32),
            pltpu.VMEM((2, lateral, 2, length, across), f32),
            pltpu.VMEM((LEVELS, SUB * SUB * length // SUB, LANES), f32),
            pltpu.VMEM((TICKS, LEVELS, lateral, SUB * SUB, length // SUB, LANES), f32),
            pltpu.VMEM((LEVELS * SUB, LANES), f32),
            pltpu.VMEM((lateral, LEVELS * SUB, LANES), f32),
            pltpu.SemaphoreType.DMA((4,)),
            dma(lateral),
            dma(lateral),
            dma(lateral),
            dma(TICKS, 2),
            dma(TICKS, 2),
            pltpu.SemaphoreType.DMA((2, lateral)),
            pltpu.SemaphoreType.DMA,
            pltpu.SemaphoreType.DMA((TICKS, LEVELS)),
            pltpu.SemaphoreType.DMA((TICKS, LEVELS)),
            dma(lateral - 1),
            pltpu.SemaphoreType.DMA((2,)),
        ],
        compiler_params=pltpu.CompilerParams(
            collective_id=0, has_side_effects=True, vmem_limit_bytes=32 * 1024 * 1024
        ),
    )(
        *(
            pltpu.with_memory_space_constraint(x, pltpu.HBM)
            for x in (
                spectral_entry_index,
                scaled_pulsations,
                inverse_speed_classes[None],
                jnp.transpose(filter_weights, (0, 3, 2, 1)),
                incoming_wave,
                speed_class_map,
            )
        )
    )


def fits(mesh):
    lateral = mesh.shape["strip"] // SECTIONS
    return NFREQ % 2 == 0 and lateral % 4 == 0


def whole_section(mesh, wave):
    lateral = mesh.shape["strip"] // SECTIONS
    full = lateral * wave.shape[2] == SUB * SUB and wave.shape[3] == SUB * LANES
    return lateral == NFREQ == 4 and wave.shape[2] % SUB == 0 and full


def body_for(mesh):
    def body(wave, *rest):
        whole = wave.shape[3] == SUB * LANES and wave.shape[2] % SUB == 0
        if whole_section(mesh, wave):
            return chains(wave, *rest)
        if fits(mesh) and whole and wave.shape[2] >= ORDER:
            return paired(wave, *rest)
        return shards(wave, *rest)

    return body


def solution(mesh):
    return jax.shard_map(
        body_for(mesh),
        mesh=mesh,
        in_specs=(
            P("groups", None, "strip", None),
            P("groups", "strip", None),
            P("groups", None),
            P(),
            P(),
            P(),
        ),
        out_specs=(P("groups", "strip", None), P("groups", None, "strip", None)),
        check_vma=False,
    )
```

```python
import functools
import jax
import jax.numpy as jnp
from jax import lax
from jax.experimental import pallas as pl
from jax.experimental.pallas import tpu as pltpu
from jax.sharding import PartitionSpec as P

SECTIONS = 4
LEVELS = 2
ORDER = 12
NFREQ = 4
NBIN = 16
NW = 16


def extended_2(shard, sides, width):
    for axis, dim in sides:
        devices, length = (lax.axis_size(axis), shard.shape[dim])
        up = [(i, (i + 1) % devices) for i in range(devices)]
        down = [(j, i) for i, j in up]
        last = lax.slice_in_dim(shard, length - width, length, axis=dim)
        initial = lax.slice_in_dim(shard, 0, width, axis=dim)
        before = lax.ppermute(last, axis, up)
        after = lax.ppermute(initial, axis, down)
        shard = jnp.concatenate([before, shard, after], axis=dim)
    return shard


def from_behind(shard, axis, by):
    devices = lax.axis_size(axis)
    return lax.ppermute(shard, axis, [(i, (i + by) % devices) for i in range(devices)])


def stencil_padded(padded):
    vertical = padded[:, :, :-2, :] + padded[:, :, 2:, :]
    middle = padded[:, :, 1:-1, :]
    return (
        -0.5 * middle[..., 1:-1]
        + 0.25 * (vertical[..., 1:-1] + middle[..., :-2] + middle[..., 2:])
        + 0.125 * (vertical[..., :-2] + vertical[..., 2:])
    )


def complex_times(coeff, field):
    real_part = coeff[:, 0] * field[:, 0] - coeff[:, 1] * field[:, 1]
    imag_part = coeff[:, 0] * field[:, 1] + coeff[:, 1] * field[:, 0]
    return jnp.stack([real_part, imag_part], axis=1)


def shards(
    incoming_wave,
    speed_class_map,
    spectral_entry_index,
    filter_weights,
    scaled_pulsations,
    inverse_speed_classes,
):
    highest = lax.Precision.HIGHEST
    summed_along = incoming_wave.shape[2]
    summed_across = incoming_wave.shape[3]
    strip_count = lax.axis_size("strip")
    lateral_count = strip_count // SECTIONS
    position = (lax.axis_index("strip") - lateral_count // 2) % strip_count
    vertical_slab = position // lateral_count
    lateral_place = position % lateral_count
    section_rows = summed_along * lateral_count
    section_cells = section_rows * summed_across
    margin = ORDER
    extended_rows = summed_along + 2 * margin
    lateral_rows = (
        lateral_place * summed_along - margin + jnp.arange(extended_rows, dtype=jnp.int32)
    )
    inside = ((lateral_rows >= 0) & (lateral_rows < section_rows)).astype(jnp.float32)[
        None, None, :, None
    ]

    def mcclellan_step(field):
        padded = jnp.pad(field, ((0, 0), (0, 0), (1, 1), (0, 0)))
        padded = jnp.pad(padded, ((0, 0), (0, 0), (0, 0), (1, 1)))
        result = stencil_padded(padded)
        result = result * inside
        return result

    def interior(field):
        return field[:, :, margin : margin + summed_along, :]

    def image_downward(field, batch_index):
        freq_row = lax.dynamic_index_in_dim(spectral_entry_index, batch_index, 0, keepdims=False)
        freq_select = (freq_row[:, None] == jnp.arange(NW, dtype=jnp.int32)[None, :]).astype(
            jnp.float32
        )
        freq_coeffs = jnp.einsum("fw,wbck->fbck", freq_select, filter_weights, precision=highest)
        freq_omega = jnp.dot(freq_select, scaled_pulsations, precision=highest)
        wavefield = field
        raws = []
        for level in range(LEVELS):
            cells = speed_class_map[level].reshape(-1)
            bin_onehot = (cells[None, :] == jnp.arange(NBIN, dtype=jnp.int32)[:, None]).astype(
                jnp.float32
            )
            cell_slowness = jnp.dot(inverse_speed_classes, bin_onehot, precision=highest).reshape(
                summed_along, summed_across
            )
            table = jnp.einsum("fbck,bn->kfcn", freq_coeffs, bin_onehot, precision=highest).reshape(
                ORDER + 1, NFREQ, 2, summed_along, summed_across
            )
            extended = extended_2(wavefield, (("strip", 2),), ORDER) * inside
            previous = extended
            current = mcclellan_step(extended)
            accumulated = complex_times(table[0], interior(previous)) + complex_times(
                table[1], interior(current)
            )

            def recursion_step(order_index, state_tuple):
                before, present, running = state_tuple
                following = 2.0 * mcclellan_step(present) - before
                coeff = lax.dynamic_index_in_dim(table, order_index, 0, keepdims=False)
                running = running + complex_times(coeff, interior(following))
                return (present, following, running)

            previous, current, accumulated = lax.fori_loop(
                2, ORDER + 1, recursion_step, (previous, current, accumulated)
            )
            phase_angle = freq_omega[:, None, None] * cell_slowness[None]
            cosine = jnp.cos(phase_angle)
            sine_part = jnp.sin(phase_angle)
            real_part = accumulated[:, 0] * cosine - accumulated[:, 1] * sine_part
            imag_part = accumulated[:, 0] * sine_part + accumulated[:, 1] * cosine
            wavefield = jnp.stack([real_part, imag_part], axis=1)
            raws.append(jnp.sum(real_part, axis=0))
        return (wavefield, raws)

    above_floor_lines, above_unscaled_waves = image_downward(incoming_wave, vertical_slab)
    arriving = from_behind(above_floor_lines, "strip", lateral_count)
    second_bottom, second_raws = image_downward(arriving, jnp.maximum(vertical_slab - 1, 0))
    handed = jnp.where(vertical_slab == 0, above_floor_lines, second_bottom)
    first_section = (vertical_slab > 0).astype(jnp.float32)
    totals = [
        above_unscaled_waves[level] + first_section * second_raws[level] for level in range(LEVELS)
    ]
    selector = (jnp.arange(SECTIONS, dtype=jnp.int32) == vertical_slab).astype(jnp.float32)
    images = []
    for level in range(LEVELS):
        raw_image = totals[level]
        spread = lax.psum(selector * jnp.sum(raw_image * raw_image), "strip")
        mean_square = jnp.sum(spread * selector) / section_cells
        images.append(raw_image / jnp.sqrt(mean_square + 1e-06))
    return (jnp.stack(images, axis=0), handed)


SUB = 8
LANES = 128
PAD = 5
UNROLL = 8
TOGETHER = 4
MESH = pl.DeviceIdType.MESH


def at_row(row):
    return pl.ds(pl.multiple_of(row * SUB, SUB), SUB)


def kernel(
    strip_count,
    entry_ref,
    wave_ref,
    map_ref,
    table_ref,
    image_ref,
    handed_ref,
    starts,
    work,
    bottom,
    last,
    last_in,
    wave_out,
    map_out,
    map_all,
    raw,
    raw_in,
    sum_own,
    sum_in,
    swap_sems,
    halo_sems,
    hand_sems,
    fin_sems,
    raw_sems,
    sum_sems,
):
    nfh = wave_ref.shape[0] // 2
    length = wave_ref.shape[2]
    rows = 2 * length
    blocks = wave_ref.shape[3] // LANES
    lateral = strip_count // SECTIONS
    shift = lateral // 2
    pairs = lateral // 2
    margin = ORDER
    first = PAD + margin
    me = lax.axis_index("strip")
    position = lax.rem(me + strip_count - shift, strip_count)
    section = position // lateral
    place = lax.rem(position, lateral)
    pair = place // 2
    half = lax.rem(place, 2)
    up = jnp.where(pair > 0, 1, 0)
    down = jnp.where(pair < pairs - 1, 1, 0)
    has_up = pair > 0
    has_down = pair < pairs - 1
    has_before = section > 0
    has_after = section < SECTIONS - 1
    other = 1 - half

    def device(pos):
        return {"strip": lax.rem(pos + shift + strip_count, strip_count)}

    partner = device(position + 1 - 2 * half)
    upper = device(position - 2)
    lower = device(position + 2)
    deeper = device(position + lateral)
    shallower = device(position + strip_count - lateral)

    def remote(src, dst, sems, index, target):
        return pltpu.make_async_remote_copy(
            src_ref=src,
            dst_ref=dst,
            send_sem=sems.at[(0,) + index],
            recv_sem=sems.at[(1,) + index],
            device_id=target,
            device_id_type=MESH,
        )

    def span(row, count):
        return pl.ds(pl.multiple_of(row * SUB, SUB), count * SUB)

    zero = jnp.zeros((SUB, LANES), jnp.float32)
    for edge in (first - 1, first + rows):
        for f in range(nfh):
            for c in range(2):
                for s in range(2 * LEVELS):
                    starts[s, f, c, at_row(edge), :] = zero
        for c in range(2):
            for k in range(ORDER):
                work[k, c, at_row(edge), :] = zero

    barrier = pltpu.get_barrier_semaphore()
    for d in range(1, lateral):
        mate = device(section * lateral + lax.rem(place + d, lateral))
        pl.semaphore_signal(barrier, inc=1, device_id=mate, device_id_type=MESH)
    for target in (deeper, shallower):
        pl.semaphore_signal(barrier, inc=1, device_id=target, device_id_type=MESH)

    def rearrange(load, store):
        for g in range(length // SUB):
            for j in range(blocks):
                store(g, j, load(g, j))

    def strided(row, g, j):
        return pl.ds((row + g * SUB) * SUB + j, SUB, stride=SUB)

    own_row = half * length
    swaps = []
    for f in range(nfh):
        for c in range(2):
            rearrange(
                lambda g, j: wave_ref[other * nfh + f, c, pl.ds(g * SUB, SUB), pl.ds(j * LANES, LANES)],
                lambda g, j, x: pltpu_store(wave_out.at[f, c], strided(0, g, j), x),
            )
        if f == 0:
            pl.semaphore_wait(barrier, lateral + 1)
        copy = remote(
            wave_out.at[f],
            starts.at[0, f, :, span(first + own_row, length), :],
            swap_sems,
            (f,),
            partner,
        )
        copy.start()
        swaps.append(copy)
    for l in range(LEVELS):
        rearrange(
            lambda g, j: map_ref[l, pl.ds(g * SUB, SUB), pl.ds(j * LANES, LANES)],
            lambda g, j, x: pltpu_store(map_out.at[l], strided(0, g, j), x),
        )
    copy = remote(
        map_out, map_all.at[:, span(own_row, length), :], swap_sems, (nfh,), partner
    )
    copy.start()
    swaps.append(copy)
    for f in range(nfh):
        for c in range(2):
            rearrange(
                lambda g, j: wave_ref[half * nfh + f, c, pl.ds(g * SUB, SUB), pl.ds(j * LANES, LANES)],
                lambda g, j, x: pltpu_store(
                    starts.at[0, f, c], strided(first + own_row, g, j), x
                ),
            )
    for l in range(LEVELS):
        rearrange(
            lambda g, j: map_ref[l, pl.ds(g * SUB, SUB), pl.ds(j * LANES, LANES)],
            lambda g, j, x: pltpu_store(map_all.at[l], strided(own_row, g, j), x),
        )

    def halo_up(stage, f):
        ref = starts.at[stage, f]
        return remote(
            ref.at[:, span(first, margin), :],
            ref.at[:, span(first + rows, margin), :],
            halo_sems,
            (stage, f, 0),
            upper,
        )

    def halo_down(stage, f):
        ref = starts.at[stage, f]
        return remote(
            ref.at[:, span(first + rows - margin, margin), :],
            ref.at[:, span(first - margin, margin), :],
            halo_sems,
            (stage, f, 1),
            lower,
        )

    def send_halo(stage, f):
        pl.when(has_up)(lambda: halo_up(stage, f).start())
        pl.when(has_down)(lambda: halo_down(stage, f).start())

    def wait_halo(stage, f):
        pl.when(has_down)(lambda: halo_up(stage, f).wait_recv())
        pl.when(has_up)(lambda: halo_down(stage, f).wait_recv())

    def hand_parts(f):
        parts = ((0, margin), (rows - margin, margin), (margin, rows - 2 * margin))
        return [
            remote(
                bottom.at[f, :, span(row, count), :],
                starts.at[LEVELS, f, :, span(first + row, count), :],
                hand_sems,
                (f, n),
                deeper,
            )
            for n, (row, count) in enumerate(parts)
        ]

    lane = lax.broadcasted_iota(jnp.int32, (SUB, LANES), 1)
    sub = lax.broadcasted_iota(jnp.int32, (SUB, LANES), 0)
    at_first = lane == 0
    at_last = lane == LANES - 1
    keep_first = sub > 0
    keep_last = sub < SUB - 1

    def across(u):
        right = pltpu.roll(u, 1, 1)
        right_fix = jnp.where(keep_first, pltpu.roll(right, 1, 0), 0.0)
        left = pltpu.roll(u, LANES - 1, 1)
        left_fix = jnp.where(keep_last, pltpu.roll(left, SUB - 1, 0), 0.0)
        return jnp.where(at_first, right_fix, right) + jnp.where(at_last, left_fix, left)

    def reach(k):
        return ((margin - k + UNROLL - 1) // UNROLL) * UNROLL

    def apply(k, present, before, target):
        extra = reach(k)
        low = first - up * extra
        count = (rows + (up + down) * extra) // UNROLL

        def block(i, carry):
            base = low + i * UNROLL
            v = [
                [present[c, at_row(base - 1 + n), :] for n in range(UNROLL + 2)]
                for c in range(2)
            ]
            old = None
            if before is not None:
                old = [
                    [before[c, at_row(base + n), :] for n in range(UNROLL)] for c in range(2)
                ]
            values = []
            for c in range(2):
                q = [v[c][n] + v[c][n + 1] for n in range(UNROLL + 1)]
                for n in range(UNROLL):
                    u = q[n] + q[n + 1]
                    w = across(u) + (u + u)
                    centre = v[c][n + 1]
                    if old is None:
                        value = 0.125 * w - centre
                    else:
                        value = 0.25 * w - (centre + centre + old[c][n])
                    values.append(value)
            for c in range(2):
                for n in range(UNROLL):
                    target[c, at_row(base + n), :] = values[c * UNROLL + n]
            return carry

        lax.fori_loop(0, count, block, 0)

    def unit(tick, level, f, meanwhile=None):
        stage = tick * LEVELS + level
        start = starts.at[stage, f]
        apply(1, start, None, work.at[0])
        apply(2, work.at[0], start, work.at[1])

        def step(k, carry):
            apply(k, work.at[k - 2], work.at[k - 3], work.at[k - 1])
            return carry

        lax.fori_loop(3, ORDER + 1, step, 0)
        if meanwhile is not None:
            meanwhile()
        batch = section if tick == 0 else jnp.maximum(section - 1, 0)
        entry = entry_ref[batch, half * nfh + f]

        def combine(i, carry):
            spots = [TOGETHER * i + n for n in range(TOGETHER)]
            bins = [map_all[level, at_row(r), :] for r in spots]
            real = [None] * TOGETHER
            imag = [None] * TOGETHER
            for n, r in enumerate(spots):
                for k in range(ORDER + 1):
                    cr, ci = (
                        jnp.take_along_axis(
                            jnp.broadcast_to(
                                table_ref[entry, pl.ds(2 * k + c, 1), :], (SUB, LANES)
                            ),
                            bins[n],
                            axis=1,
                            mode="promise_in_bounds",
                        )
                        for c in range(2)
                    )
                    source = start if k == 0 else work.at[k - 1]
                    tr = source[0, at_row(first + r), :]
                    ti = source[1, at_row(first + r), :]
                    re = cr * tr - ci * ti
                    im = cr * ti + ci * tr
                    real[n] = re if k == 0 else real[n] + re
                    imag[n] = im if k == 0 else imag[n] + im
            for n, r in enumerate(spots):
                re, im = real[n], imag[n]
                if tick == 0 and f == 0:
                    raw[level, at_row(r), :] = re
                else:
                    part = re if tick == 0 else jnp.where(has_before, re, 0.0)
                    raw[level, at_row(r), :] = raw[level, at_row(r), :] + part
                for c, value in enumerate((re, im)):
                    if level < LEVELS - 1:
                        starts[stage + 1, f, c, at_row(first + r), :] = value
                    elif tick == 0:
                        bottom[f, c, at_row(r), :] = value
                    else:
                        last[f, c, at_row(r), :] = jnp.where(
                            has_before, value, bottom[f, c, at_row(r), :]
                        )
            return carry

        lax.fori_loop(0, rows // TOGETHER, combine, 0)

    def finish_wave(f):
        return remote(
            last.at[f, :, span(other * length, length), :],
            last_in.at[f],
            fin_sems,
            (f,),
            partner,
        )

    def finish_raw(l):
        return remote(
            raw.at[l, span(other * length, length), :], raw_in.at[l], raw_sems, (l,), partner
        )

    for f in range(nfh):
        swaps[f].wait_recv()
        send_halo(0, f)
    swaps[nfh].wait_recv()
    for level in range(LEVELS):
        for f in range(nfh):
            wait_halo(level, f)
            unit(0, level, f)
            if level < LEVELS - 1:
                send_halo(level + 1, f)
            else:

                @pl.when(has_after)
                def _():
                    for copy in hand_parts(f):
                        copy.start()

    def forward(f):
        @pl.when(has_before)
        def _():
            high, low, mid = hand_parts(f)
            high.wait_recv()
            pl.when(has_up)(lambda: halo_up(LEVELS, f).start())
            low.wait_recv()
            pl.when(has_down)(lambda: halo_down(LEVELS, f).start())
            mid.wait_recv()

    def skip_or(fn):
        pl.when(has_before)(fn)

    forward(0)
    for level in range(LEVELS):
        for f in range(nfh):

            @pl.when(has_before)
            def _():
                wait_halo(LEVELS + level, f)

            later = f + 1 if level == 0 and f + 1 < nfh else None
            unit(1, level, f, None if later is None else lambda: forward(later))
            if level < LEVELS - 1:

                @pl.when(has_before)
                def _():
                    send_halo(LEVELS + level + 1, f)

            else:
                finish_wave(f).start()
        finish_raw(level).start()

    for l in range(LEVELS):
        finish_raw(l).wait_recv()

        def merge(i, carry):
            value = raw[l, at_row(own_row + i), :] + raw_in[l, at_row(i), :]
            raw_in[l, at_row(i), :] = value
            return carry + value * value

        sum_own[pl.ds(l * SUB, SUB), :] = lax.fori_loop(0, length, merge, zero)
    for d in range(1, lateral):
        mate = device(section * lateral + lax.rem(place + d, lateral))
        remote(sum_own, sum_in.at[d], sum_sems, (d,), mate).start()

    for f in range(nfh):
        for c in range(2):
            rearrange(
                lambda g, j: last[f, c, strided(own_row, g, j), :],
                lambda g, j, x: out_store(handed_ref, half * nfh + f, c, g, j, x),
            )
    for f in range(nfh):
        finish_wave(f).wait_recv()
        for c in range(2):
            rearrange(
                lambda g, j: last_in[f, c, strided(0, g, j), :],
                lambda g, j, x: out_store(handed_ref, other * nfh + f, c, g, j, x),
            )

    total = sum_own[...]
    for d in range(1, lateral):
        mate = device(section * lateral + lax.rem(place + d, lateral))
        remote(sum_own, sum_in.at[d], sum_sems, (d,), mate).wait_recv()
        total = total + sum_in[d]
    cells = length * lateral * blocks * LANES
    for l in range(LEVELS):
        mean = jnp.sum(total[l * SUB : (l + 1) * SUB], axis=(0, 1), keepdims=True) / cells
        scale = jnp.broadcast_to(1.0 / jnp.sqrt(mean + 1e-06), (SUB, LANES))

        def put(g, j, x):
            image_ref[l, pl.ds(g * SUB, SUB), pl.ds(j * LANES, LANES)] = x * scale

        rearrange(lambda g, j: raw_in[l, strided(0, g, j), :], put)

    for copy in swaps:
        copy.wait_send()
    for f in range(nfh):
        send_done = lambda make, stage: make(stage, f).wait_send()
        for stage in range(2 * LEVELS):
            live_up = has_up if stage < LEVELS else has_up & has_before
            live_down = has_down if stage < LEVELS else has_down & has_before
            pl.when(live_up)(lambda: send_done(halo_up, stage))
            pl.when(live_down)(lambda: send_done(halo_down, stage))

        @pl.when(has_after)
        def _():
            for copy in hand_parts(f):
                copy.wait_send()

        finish_wave(f).wait_send()
    for l in range(LEVELS):
        finish_raw(l).wait_send()
    for d in range(1, lateral):
        mate = device(section * lateral + lax.rem(place + d, lateral))
        remote(sum_own, sum_in.at[d], sum_sems, (d,), mate).wait_send()


def pltpu_store(ref, where, x):
    ref[where, :] = x


def out_store(ref, f, c, g, j, x):
    ref[f, c, pl.ds(g * SUB, SUB), pl.ds(j * LANES, LANES)] = x


def paired(
    incoming_wave,
    speed_class_map,
    spectral_entry_index,
    filter_weights,
    scaled_pulsations,
    inverse_speed_classes,
):
    strip_count = lax.axis_size("strip")
    lateral = strip_count // SECTIONS
    length = incoming_wave.shape[2]
    nfh = NFREQ // 2
    rows = 2 * length
    tall = (rows + 2 * ORDER + 2 * PAD) * SUB
    table = phase_table(filter_weights, scaled_pulsations, inverse_speed_classes)
    f32 = jnp.float32
    vmem = pl.BlockSpec(memory_space=pltpu.VMEM)

    def dma(*shape):
        return pltpu.SemaphoreType.DMA((2,) + shape)

    return pl.pallas_call(
        functools.partial(kernel, strip_count),
        out_shape=(
            jax.ShapeDtypeStruct(speed_class_map.shape, f32),
            jax.ShapeDtypeStruct(incoming_wave.shape, f32),
        ),
        in_specs=[pl.BlockSpec(memory_space=pltpu.SMEM), vmem, vmem, vmem],
        out_specs=(vmem, vmem),
        scratch_shapes=[
            pltpu.VMEM((2 * LEVELS, nfh, 2, tall, LANES), f32),
            pltpu.VMEM((ORDER, 2, tall, LANES), f32),
            pltpu.VMEM((nfh, 2, rows * SUB, LANES), f32),
            pltpu.VMEM((nfh, 2, rows * SUB, LANES), f32),
            pltpu.VMEM((nfh, 2, length * SUB, LANES), f32),
            pltpu.VMEM((nfh, 2, length * SUB, LANES), f32),
            pltpu.VMEM((LEVELS, length * SUB, LANES), jnp.int32),
            pltpu.VMEM((LEVELS, rows * SUB, LANES), jnp.int32),
            pltpu.VMEM((LEVELS, rows * SUB, LANES), f32),
            pltpu.VMEM((LEVELS, length * SUB, LANES), f32),
            pltpu.VMEM((LEVELS * SUB, LANES), f32),
            pltpu.VMEM((lateral, LEVELS * SUB, LANES), f32),
            dma(nfh + 1),
            dma(2 * LEVELS, nfh, 2),
            dma(nfh, 3),
            dma(nfh),
            dma(LEVELS),
            dma(lateral),
        ],
        compiler_params=pltpu.CompilerParams(
            collective_id=0, has_side_effects=True, vmem_limit_bytes=48 * 1024 * 1024
        ),
    )(spectral_entry_index, incoming_wave, speed_class_map, table)


ROWS = 2 * (ORDER + 1)
TICKS = 2


def lane_pick(x, index):
    return jnp.take_along_axis(
        x, index, axis=1, mode="promise_in_bounds", wrap_negative_indices=False
    )


def transposed(x):
    lane = lax.broadcasted_iota(jnp.int32, (SUB, LANES), 1)
    low = lane % SUB
    bits = [(step, (lane // step) % 2 == 1) for step in (1, 2, 4)]
    x = list(x)
    for step, bit in bits:
        x = [jnp.where(bit, x[(a + step) % SUB], x[a]) for a in range(SUB)]
    for a in range(1, SUB):
        x[a] = lane_pick(x[a], lane - low + (low + SUB - a) % SUB)
    x = [x[-n % SUB] for n in range(SUB)]
    for step, bit in bits:
        x = [jnp.where(bit, x[(m - step) % SUB], x[m]) for m in range(SUB)]
    return x


def chain_kernel(
    count,
    entry_ref,
    pulsation_ref,
    slowness_ref,
    weight_ref,
    wave_ref,
    map_ref,
    image_ref,
    handed_ref,
    entries,
    pulsations,
    slownesses,
    weights,
    rows,
    hop,
    starts,
    last,
    even,
    odd,
    paired_sum,
    running,
    coeffs,
    spread_table,
    wave_in,
    map_in,
    bins,
    raw,
    wave_out,
    summed,
    raw_in,
    sum_own,
    sum_in,
    small_sems,
    wave_sems,
    hop_sems,
    on_sems,
    map_sems,
    relay_sems,
    back_sent,
    back_got,
    raw_sent,
    raw_got,
    sum_sems,
    own_sems,
):
    length = wave_ref.shape[2]
    groups = length // SUB
    lateral = count // SECTIONS
    half = lateral // 2
    me = lax.axis_index("strip")
    plane = me // lateral
    place = lax.rem(me, lateral)
    side = place // 2
    core = lax.rem(place, 2)
    chain = lax.rem(plane + SECTIONS - 1, SECTIONS)
    section = lax.rem(chain + side, SECTIONS)
    slab = lax.rem(place + half, lateral)
    home = lax.rem(section + 1, SECTIONS)
    near = side == 0
    has_next = chain < SECTIONS - 1
    is_deep = section > 0

    def wrapped(index):
        return lax.rem(index + count, count)

    def device(index):
        return {"strip": wrapped(index)}

    def worker(plane_, f):
        return wrapped(plane_ * lateral + f)

    def owner(section_, d):
        return wrapped(section_ * lateral + half + d)

    partner = device(me + 1 - 2 * core)

    def remote(src, dst, sems, index, target, arrival=None):
        return pltpu.make_async_remote_copy(
            src_ref=src,
            dst_ref=dst,
            send_sem=sems.at[(0,) + index],
            recv_sem=sems.at[(1,) + (index if arrival is None else arrival)],
            device_id=target,
            device_id_type=MESH,
        )

    barrier = pltpu.get_barrier_semaphore()
    base = (plane - 1) * lateral
    for n in range(3 * lateral):
        mate = wrapped(base + n)

        @pl.when(mate != me)
        def _():
            pl.semaphore_signal(barrier, inc=1, device_id=device(mate), device_id_type=MESH)

    small = [
        pltpu.make_async_copy(source, target, small_sems.at[n])
        for n, (source, target) in enumerate(
            (
                (entry_ref, entries),
                (pulsation_ref, pulsations),
                (slowness_ref, slownesses),
                (weight_ref, weights),
            )
        )
    ]
    for copy in small:
        copy.start()
    own_wave = pltpu.make_async_copy(wave_ref.at[place], wave_in.at[slab], own_sems.at[0])
    own_map = pltpu.make_async_copy(map_ref, map_in.at[side, slab], own_sems.at[1])
    pl.when(near)(own_wave.start)
    pl.when(near | has_next)(own_map.start)

    lane = lax.broadcasted_iota(jnp.int32, (SUB, LANES), 1)
    sub = lax.broadcasted_iota(jnp.int32, (SUB, LANES), 0)
    high_lane, low_lane = lane // SUB, lane % SUB
    to_left = jnp.where(high_lane > 0, lane - SUB, jnp.where(low_lane > 0, 119 + low_lane, 0))
    to_right = jnp.where(
        high_lane < 15, lane + SUB, jnp.where(low_lane < 7, low_lane + 1, LANES - 1)
    )
    not_first_lane = lane > 0
    not_last_lane = lane < LANES - 1
    not_first_sub = sub > 0
    not_last_sub = sub < SUB - 1

    pl.semaphore_wait(barrier, 3 * lateral - 1)

    def wave_copy(f):
        return remote(
            wave_ref.at[f],
            wave_in.at[slab],
            wave_sems,
            (f,),
            device(worker(home, f)),
            (slab,),
        )

    def wave_arrival(d):
        return remote(
            wave_ref.at[0], wave_in.at[d], wave_sems, (d,), device(owner(chain, d))
        )

    def map_copy(tick, y):
        to = worker(home if tick == 0 else section, 2 * y + core)
        copy = remote(
            map_ref,
            map_in.at[tick, slab],
            map_sems,
            (tick, y),
            device(to),
            (tick, slab // 2),
        )
        live = to != me
        return copy, live if tick == 0 else live & is_deep

    def map_arrival(tick, h):
        d = core + 2 * h
        source = owner(chain + tick, d)
        copy = remote(map_ref, map_in.at[tick, d], map_sems, (tick, h), device(source))
        return copy, source != me

    def map_relay(tick, h):
        part = map_in.at[tick, core + 2 * h]
        return remote(part, part, relay_sems, (tick, h), partner)

    def pass_map_on(tick):
        for h in range(2):
            copy, foreign = map_arrival(tick, h)
            pl.when(foreign)(copy.wait_recv)
            pl.when(jnp.logical_not(foreign))(own_map.wait)
            map_relay(tick, h).start()

    def start_map(tick):
        for y in (1, 0):
            copy, live = map_copy(tick, y)
            pl.when(live)(copy.start)

    far = side == 1

    def hop_in(i):
        return pltpu.make_async_remote_copy(
            src_ref=wave_ref.at[i // 2, i % 2],
            dst_ref=hop.at[i // 2, i % 2],
            send_sem=hop_sems.at[0, i],
            recv_sem=hop_sems.at[1, i],
            device_id=device(worker(plane, core)),
            device_id_type=MESH,
        )

    def hop_on(i):
        return remote(
            hop.at[i // 2, i % 2],
            wave_in.at[core, i % 2],
            on_sems,
            (i,),
            device(worker(plane + 1, i // 2)),
            (2 * core + i % 2,),
        )

    def hop_arrival(d, c):
        return remote(
            hop.at[0, c],
            wave_in.at[d, c],
            on_sems,
            (2 * d + c,),
            device(worker(chain, d)),
        )

    start_map(0)

    @pl.when(far)
    def _():
        for i in range(lateral):
            hop_in(i).start()

    for f in range(half, lateral):
        wave_copy(f).start()

    @pl.when(near)
    def _():
        for f in range(half):
            pl.when(worker(home, f) != me)(wave_copy(f).start)
        start_map(1)

    for copy in small:
        copy.wait()
    entry = entries[chain, place]
    angle = pulsations[entry] * slownesses[...]
    cosine, sine = jnp.cos(angle), jnp.sin(angle)
    for k in range(ORDER + 1):
        fr, fi = (weights[entry, k, pl.ds(c, 1), :] for c in range(2))
        rows[pl.ds(k, 1), pl.ds(0, NBIN)] = fr * cosine - fi * sine
        rows[pl.ds(ORDER + 1 + k, 1), pl.ds(0, NBIN)] = fr * sine + fi * cosine
    for n in range(ROWS):
        row = jnp.broadcast_to(rows[pl.ds(n, 1), :], (SUB, LANES))
        for part in range(NBIN // SUB):
            spread_table[part, n] = lane_pick(row, sub + part * SUB)

    def pass_waves_on(some):
        for i in some:
            hop_in(i).wait_recv()
            hop_on(i).start()

    pl.when(near)(lambda: pass_waves_on(range(lateral - 1)))


    def cell(m, r):
        return pl.ds((m * SUB + r) * SUB, SUB)

    def column(m, slot):
        return pl.ds(m * SUB * SUB + slot, SUB, stride=SUB)

    def gather_back(source, d, g):
        return transposed([source[column(m, groups * d + g), :] for m in range(SUB)])

    def tile(g, j):
        return pl.ds(g * SUB, SUB), pl.ds(j * LANES, LANES)

    def spread(load, ref, d):
        for g in range(groups):
            for m, x in enumerate(transposed([load(*tile(g, j)) for j in range(SUB)])):
                ref[column(m, groups * d + g), :] = x

    def fill(tick, level):
        for d in range(lateral):
            spread(lambda row, col: map_in[tick, d, level, row, col], bins, d)
        n_cells = 16

        def some(i, carry):
            for n in range(n_cells):
                where = pl.ds(pl.multiple_of((i * n_cells + n) * SUB, SUB), SUB)
                bin_ = bins[where, :]
                high = bin_ >= SUB
                low_bits = bin_ % SUB
                for row in range(ROWS):
                    a, b = (
                        jnp.take_along_axis(
                            spread_table[part, row],
                            low_bits,
                            axis=0,
                            mode="promise_in_bounds",
                            wrap_negative_indices=False,
                        )
                        for part in range(NBIN // SUB)
                    )
                    coeffs[level, row, where, :] = jnp.where(high, b, a)
            return carry

        lax.fori_loop(0, SUB * SUB // n_cells, some, 0)

    def stencil(present, target, first=False, last=False):
        def channel(c, carry):
            below = []
            for m in range(8):
                edge = pltpu.roll(present[c, cell(m, 7), :], 1, 0)
                edge = jnp.where(not_first_sub, edge, 0.0)
                below.append(edge + present[c, cell(m, 0), :])
            for r in range(8):
                u = []
                for m in range(8):
                    here = present[c, cell(m, r), :]
                    if r < 7:
                        above = present[c, cell(m, r + 1), :]
                    else:
                        above = pltpu.roll(present[c, cell(m, 0), :], SUB - 1, 0)
                        above = jnp.where(not_last_sub, above, 0.0)
                    q = here + above
                    u.append(below[m] + q)
                    below[m] = q
                left = jnp.where(not_first_lane, lane_pick(u[7], to_left), 0.0)
                right = jnp.where(not_last_lane, lane_pick(u[0], to_right), 0.0)
                u = [left] + u + [right]
                h = [u[m] + u[m + 1] for m in range(9)]
                for m in range(8):
                    w = h[m] + h[m + 1]
                    here = present[c, cell(m, r), :]
                    if first:
                        both = 0.125 * w
                    else:
                        both = 0.25 * w - paired_sum[c, cell(m, r), :]
                    if not last:
                        paired_sum[c, cell(m, r), :] = both
                    target[c, cell(m, r), :] = both - here
            return carry

        lax.fori_loop(0, 2, channel, 0)

    def add_orders(tick, level, terms, where, total):
        re, im = (None, None) if total is None else total
        for order, ref in terms:
            tr, ti = (ref[c, where, :] for c in range(2))
            br = coeffs[level, order, where, :]
            bi = coeffs[level, ORDER + 1 + order, where, :]
            dr = br * tr - bi * ti
            di = br * ti + bi * tr
            re, im = (dr, di) if re is None else (re + dr, im + di)
        return re, im

    def sum_so_far(where):
        return [running[c, where, :] for c in range(2)]

    def unit(tick, level, output):
        start = starts.at[tick * LEVELS + level]
        stencil(start, odd, first=True)
        for i in range(SUB * SUB):
            where = pl.ds(i * SUB, SUB)
            total = add_orders(tick, level, [(0, start), (1, odd)], where, None)
            for c in range(2):
                running[c, where, :] = total[c]

        def steps(i, carry):
            stencil(odd, even)
            stencil(even, odd)
            for n in range(SUB * SUB):
                where = pl.ds(n * SUB, SUB)
                terms = [(2 * i + 2, even), (2 * i + 3, odd)]
                total = add_orders(tick, level, terms, where, sum_so_far(where))
                for c in range(2):
                    running[c, where, :] = total[c]
            return carry

        lax.fori_loop(0, ORDER // 2 - 1, steps, 0)
        stencil(odd, even, last=True)
        for i in range(SUB * SUB):
            where = pl.ds(i * SUB, SUB)
            total = add_orders(tick, level, [(ORDER, even)], where, sum_so_far(where))
            for c in range(2):
                output[c, where, :] = total[c]
            raw[tick, level, i] = total[0]

    def slot(n):
        return pl.ds(groups * n, groups)

    def raw_part(tick, level, d):
        return raw.at[tick, level, :, slot(d), :]

    def raw_copy(tick, level, d):
        to = owner(chain + tick, d)
        copy = pltpu.make_async_remote_copy(
            src_ref=raw_part(tick, level, d),
            dst_ref=raw_in.at[tick, level, place],
            send_sem=raw_sent.at[tick, level],
            recv_sem=raw_got.at[tick, level],
            device_id=device(to),
            device_id_type=MESH,
        )
        return copy, to != me

    def own_raw(tick, level):
        return pltpu.make_async_copy(
            raw_part(tick, level, slab), raw_in.at[tick, level, place], raw_got.at[tick, level]
        )

    def raw_arrivals(tick, level):
        every = raw_in.at[tick, level]
        return pltpu.make_async_copy(every, every, raw_got.at[tick, level])

    def raw_departures(tick, level, n):
        some = raw.at[tick, level, :, pl.ds(0, groups * n), :]
        return pltpu.make_async_copy(some, some, raw_sent.at[tick, level])

    def send_raw(tick, level):
        for d in range(lateral):
            copy, foreign = raw_copy(tick, level, d)
            pl.when(foreign)(copy.start)
        pl.when(side == tick)(own_raw(tick, level).start)

    def wave_back(which, d):
        to = owner(chain + which, d)
        copy = pltpu.make_async_remote_copy(
            src_ref=wave_out.at[which, d],
            dst_ref=handed_ref.at[place],
            send_sem=back_sent.at[which, d],
            recv_sem=back_got,
            device_id=device(to),
            device_id_type=MESH,
        )
        return copy, to != me

    def own_back(which):
        return pltpu.make_async_copy(wave_out.at[which, slab], handed_ref.at[place], back_got)

    def send_wave(which, source):
        for d in (2, 0, 3, 1):
            for c in range(2):
                for g in range(groups):
                    for j, x in enumerate(gather_back(source.at[c], d, g)):
                        wave_out[(which, d, c) + tile(g, j)] = x
            copy, foreign = wave_back(which, d)
            pl.when(foreign)(copy.start)
            pl.when(jnp.logical_not(foreign))(own_back(which).start)

    def sum_copy(x):
        mate = lax.rem(slab + x, lateral)
        return remote(
            sum_own, sum_in.at[x], sum_sems, (x - 1,), device(owner(section, mate))
        )

    def square_up():
        for level in range(LEVELS):
            for tick in range(TICKS):
                arrivals = raw_arrivals(tick, level)
                if tick == 0:
                    arrivals.wait()
                else:
                    pl.when(is_deep)(arrivals.wait)
            total = jnp.zeros((groups, LANES), jnp.float32)
            for i in range(SUB * SUB):
                value = second = None
                for f in range(lateral):
                    a, b = (raw_in[t, level, f, i] for t in range(TICKS))
                    value = a if value is None else value + a
                    second = b if second is None else second + b
                value = value + jnp.where(is_deep, second, 0.0)
                summed[level, pl.ds(i * groups, groups), :] = value
                total = total + value * value
            sum_own[pl.ds(level * SUB, groups), :] = total
            sum_own[pl.ds(level * SUB + groups, SUB - groups), :] = jnp.zeros(
                (SUB - groups, LANES), jnp.float32
            )
        for x in range(1, lateral):
            sum_copy(x).start()

    pass_map_on(0)
    for h in range(2):
        map_relay(0, h).wait_recv()
    pl.when(far)(lambda: start_map(1))
    fill(0, 0)
    pl.when(near)(lambda: pass_waves_on((lateral - 1,)))
    fill(0, 1)
    def take_waves(order):
        for d in order:
            foreign = owner(chain, d) != me
            pl.when(foreign)(wave_arrival(d).wait_recv)
            pl.when(jnp.logical_not(foreign))(own_wave.wait)
            for c in range(2):
                spread(lambda row, col: wave_in[d, c, row, col], starts.at[0, c], d)

    @pl.when(near)
    def _():
        take_waves((2, 3))
        for d in range(half):
            for c in range(2):
                hop_arrival(d, c).wait_recv()
                spread(lambda row, col: wave_in[d, c, row, col], starts.at[0, c], d)

    pl.when(far)(lambda: take_waves((0, 1, 2, 3)))
    unit(0, 0, starts.at[1])
    send_raw(0, 0)
    pl.when(has_next)(lambda: pass_map_on(1))
    unit(0, 1, starts.at[2])
    send_raw(0, 1)

    @pl.when(chain == 0)
    def _():
        send_wave(0, starts.at[2])

    @pl.when(has_next)
    def _():
        for h in range(2):
            map_relay(1, h).wait_recv()
        fill(1, 0)
        fill(1, 1)
        unit(1, 0, starts.at[3])
        send_raw(1, 0)
        pl.when(jnp.logical_not(is_deep))(square_up)
        unit(1, 1, last)
        send_raw(1, 1)
        send_wave(1, last)

    pl.when(is_deep | jnp.logical_not(has_next))(square_up)
    for tick in range(TICKS):
        for y in range(2):
            copy, live = map_copy(tick, y)
            pl.when(live)(copy.wait_send)
    for h in range(2):
        map_relay(0, h).wait_send()
        pl.when(has_next)(map_relay(1, h).wait_send)
    for n in range(lateral):
        if n < half:
            pl.when(near & (worker(home, n) != me))(wave_copy(n).wait_send)
        else:
            wave_copy(n).wait_send()
        pl.when(near)(hop_on(n).wait_send)
        pl.when(far)(hop_in(n).wait_send)
        for which, live in ((0, chain == 0), (1, has_next)):
            copy, foreign = wave_back(which, n)
            pl.when(foreign & live)(copy.wait_send)
    for level in range(LEVELS):
        for tick in range(TICKS):
            live = True if tick == 0 else has_next
            own = side == tick
            pl.when(own & live)(raw_departures(tick, level, lateral - 1).wait)
            pl.when(jnp.logical_not(own) & live)(raw_departures(tick, level, lateral).wait)
    for level in range(LEVELS):
        for g in range(groups):
            part = [
                summed[level, pl.ds(m * SUB * groups + g, SUB, stride=groups), :]
                for m in range(SUB)
            ]
            for j, x in enumerate(transposed(part)):
                image_ref[(level,) + tile(g, j)] = x
    total = sum_own[...]
    for x in range(1, lateral):
        sum_copy(x).wait_recv()
        total = total + sum_in[x]
    cells = length * lateral * SUB * LANES
    for level in range(LEVELS):
        mean = (
            jnp.sum(total[level * SUB : (level + 1) * SUB], axis=(0, 1), keepdims=True) / cells
        )
        scale = jnp.broadcast_to(1.0 / jnp.sqrt(mean + 1e-06), (SUB, LANES))
        for g in range(groups):
            for j in range(SUB):
                where = (level,) + tile(g, j)
                image_ref[where] = image_ref[where] * scale
    pltpu.make_async_copy(handed_ref, handed_ref, back_got).wait()
    for x in range(1, lateral):
        sum_copy(x).wait_send()


def phase_table(filter_weights, scaled_pulsations, inverse_speed_classes):
    angle = scaled_pulsations[:, None] * inverse_speed_classes[None, :]
    cosine = jnp.cos(angle)[:, None, :]
    sine = jnp.sin(angle)[:, None, :]
    by_order = jnp.transpose(filter_weights, (2, 0, 3, 1))
    real = by_order[0] * cosine - by_order[1] * sine
    imag = by_order[0] * sine + by_order[1] * cosine
    table = jnp.stack([real, imag], axis=2).reshape(NW, 2 * (ORDER + 1), NBIN)
    return jnp.pad(table, ((0, 0), (0, 0), (0, LANES - NBIN)))


def chains(
    incoming_wave,
    speed_class_map,
    spectral_entry_index,
    filter_weights,
    scaled_pulsations,
    inverse_speed_classes,
):
    count = lax.axis_size("strip")
    lateral = count // SECTIONS
    length, across = incoming_wave.shape[2:]
    tall = length * lateral * SUB
    f32 = jnp.float32
    vmem = pl.BlockSpec(memory_space=pltpu.VMEM)
    anywhere = pl.BlockSpec(memory_space=pl.ANY)
    def dma(*shape):
        return pltpu.SemaphoreType.DMA((2,) + shape)

    return pl.pallas_call(
        functools.partial(chain_kernel, count),
        out_shape=(
            jax.ShapeDtypeStruct(speed_class_map.shape, f32),
            jax.ShapeDtypeStruct(incoming_wave.shape, f32),
        ),
        in_specs=[anywhere] * 6,
        out_specs=(vmem, vmem),
        scratch_shapes=[
            pltpu.SMEM(spectral_entry_index.shape, jnp.int32),
            pltpu.SMEM((NW,), f32),
            pltpu.VMEM((1, NBIN), f32),
            pltpu.VMEM((NW, ORDER + 1, 2, NBIN), f32),
            pltpu.VMEM((ROWS, LANES), f32),
            pltpu.VMEM((lateral // 2, 2, length, across), f32),
            pltpu.VMEM((TICKS * LEVELS, 2, tall, LANES), f32),
            pltpu.VMEM((2, tall, LANES), f32),
            pltpu.VMEM((2, tall, LANES), f32),
            pltpu.VMEM((2, tall, LANES), f32),
            pltpu.VMEM((2, tall, LANES), f32),
            pltpu.VMEM((2, tall, LANES), f32),
            pltpu.VMEM((LEVELS, ROWS, tall, LANES), f32),
            pltpu.VMEM((NBIN // SUB, ROWS, SUB, LANES), f32),
            pltpu.VMEM((lateral, 2, length, across), f32),
            pltpu.VMEM((TICKS, lateral, LEVELS, length, across), jnp.int32),
            pltpu.VMEM((tall, LANES), jnp.int32),
            pltpu.VMEM((TICKS, LEVELS, SUB * SUB, SUB, LANES), f32),
            pltpu.VMEM((2, lateral, 2, length, across), f32),
            pltpu.VMEM((LEVELS, SUB * SUB * length // SUB, LANES), f32),
            pltpu.VMEM((TICKS, LEVELS, lateral, SUB * SUB, length // SUB, LANES), f32),
            pltpu.VMEM((LEVELS * SUB, LANES), f32),
            pltpu.VMEM((lateral, LEVELS * SUB, LANES), f32),
            pltpu.SemaphoreType.DMA((4,)),
            dma(lateral),
            dma(lateral),
            dma(lateral),
            dma(TICKS, 2),
            dma(TICKS, 2),
            pltpu.SemaphoreType.DMA((2, lateral)),
            pltpu.SemaphoreType.DMA,
            pltpu.SemaphoreType.DMA((TICKS, LEVELS)),
            pltpu.SemaphoreType.DMA((TICKS, LEVELS)),
            dma(lateral - 1),
            pltpu.SemaphoreType.DMA((2,)),
        ],
        compiler_params=pltpu.CompilerParams(
            collective_id=0, has_side_effects=True, vmem_limit_bytes=32 * 1024 * 1024
        ),
    )(
        *(
            pltpu.with_memory_space_constraint(x, pltpu.HBM)
            for x in (
                spectral_entry_index,
                scaled_pulsations,
                inverse_speed_classes[None],
                jnp.transpose(filter_weights, (0, 3, 2, 1)),
                incoming_wave,
                speed_class_map,
            )
        )
    )


def fits(mesh):
    lateral = mesh.shape["strip"] // SECTIONS
    return NFREQ % 2 == 0 and lateral % 4 == 0


def whole_section(mesh, wave):
    lateral = mesh.shape["strip"] // SECTIONS
    full = lateral * wave.shape[2] == SUB * SUB and wave.shape[3] == SUB * LANES
    return lateral == NFREQ == 4 and wave.shape[2] % SUB == 0 and full


def body_for(mesh):
    def body(wave, *rest):
        whole = wave.shape[3] == SUB * LANES and wave.shape[2] % SUB == 0
        if whole_section(mesh, wave):
            return chains(wave, *rest)
        if fits(mesh) and whole and wave.shape[2] >= ORDER:
            return paired(wave, *rest)
        return shards(wave, *rest)

    return body


def solution(mesh):
    return jax.shard_map(
        body_for(mesh),
        mesh=mesh,
        in_specs=(
            P("groups", None, "strip", None),
            P("groups", "strip", None),
            P("groups", None),
            P(),
            P(),
            P(),
        ),
        out_specs=(P("groups", "strip", None), P("groups", None, "strip", None)),
        check_vma=False,
    )
```
